8 devices in a mesh: sub: 4 (over z, y, x), fsdp: 2 (over core).
Axes of the slice: x: 2, y: 2, z: 1, core: 2. Of those that a mesh axis runs over, the one named last changes fastest.
Arguments:
- x_in: bfloat16 [16, 512, 1536], P(('sub', 'fsdp'))
- w_q: bfloat16 [2, 1536, 12, 128], P(None, ('sub', 'fsdp'))
- w_k: bfloat16 [2, 1536, 2, 128], P(None, ('sub', 'fsdp'))
- w_v: bfloat16 [2, 1536, 2, 128], P(None, ('sub', 'fsdp'))
- w_o: bfloat16 [2, 1536, 12, 128], P(None, ('sub', 'fsdp'))
- w_up: bfloat16 [2, 1536, 8960], P(None, ('sub', 'fsdp'))
- w_down: bfloat16 [2, 8960, 1536], P(None, ('sub', 'fsdp'))
- grad_out: bfloat16 [16, 512, 1536], P(('sub', 'fsdp'))
Outputs:
- output 1: bfloat16 [16, 512, 1536], P(('sub', 'fsdp'))
- output 2: bfloat16 [16, 512, 1536], P(('sub', 'fsdp'))
- output 3: float32 [2, 1536, 12, 128], P(None, ('sub', 'fsdp'))
- output 4: float32 [2, 1536, 2, 128], P(None, ('sub', 'fsdp'))
- output 5: float32 [2, 1536, 2, 128], P(None, ('sub', 'fsdp'))
- output 6: float32 [2, 1536, 12, 128], P(None, ('sub', 'fsdp'))
- output 7: float32 [2, 1536, 8960], P(None, ('sub', 'fsdp'))
- output 8: float32 [2, 8960, 1536], P(None, ('sub', 'fsdp'))
All inputs are finite; a program needn't handle non-finite values.
Results may differ from the reference program's by a relative error of at most 0.02.
Values are sent between devices in bfloat16 or wider.
A program may use at most 1 GiB of HBM per device.

```python
import jax
import jax.numpy as jnp
from jax import lax

D = 1536
FF = 8960
HEADS = 12
KV_HEADS = 2
HEAD = 128
SEQ = 512
SEQS_DEV = 2
BLOCKS = 8
PAIRS = 2
EPS = 1e-6
MASK_FILL = -1e30

SEQS = BLOCKS * SEQS_DEV
ROWS = SEQS_DEV * SEQ
Q_PER_KV = HEADS // KV_HEADS
Q_WIDTH = HEADS * HEAD
KV_WIDTH = KV_HEADS * HEAD
SCALE = HEAD ** -0.5


def setup_inputs(seed: int = 0) -> dict:
    key_list = jax.random.split(jax.random.key(seed), 8)
    x_in = jax.random.normal(key_list[0], (SEQS, SEQ, D), jnp.float32)
    w_q = jax.random.normal(key_list[1], (PAIRS, D, HEADS, HEAD), jnp.float32) * D ** -0.5
    w_k = jax.random.normal(key_list[2], (PAIRS, D, KV_HEADS, HEAD), jnp.float32) * D ** -0.5
    w_v = jax.random.normal(key_list[3], (PAIRS, D, KV_HEADS, HEAD), jnp.float32) * D ** -0.5
    w_o = jax.random.normal(key_list[4], (PAIRS, D, HEADS, HEAD), jnp.float32) * (2.0 * (Q_WIDTH * PAIRS) ** -0.5)
    w_up = jax.random.normal(key_list[5], (PAIRS, D, FF), jnp.float32) * D ** -0.5
    w_down = jax.random.normal(key_list[6], (PAIRS, FF, D), jnp.float32) * (1.5 * (FF * PAIRS) ** -0.5)
    grad_out = jax.random.normal(key_list[7], (SEQS, SEQ, D), jnp.float32)
    arrays = {"x_in": x_in, "w_q": w_q, "w_k": w_k, "w_v": w_v, "w_o": w_o, "w_up": w_up, "w_down": w_down, "grad_out": grad_out}
    return {name: value.astype(jnp.bfloat16) for name, value in arrays.items()}


def rms_norm(values):
    return values * lax.rsqrt(jnp.mean(values * values, axis=-1, keepdims=True) + EPS)


def norm_bf16(x_blk):
    return rms_norm(x_blk.astype(jnp.float32)).astype(jnp.bfloat16)


def norm_back(x_blk, grad_norm):
    _, pull_back = jax.vjp(rms_norm, x_blk.astype(jnp.float32))
    return pull_back(grad_norm)[0]


def matmul(left, right):
    return jnp.dot(left, right, preferred_element_type=jnp.float32)


def attn_inner(x_blk, q_weight, k_weight, v_weight):
    normed = norm_bf16(x_blk)
    q_act = matmul(normed, q_weight.reshape(D, Q_WIDTH)).astype(jnp.bfloat16)
    k_act = matmul(normed, k_weight.reshape(D, KV_WIDTH)).astype(jnp.bfloat16)
    v_act = matmul(normed, v_weight.reshape(D, KV_WIDTH)).astype(jnp.bfloat16)
    q_grid = q_act.reshape(SEQS_DEV, SEQ, KV_HEADS, Q_PER_KV, HEAD).astype(jnp.float32)
    k_grid = k_act.reshape(SEQS_DEV, SEQ, KV_HEADS, HEAD).astype(jnp.float32)
    v_grid = v_act.reshape(SEQS_DEV, SEQ, KV_HEADS, HEAD).astype(jnp.float32)
    scores = jnp.einsum("bskge,btke->bkgst", q_grid, k_grid) * SCALE
    positions = jnp.arange(SEQ)
    causal = positions[:, None] >= positions[None, :]
    p_float = jax.nn.softmax(jnp.where(causal, scores, MASK_FILL), axis=-1)
    p_bf16 = p_float.astype(jnp.bfloat16)
    o_act = jnp.einsum("bkgst,btke->bskge", p_bf16.astype(jnp.float32), v_grid).astype(jnp.bfloat16)
    return normed, q_grid, k_grid, v_grid, p_float, p_bf16, o_act.reshape(ROWS, Q_WIDTH)


def attn_forward(x_blk, q_weight, k_weight, v_weight, o_weight):
    o_act = attn_inner(x_blk, q_weight, k_weight, v_weight)[6]
    proj = matmul(o_act, o_weight.reshape(D, Q_WIDTH).T)
    return (x_blk.astype(jnp.float32) + proj).astype(jnp.bfloat16)


def attn_backward(x_blk, q_weight, k_weight, v_weight, o_weight, grad_y):
    normed, q_grid, k_grid, v_grid, p_float, p_bf16, o_act = attn_inner(x_blk, q_weight, k_weight, v_weight)
    q_mat = q_weight.reshape(D, Q_WIDTH)
    k_mat = k_weight.reshape(D, KV_WIDTH)
    v_mat = v_weight.reshape(D, KV_WIDTH)
    d_o_w = matmul(grad_y.T, o_act)
    d_o = matmul(grad_y, o_weight.reshape(D, Q_WIDTH)).astype(jnp.bfloat16)
    d_o_grid = d_o.reshape(SEQS_DEV, SEQ, KV_HEADS, Q_PER_KV, HEAD).astype(jnp.float32)
    d_p = jnp.einsum("bskge,btke->bkgst", d_o_grid, v_grid)
    d_v = jnp.einsum("bkgst,bskge->btke", p_bf16.astype(jnp.float32), d_o_grid).astype(jnp.bfloat16)
    d_s = p_float * (d_p - jnp.sum(p_float * d_p, axis=-1, keepdims=True))
    ds_bf16 = (d_s * SCALE).astype(jnp.bfloat16).astype(jnp.float32)
    d_q = jnp.einsum("bkgst,btke->bskge", ds_bf16, k_grid).astype(jnp.bfloat16).reshape(ROWS, Q_WIDTH)
    d_k = jnp.einsum("bkgst,bskge->btke", ds_bf16, q_grid).astype(jnp.bfloat16).reshape(ROWS, KV_WIDTH)
    d_v = d_v.reshape(ROWS, KV_WIDTH)
    d_q_w = matmul(normed.T, d_q)
    d_k_w = matmul(normed.T, d_k)
    d_v_w = matmul(normed.T, d_v)
    d_norm = matmul(d_q, q_mat.T) + matmul(d_k, k_mat.T) + matmul(d_v, v_mat.T)
    grad_x = (grad_y.astype(jnp.float32) + norm_back(x_blk, d_norm)).astype(jnp.bfloat16)
    return (grad_x, d_q_w.reshape(D, HEADS, HEAD), d_k_w.reshape(D, KV_HEADS, HEAD),
            d_v_w.reshape(D, KV_HEADS, HEAD), d_o_w.reshape(D, HEADS, HEAD))


def mlp_forward(x_blk, up_weight, down_weight):
    normed = norm_bf16(x_blk)
    gelu_act = jax.nn.gelu(matmul(normed, up_weight)).astype(jnp.bfloat16)
    return (x_blk.astype(jnp.float32) + matmul(gelu_act, down_weight)).astype(jnp.bfloat16)


def mlp_backward(x_blk, up_weight, down_weight, grad_y):
    normed = norm_bf16(x_blk)
    gelu_f32, gelu_pull = jax.vjp(jax.nn.gelu, matmul(normed, up_weight))
    gelu_act = gelu_f32.astype(jnp.bfloat16)
    d_down = matmul(gelu_act.T, grad_y)
    d_hid = gelu_pull(matmul(grad_y, down_weight.T))[0].astype(jnp.bfloat16)
    d_up = matmul(normed.T, d_hid)
    d_norm = matmul(d_hid, up_weight.T)
    grad_x = (grad_y.astype(jnp.float32) + norm_back(x_blk, d_norm)).astype(jnp.bfloat16)
    return grad_x, d_up, d_down


def block_pass(x_blk, g_blk, weights):
    def fwd_step(carry_x, layer_w):
        q_weight, k_weight, v_weight, o_weight, up_weight, down_weight = layer_w
        mid_act = attn_forward(carry_x, q_weight, k_weight, v_weight, o_weight)
        out_act = mlp_forward(mid_act, up_weight, down_weight)
        return out_act, (carry_x, mid_act)

    y_blk, (attn_in, mlp_in) = lax.scan(fwd_step, x_blk, weights)

    def bwd_step(grad_act, packed):
        q_weight, k_weight, v_weight, o_weight, up_weight, down_weight, attn_x, mlp_x = packed
        grad_mid, d_up, d_down = mlp_backward(mlp_x, up_weight, down_weight, grad_act)
        grad_in, d_q, d_k, d_v, d_o = attn_backward(attn_x, q_weight, k_weight, v_weight, o_weight, grad_mid)
        return grad_in, (d_q, d_k, d_v, d_o, d_up, d_down)

    dx_blk, grads = lax.scan(bwd_step, g_blk, weights + (attn_in, mlp_in), reverse=True)
    return y_blk, dx_blk, grads


def reference(x_in, w_q, w_k, w_v, w_o, w_up, w_down, grad_out):
    weights = (w_q, w_k, w_v, w_o, w_up, w_down)
    x_blocks = x_in.reshape(BLOCKS, ROWS, D)
    g_blocks = grad_out.reshape(BLOCKS, ROWS, D)
    zero_grads = tuple(jnp.zeros(weight.shape, jnp.float32) for weight in weights)

    def block_step(acc_grads, pair_blk):
        y_blk, dx_blk, grads = block_pass(pair_blk[0], pair_blk[1], weights)
        acc_grads = tuple(prev_sum + block_grad for prev_sum, block_grad in zip(acc_grads, grads))
        return acc_grads, (y_blk, dx_blk)

    totals, (y_all, dx_all) = lax.scan(block_step, zero_grads, (x_blocks, g_blocks))
    return (y_all.reshape(SEQS, SEQ, D), dx_all.reshape(SEQS, SEQ, D),
            totals[0], totals[1], totals[2], totals[3], totals[4], totals[5])
```

```python
import jax
import jax.numpy as jnp
from jax import lax
from jax.sharding import PartitionSpec as P

AXES = ("sub", "fsdp")
EPS = 1e-6
MASK_FILL = -1e30
CORES = 2


def rms_norm(values):
    return values * lax.rsqrt(jnp.mean(values * values, axis=-1, keepdims=True) + EPS)


def norm_bf16(x_loc):
    return rms_norm(x_loc.astype(jnp.float32)).astype(jnp.bfloat16)


def norm_back(x_loc, grad_norm):
    _, pull_back = jax.vjp(rms_norm, x_loc.astype(jnp.float32))
    return pull_back(grad_norm)[0]


def mixed(form, left, right):
    return jnp.einsum(form, left, right, preferred_element_type=jnp.float32)


def swap(value):
    return lax.ppermute(value, "fsdp", [(0, 1), (1, 0)])


def by_core(core, mine, other):
    return jnp.where(core == 0, mine, other), jnp.where(core == 0, other, mine)


def to_columns(core, halves):
    keep = jnp.where(core == 0, halves[0], halves[1])
    send = jnp.where(core == 0, halves[1], halves[0])
    first, second = by_core(core, keep, swap(send))
    return jnp.concatenate([first, second], axis=0)


def to_rows(core, grad):
    rows = grad.shape[0] // CORES
    grad = grad.reshape((CORES, rows) + grad.shape[1:])
    keep = lax.dynamic_index_in_dim(grad, core, 0, keepdims=False)
    send = lax.dynamic_index_in_dim(grad, 1 - core, 0, keepdims=False)
    return by_core(core, keep, swap(send))


def gather(piece):
    return lax.all_gather(piece, "sub", axis=0, tiled=True)


def scatter_sum(grad_full):
    return lax.psum_scatter(grad_full, "sub", scatter_dimension=0, tiled=True)


def pair_rows(value):
    return jnp.concatenate([value, swap(value)], axis=0)


def attn_forward(x_own, weight, q_width, head, seq):
    normed = pair_rows(norm_bf16(x_own))
    seqs = normed.shape[0] // seq
    qkv = mixed("td,de->te", normed, weight[:, :q_width + 2 * head]).astype(jnp.bfloat16)
    q_act = qkv[:, :q_width].reshape(seqs, seq, q_width // head, head)
    k_act = qkv[:, q_width:q_width + head].reshape(seqs, seq, head)
    v_act = qkv[:, q_width + head:].reshape(seqs, seq, head)
    scores = mixed("bsge,bte->bgst", q_act, k_act) * (head ** -0.5)
    positions = jnp.arange(seq)
    causal = positions[:, None] >= positions[None, :]
    p_float = jax.nn.softmax(jnp.where(causal, scores, MASK_FILL), axis=-1)
    p_bf16 = p_float.astype(jnp.bfloat16)
    o_act = mixed("bgst,bte->bsge", p_bf16, v_act).astype(jnp.bfloat16).reshape(seqs * seq, q_width)
    o_weight = weight[:, q_width + 2 * head:]
    rows = x_own.shape[0]
    other = swap(mixed("te,de->td", o_act[rows:], o_weight))
    proj = mixed("te,de->td", o_act[:rows], o_weight) + other
    y_own = (x_own.astype(jnp.float32) + proj).astype(jnp.bfloat16)
    return y_own, (x_own, normed, q_act, k_act, v_act, p_float, o_act)


def attn_backward(saved, weight, q_width, head, seq, grad_own):
    x_own, normed, q_act, k_act, v_act, p_float, o_act = saved
    scale = head ** -0.5
    grad_y = pair_rows(grad_own)
    seqs = grad_y.shape[0] // seq
    rows = grad_own.shape[0]
    d_o = mixed("td,de->te", grad_y, weight[:, q_width + 2 * head:]).astype(jnp.bfloat16)
    d_o = d_o.reshape(seqs, seq, q_width // head, head)
    d_o_w = mixed("td,te->de", grad_y, o_act)
    p_bf16 = p_float.astype(jnp.bfloat16)
    d_p = mixed("bsge,bte->bgst", d_o, v_act)
    d_v = mixed("bgst,bsge->bte", p_bf16, d_o).astype(jnp.bfloat16)
    d_s = p_float * (d_p - jnp.sum(p_float * d_p, axis=-1, keepdims=True))
    ds_bf16 = (d_s * scale).astype(jnp.bfloat16)
    d_q = mixed("bgst,bte->bsge", ds_bf16, k_act).astype(jnp.bfloat16)
    d_k = mixed("bgst,bsge->bte", ds_bf16, q_act).astype(jnp.bfloat16)
    d_qkv = jnp.concatenate([d_q.reshape(seqs * seq, q_width), d_k.reshape(seqs * seq, head),
                             d_v.reshape(seqs * seq, head)], axis=1)
    w_qkv = weight[:, :q_width + 2 * head]
    other = swap(mixed("te,de->td", d_qkv[rows:], w_qkv))
    d_norm = mixed("te,de->td", d_qkv[:rows], w_qkv) + other
    grad_x = (grad_own.astype(jnp.float32) + norm_back(x_own, d_norm)).astype(jnp.bfloat16)
    d_qkv_w = mixed("td,te->de", normed, d_qkv)
    return grad_x, d_qkv_w, d_o_w


def mlp_forward(x_own, up_weight, down_weight):
    n_own = norm_bf16(x_own)
    hidden = mixed("td,df->tf", pair_rows(n_own), up_weight)
    gelu_act = jax.nn.gelu(hidden).astype(jnp.bfloat16)
    rows = x_own.shape[0]
    other = swap(mixed("tf,fd->td", gelu_act[rows:], down_weight))
    proj = mixed("tf,fd->td", gelu_act[:rows], down_weight) + other
    y_own = (x_own.astype(jnp.float32) + proj).astype(jnp.bfloat16)
    return y_own, n_own, hidden


def grad_hidden(hidden, grad_y, down_weight):
    _, gelu_pull = jax.vjp(jax.nn.gelu, hidden)
    return gelu_pull(mixed("td,fd->tf", grad_y, down_weight))[0].astype(jnp.bfloat16)


def mlp_backward(x_own, hidden, up_weight, down_weight, grad_own):
    rows = grad_own.shape[0]
    d_hid = grad_hidden(hidden, pair_rows(grad_own), down_weight)
    other = swap(mixed("tf,df->td", d_hid[rows:], up_weight))
    d_norm = mixed("tf,df->td", d_hid[:rows], up_weight) + other
    return (grad_own.astype(jnp.float32) + norm_back(x_own, d_norm)).astype(jnp.bfloat16)


def all_rows(value):
    mine = gather(value)
    return mine, swap(mine)


def mlp_weight_grads(norms, grads, up_block, down_block):
    d_up, d_down = 0.0, 0.0
    for normed, grad_y in zip(norms, grads):
        hidden = mixed("td,df->tf", normed, up_block)
        gelu_act = jax.nn.gelu(hidden).astype(jnp.bfloat16)
        d_down = d_down + mixed("tf,td->fd", gelu_act, grad_y)
        d_hid = grad_hidden(hidden, grad_y, down_block)
        d_up = d_up + mixed("td,tf->df", normed, d_hid)
    return d_up, d_down


def up_rows(core, chip, chips, d_up):
    grid = d_up.reshape((chips, -1) + d_up.shape[1:])
    parts = []
    for step in range(chips):
        part = lax.dynamic_index_in_dim(grid, chip ^ step, 0, keepdims=False)
        parts.append(lax.ppermute(part, "sub", [(i, i ^ step) for i in range(chips)]) if step else part)
    grid = jnp.stack(parts)
    grid = grid.reshape(chips, CORES, grid.shape[1] // CORES, grid.shape[2])
    keep = lax.dynamic_index_in_dim(grid, core, 1, keepdims=False)
    other = swap(lax.dynamic_index_in_dim(grid, 1 - core, 1, keepdims=False))
    both = by_core(core, keep, other)
    cols = [lax.dynamic_index_in_dim(part, chip ^ i, 0, keepdims=False) for i in range(chips) for part in both]
    return jnp.concatenate(cols, axis=1)


def solution(mesh):
    row_spec = P(AXES)
    weight_spec = P(None, AXES)
    chips = mesh.shape["sub"]

    def body(x_loc, w_q, w_k, w_v, w_o, w_up, w_down, grad_out):
        core = lax.axis_index("fsdp")
        chip = lax.axis_index("sub")
        pairs, shard, heads, head = w_q.shape
        seqs, seq, width = x_loc.shape
        q_width = heads // CORES * head
        block = w_down.shape[1]

        def attn_piece(layer):
            halves = []
            for part in range(CORES):
                cols = [w[layer].reshape(shard, CORES, -1)[:, part] for w in (w_q, w_k, w_v, w_o)]
                halves.append(jnp.concatenate(cols, axis=1))
            return to_columns(core, halves)

        def up_piece(layer):
            grid = w_up[layer].reshape(shard, chips, CORES, block)
            return to_columns(core, [grid[:, :, part].reshape(shard, chips * block) for part in range(CORES)])

        attn_full, up_full, down_full, up_block = [], [], [], []
        for layer in range(pairs):
            attn_full.append(gather(attn_piece(layer)))
            up_full.append(gather(up_piece(layer)))
            down_full.append(gather(w_down[layer]))
            up_block.append(lax.select_n(chip, *[up_full[layer][:, i * block:(i + 1) * block] for i in range(chips)]))
        carry_x = x_loc.reshape(seqs * seq, width)
        grad_x = grad_out.reshape(seqs * seq, width)
        attn_saved, mlp_saved = [], []
        for layer in range(pairs):
            carry_x, saved = attn_forward(carry_x, attn_full[layer], q_width, head, seq)
            attn_saved.append(saved)
            x_own = carry_x
            carry_x, n_own, hidden = mlp_forward(x_own, up_full[layer], down_full[layer])
            mlp_saved.append((x_own, all_rows(n_own), hidden))
        y_loc = carry_x.reshape(x_loc.shape)
        grad_lists = ([], [], [], [], [], [])
        for layer in reversed(range(pairs)):
            x_own, norms, hidden = mlp_saved[layer]
            grads = all_rows(grad_x)
            grad_x = mlp_backward(x_own, hidden, up_full[layer], down_full[layer], grad_x)
            d_up, d_down = mlp_weight_grads(norms, grads, up_block[layer], w_down[layer])
            grad_lists[5].append(d_down)
            grad_lists[4].append(up_rows(core, chip, chips, d_up))
            grad_x, d_qkv, d_o = attn_backward(attn_saved[layer], attn_full[layer], q_width, head, seq, grad_x)
            grad_x, d_qkv, d_o = lax.optimization_barrier((grad_x, d_qkv, d_o))
            parts = to_rows(core, scatter_sum(d_o))
            grad_lists[3].append(jnp.concatenate(parts, axis=1).reshape(shard, heads, head))
            parts = to_rows(core, scatter_sum(d_qkv))
            grad_lists[0].append(jnp.concatenate([part[:, :q_width] for part in parts], axis=1)
                                 .reshape(shard, heads, head))
            grad_lists[1].append(jnp.stack([part[:, q_width:q_width + head] for part in parts], axis=1))
            grad_lists[2].append(jnp.stack([part[:, q_width + head:] for part in parts], axis=1))
        return (y_loc, grad_x.reshape(x_loc.shape)) + tuple(jnp.stack(grad_list[::-1]) for grad_list in grad_lists)

    return jax.shard_map(body, mesh=mesh, in_specs=(row_spec,) + (weight_spec,) * 6 + (row_spec,),
                         out_specs=(row_spec, row_spec) + (weight_spec,) * 6, check_vma=False)
```

```python
import functools

import jax
import jax.numpy as jnp
from jax import lax
from jax.experimental import pallas as pl
from jax.experimental.layout import Layout, with_layout_constraint
from jax.experimental.pallas import tpu as pltpu
from jax.sharding import PartitionSpec as P


AXES = ("sub", "fsdp")
EPS = 1e-6
MASK_FILL = -1e30
GELU_A = (2.0 / 3.141592653589793) ** 0.5
GELU_B = 0.044715
CORES = 2
QUERY_BLOCK = 256


def rms_norm(values):
    return values * lax.rsqrt(jnp.mean(values * values, axis=-1, keepdims=True) + EPS)


def norm_bf16(x_loc):
    return rms_norm(x_loc.astype(jnp.float32)).astype(jnp.bfloat16)


def norm_back(x_loc, grad_norm):
    _, pull_back = jax.vjp(rms_norm, x_loc.astype(jnp.float32))
    return pull_back(grad_norm)[0]


def mixed(form, left, right):
    return jnp.einsum(form, left, right, preferred_element_type=jnp.float32)


def swap(value):
    return lax.ppermute(value, "fsdp", [(0, 1), (1, 0)])


def by_core(core, mine, other):
    return jnp.where(core == 0, mine, other), jnp.where(core == 0, other, mine)


def to_columns(core, halves):
    keep = jnp.where(core == 0, halves[0], halves[1])
    send = jnp.where(core == 0, halves[1], halves[0])
    first, second = by_core(core, keep, swap(send))
    return jnp.concatenate([first, second], axis=0)


def to_rows(core, grad):
    rows = grad.shape[0] // CORES
    grad = grad.reshape((CORES, rows) + grad.shape[1:])
    keep = lax.dynamic_index_in_dim(grad, core, 0, keepdims=False)
    send = lax.dynamic_index_in_dim(grad, 1 - core, 0, keepdims=False)
    return by_core(core, keep, swap(send))


def gather(piece):
    return lax.all_gather(piece, "sub", axis=0, tiled=True)


def scatter_sum(grad_full):
    return lax.psum_scatter(grad_full, "sub", scatter_dimension=0, tiled=True)


def pair_rows(value):
    return jnp.concatenate([value, swap(value)], axis=0)


def causal_blocks(seq):
    return [(start, start + QUERY_BLOCK) for start in range(0, seq, QUERY_BLOCK)]


def dot(left, right, contract):
    return lax.dot_general(left, right, (contract, ((), ())), preferred_element_type=jnp.float32)


def probabilities(k_blk, q_blk, scale):
    scores = dot(k_blk, q_blk, ((1,), (1,))) * scale
    keys, queries = scores.shape
    key = lax.broadcasted_iota(jnp.int32, (queries, queries), 0)
    query = lax.broadcasted_iota(jnp.int32, (queries, queries), 1)
    last = jnp.where(key <= query, scores[keys - queries:], MASK_FILL)
    scores = last if keys == queries else jnp.concatenate([scores[:keys - queries], last], axis=0)
    powers = jnp.exp(scores - jnp.max(scores, axis=0, keepdims=True))
    return powers * (1.0 / jnp.sum(powers, axis=0, keepdims=True))


def attn_fwd_kernel(q_width, head, qkv_ref, o_ref):
    seq = qkv_ref.shape[0]
    k_all = qkv_ref[:, q_width:q_width + head]
    v_flip = jnp.transpose(qkv_ref[:, q_width + head:].astype(jnp.float32)).astype(jnp.bfloat16)
    for col in range(0, q_width, head):
        for start, end in causal_blocks(seq):
            probs = probabilities(k_all[:end], qkv_ref[start:end, col:col + head], head ** -0.5)
            o_flip = dot(v_flip[:, :end], probs.astype(jnp.bfloat16), ((1,), (0,)))
            o_ref[start:end, col:col + head] = jnp.transpose(o_flip).astype(jnp.bfloat16)


def attn_bwd_kernel(q_width, head, qkv_ref, d_o_ref, out_ref, d_k_ref, d_v_ref):
    seq = qkv_ref.shape[0]
    scale = head ** -0.5
    k_all = qkv_ref[:, q_width:q_width + head]
    v_all = qkv_ref[:, q_width + head:]
    k_flip = jnp.transpose(k_all.astype(jnp.float32)).astype(jnp.bfloat16)
    d_k_ref[...] = jnp.zeros_like(d_k_ref)
    d_v_ref[...] = jnp.zeros_like(d_v_ref)
    for col in range(0, q_width, head):
        for start, end in causal_blocks(seq):
            q_blk = qkv_ref[start:end, col:col + head]
            d_o_blk = d_o_ref[start:end, col:col + head]
            probs = probabilities(k_all[:end], q_blk, scale)
            d_p = dot(v_all[:end], d_o_blk, ((1,), (1,)))
            d_v_ref[:end] += dot(probs.astype(jnp.bfloat16), d_o_blk, ((1,), (0,)))
            d_s = probs * (d_p - jnp.sum(probs * d_p, axis=0, keepdims=True))
            d_s = (d_s * scale).astype(jnp.bfloat16)
            d_k_ref[:end] += dot(d_s, q_blk, ((1,), (0,)))
            d_q_flip = dot(k_flip[:, :end], d_s, ((1,), (0,)))
            out_ref[start:end, col:col + head] = jnp.transpose(d_q_flip).astype(jnp.bfloat16)
    out_ref[:, q_width:q_width + head] = d_k_ref[...].astype(jnp.bfloat16)
    out_ref[:, q_width + head:] = d_v_ref[...].astype(jnp.bfloat16)


def by_sequence(kernel, seq, q_width, head, args, width, scratch, flops):
    rows = args[0].shape[0]
    return pl.pallas_call(
        functools.partial(kernel, q_width, head),
        grid=(rows // seq,),
        in_specs=[pl.BlockSpec((seq, arg.shape[1]), lambda i: (i, 0)) for arg in args],
        out_specs=pl.BlockSpec((seq, width), lambda i: (i, 0)),
        out_shape=jax.ShapeDtypeStruct((rows, width), jnp.bfloat16),
        scratch_shapes=[pltpu.VMEM((seq, head), jnp.float32)] * scratch,
        cost_estimate=pl.CostEstimate(flops=flops, bytes_accessed=0, transcendentals=0),
    )(*args)


def attn_forward(x_own, weight, q_width, head, seq):
    normed = pair_rows(norm_bf16(x_own))
    qkv = mixed("td,de->te", normed, weight[:, :q_width + 2 * head]).astype(jnp.bfloat16)
    o_act = by_sequence(attn_fwd_kernel, seq, q_width, head, (qkv,), q_width, 0, 20_000_000_000)
    o_weight = weight[:, q_width + 2 * head:]
    rows = x_own.shape[0]
    other = swap(mixed("te,de->td", o_act[rows:], o_weight))
    proj = mixed("te,de->td", o_act[:rows], o_weight) + other
    y_own = (x_own.astype(jnp.float32) + proj).astype(jnp.bfloat16)
    return y_own, (x_own, normed, qkv, o_act)


def attn_backward(saved, weight, q_width, head, seq, grad_own):
    x_own, normed, qkv, o_act = saved
    rows = grad_own.shape[0]
    grad_y = pair_rows(grad_own)
    d_o = mixed("td,de->te", grad_y, weight[:, q_width + 2 * head:]).astype(jnp.bfloat16)
    d_qkv = by_sequence(attn_bwd_kernel, seq, q_width, head, (qkv, d_o), qkv.shape[1], 2, 40_000_000_000)
    w_qkv = weight[:, :q_width + 2 * head]
    other = swap(mixed("te,de->td", d_qkv[rows:], w_qkv))
    d_norm = mixed("te,de->td", d_qkv[:rows], w_qkv) + other
    grad_x = (grad_own.astype(jnp.float32) + norm_back(x_own, d_norm)).astype(jnp.bfloat16)
    return grad_x, mixed("td,te->de", normed, d_qkv), mixed("td,te->de", grad_y, o_act)


def gelu_parts(hidden):
    square = hidden * hidden
    half = 0.5 + 0.5 * jnp.tanh(hidden * (GELU_A + GELU_A * GELU_B * square))
    value = hidden * half
    slope = half + value * (1.0 - half) * (2.0 * GELU_A + 6.0 * GELU_A * GELU_B * square)
    return value.astype(jnp.bfloat16), slope


def mlp_hidden(normed, up_weight):
    return lax.optimization_barrier(gelu_parts(mixed("td,df->tf", normed, up_weight)))


def mlp_output(x_own, gelu_act, down_weight):
    rows = x_own.shape[0]
    other = swap(mixed("tf,fd->td", gelu_act[rows:], down_weight))
    proj = mixed("tf,fd->td", gelu_act[:rows], down_weight) + other
    return (x_own.astype(jnp.float32) + proj).astype(jnp.bfloat16)


def grad_hidden(slope, grad_y, down_weight):
    return (mixed("td,fd->tf", grad_y, down_weight) * slope).astype(jnp.bfloat16)


def mlp_backward(x_own, slope, up_weight, down_weight, grad_own):
    rows = grad_own.shape[0]
    d_hid = grad_hidden(slope, pair_rows(grad_own), down_weight)
    other = swap(mixed("tf,df->td", d_hid[rows:], up_weight))
    d_norm = mixed("tf,df->td", d_hid[:rows], up_weight) + other
    return (grad_own.astype(jnp.float32) + norm_back(x_own, d_norm)).astype(jnp.bfloat16)


def all_rows(value):
    mine = gather(value)
    return mine, swap(mine)


def mlp_weight_grads(norms, grads, up_block, down_block):
    d_up, d_down = 0.0, 0.0
    for normed, grad_y in zip(norms, grads):
        gelu_act, slope = mlp_hidden(normed, up_block)
        d_down = d_down + mixed("tf,td->fd", gelu_act, grad_y)
        d_hid = lax.optimization_barrier(grad_hidden(slope, grad_y, down_block))
        d_up = d_up + mixed("td,tf->df", normed, d_hid)
    return d_up, d_down


def up_rows(core, chip, chips, d_up):
    grid = with_layout_constraint(d_up.reshape((chips, -1) + d_up.shape[1:]), Layout(major_to_minor=(0, 1, 2)))
    parts = []
    for step in range(chips):
        part = lax.dynamic_index_in_dim(grid, chip ^ step, 0, keepdims=False)
        parts.append(lax.ppermute(part, "sub", [(i, i ^ step) for i in range(chips)]) if step else part)
    grid = jnp.stack(parts)
    grid = grid.reshape(chips, CORES, grid.shape[1] // CORES, grid.shape[2])
    keep = lax.dynamic_index_in_dim(grid, core, 1, keepdims=False)
    other = swap(lax.dynamic_index_in_dim(grid, 1 - core, 1, keepdims=False))
    both = by_core(core, keep, other)
    cols = [lax.dynamic_index_in_dim(part, chip ^ i, 0, keepdims=False) for i in range(chips) for part in both]
    return jnp.concatenate(cols, axis=1)


def solution(mesh):
    row_spec = P(AXES)
    weight_spec = P(None, AXES)
    chips = mesh.shape["sub"]

    def body(x_loc, w_q, w_k, w_v, w_o, w_up, w_down, grad_out):
        core = lax.axis_index("fsdp")
        chip = lax.axis_index("sub")
        pairs, shard, heads, head = w_q.shape
        seqs, seq, width = x_loc.shape
        q_width = heads // CORES * head
        block = w_down.shape[1]

        def attn_piece(layer):
            halves = []
            for part in range(CORES):
                cols = [w[layer].reshape(shard, CORES, -1)[:, part] for w in (w_q, w_k, w_v, w_o)]
                halves.append(jnp.concatenate(cols, axis=1))
            return to_columns(core, halves)

        def up_piece(layer):
            grid = w_up[layer].reshape(shard, chips, CORES, block)
            return to_columns(core, [grid[:, :, part].reshape(shard, chips * block) for part in range(CORES)])

        attn_full, up_full, down_full, up_block = [], [], [], []
        for layer in range(pairs):
            attn_full.append(gather(attn_piece(layer)))
            up_full.append(gather(up_piece(layer)))
            down_full.append(gather(w_down[layer]))
            up_block.append(lax.select_n(chip, *[up_full[layer][:, i * block:(i + 1) * block] for i in range(chips)]))
        carry_x = x_loc.reshape(seqs * seq, width)
        grad_x = grad_out.reshape(seqs * seq, width)
        attn_saved, mlp_saved = [], []
        for layer in range(pairs):
            x_own, saved = attn_forward(carry_x, attn_full[layer], q_width, head, seq)
            attn_saved.append(saved)
            n_own = norm_bf16(x_own)
            gelu_act, slope = mlp_hidden(pair_rows(n_own), up_full[layer])
            norms = all_rows(n_own)
            if layer == pairs - 1:
                mlp_grads = mlp_weight_grads(norms, all_rows(grad_x), up_block[layer], w_down[layer])
                down_full[layer], mlp_grads = lax.optimization_barrier((down_full[layer], mlp_grads))
            carry_x = mlp_output(x_own, gelu_act, down_full[layer])
            mlp_saved.append((x_own, norms, slope))
        y_loc = carry_x.reshape(x_loc.shape)
        grad_lists = ([], [], [], [], [], [])
        for layer in reversed(range(pairs)):
            x_own, norms, slope = mlp_saved[layer]
            if layer < pairs - 1:
                mlp_grads = mlp_weight_grads(norms, all_rows(grad_x), up_block[layer], w_down[layer])
            grad_lists[5].append(mlp_grads[1])
            grad_lists[4].append(up_rows(core, chip, chips, mlp_grads[0]))
            grad_x = mlp_backward(x_own, slope, up_full[layer], down_full[layer], grad_x)
            grad_x, d_qkv, d_o = attn_backward(attn_saved[layer], attn_full[layer], q_width, head, seq, grad_x)
            grad_x, d_qkv, d_o = lax.optimization_barrier((grad_x, d_qkv, d_o))
            parts = to_rows(core, scatter_sum(d_o))
            grad_lists[3].append(jnp.concatenate(parts, axis=1).reshape(shard, heads, head))
            parts = to_rows(core, scatter_sum(d_qkv))
            grad_lists[0].append(jnp.concatenate([part[:, :q_width] for part in parts], axis=1)
                                 .reshape(shard, heads, head))
            grad_lists[1].append(jnp.stack([part[:, q_width:q_width + head] for part in parts], axis=1))
            grad_lists[2].append(jnp.stack([part[:, q_width + head:] for part in parts], axis=1))
        return (y_loc, grad_x.reshape(x_loc.shape)) + tuple(jnp.stack(grad_list[::-1]) for grad_list in grad_lists)

    return jax.shard_map(body, mesh=mesh, in_specs=(row_spec,) + (weight_spec,) * 6 + (row_spec,),
                         out_specs=(row_spec, row_spec) + (weight_spec,) * 6, check_vma=False)
```

```python
import functools

import jax
import jax.numpy as jnp
from jax import lax
from jax.experimental import pallas as pl
from jax.experimental.pallas import tpu as pltpu
from jax.sharding import PartitionSpec as P


AXES = ("sub", "fsdp")
EPS = 1e-6
MASK_FILL = -1e30
GELU_A = (2.0 / 3.141592653589793) ** 0.5
GELU_B = 0.044715
CHIPS = 4
CORES = 2
QUERY_BLOCK = 256
TOKEN_TILE = 512
ROW_TILE = 48


def rms_norm(values):
    return values * lax.rsqrt(jnp.mean(values * values, axis=-1, keepdims=True) + EPS)


def norm_bf16(x_loc):
    return rms_norm(x_loc.astype(jnp.float32)).astype(jnp.bfloat16)


def norm_back(x_loc, grad_norm):
    _, pull_back = jax.vjp(rms_norm, x_loc.astype(jnp.float32))
    return pull_back(grad_norm)[0]


def mixed(form, left, right):
    return jnp.einsum(form, left, right, preferred_element_type=jnp.float32)


def swap(value):
    return lax.ppermute(value, "fsdp", [(0, 1), (1, 0)])


def by_core(core, mine, other):
    return jnp.where(core == 0, mine, other), jnp.where(core == 0, other, mine)


def to_columns(core, halves):
    keep = jnp.where(core == 0, halves[0], halves[1])
    send = jnp.where(core == 0, halves[1], halves[0])
    first, second = by_core(core, keep, swap(send))
    return jnp.concatenate([first, second], axis=0)


def to_rows(core, grad):
    rows = grad.shape[0] // CORES
    grad = grad.reshape((CORES, rows) + grad.shape[1:])
    keep = lax.dynamic_index_in_dim(grad, core, 0, keepdims=False)
    send = lax.dynamic_index_in_dim(grad, 1 - core, 0, keepdims=False)
    return by_core(core, keep, swap(send))


def gather(piece):
    return lax.all_gather(piece, "sub", axis=0, tiled=True)


def scatter_sum(grad_full):
    return lax.psum_scatter(grad_full, "sub", scatter_dimension=0, tiled=True)


def pair_rows(value):
    return jnp.concatenate([value, swap(value)], axis=0)


def causal_blocks(seq):
    return [(start, start + QUERY_BLOCK) for start in range(0, seq, QUERY_BLOCK)]


def dot(left, right, contract):
    return lax.dot_general(left, right, (contract, ((), ())), preferred_element_type=jnp.float32)


def probabilities(k_blk, q_blk, scale):
    scores = dot(k_blk, q_blk, ((1,), (1,))) * scale
    keys, queries = scores.shape
    key = lax.broadcasted_iota(jnp.int32, (queries, queries), 0)
    query = lax.broadcasted_iota(jnp.int32, (queries, queries), 1)
    last = jnp.where(key <= query, scores[keys - queries:], MASK_FILL)
    scores = last if keys == queries else jnp.concatenate([scores[:keys - queries], last], axis=0)
    powers = jnp.exp(scores - jnp.max(scores, axis=0, keepdims=True))
    return powers * (1.0 / jnp.sum(powers, axis=0, keepdims=True))


def attn_fwd_kernel(q_width, head, qkv_ref, o_ref):
    seq = qkv_ref.shape[0]
    k_all = qkv_ref[:, q_width:q_width + head]
    v_flip = jnp.transpose(qkv_ref[:, q_width + head:].astype(jnp.float32)).astype(jnp.bfloat16)
    for col in range(0, q_width, head):
        for start, end in causal_blocks(seq):
            probs = probabilities(k_all[:end], qkv_ref[start:end, col:col + head], head ** -0.5)
            o_flip = dot(v_flip[:, :end], probs.astype(jnp.bfloat16), ((1,), (0,)))
            o_ref[start:end, col:col + head] = jnp.transpose(o_flip).astype(jnp.bfloat16)


def attn_bwd_kernel(q_width, head, qkv_ref, d_o_ref, out_ref, d_k_ref, d_v_ref):
    seq = qkv_ref.shape[0]
    scale = head ** -0.5
    k_all = qkv_ref[:, q_width:q_width + head]
    v_all = qkv_ref[:, q_width + head:]
    k_flip = jnp.transpose(k_all.astype(jnp.float32)).astype(jnp.bfloat16)
    d_k_ref[...] = jnp.zeros_like(d_k_ref)
    d_v_ref[...] = jnp.zeros_like(d_v_ref)
    for col in range(0, q_width, head):
        for start, end in causal_blocks(seq):
            q_blk = qkv_ref[start:end, col:col + head]
            d_o_blk = d_o_ref[start:end, col:col + head]
            probs = probabilities(k_all[:end], q_blk, scale)
            d_p = dot(v_all[:end], d_o_blk, ((1,), (1,)))
            d_v_ref[:end] += dot(probs.astype(jnp.bfloat16), d_o_blk, ((1,), (0,)))
            d_s = probs * (d_p - jnp.sum(probs * d_p, axis=0, keepdims=True))
            d_s = (d_s * scale).astype(jnp.bfloat16)
            d_k_ref[:end] += dot(d_s, q_blk, ((1,), (0,)))
            d_q_flip = dot(k_flip[:, :end], d_s, ((1,), (0,)))
            out_ref[start:end, col:col + head] = jnp.transpose(d_q_flip).astype(jnp.bfloat16)
    out_ref[:, q_width:q_width + head] = d_k_ref[...].astype(jnp.bfloat16)
    out_ref[:, q_width + head:] = d_v_ref[...].astype(jnp.bfloat16)


def by_sequence(kernel, seq, q_width, head, args, width, scratch, flops):
    rows = args[0].shape[0]
    return pl.pallas_call(
        functools.partial(kernel, q_width, head),
        grid=(rows // seq,),
        in_specs=[pl.BlockSpec((seq, arg.shape[1]), lambda i: (i, 0)) for arg in args],
        out_specs=pl.BlockSpec((seq, width), lambda i: (i, 0)),
        out_shape=jax.ShapeDtypeStruct((rows, width), jnp.bfloat16),
        scratch_shapes=[pltpu.VMEM((seq, head), jnp.float32)] * scratch,
        cost_estimate=pl.CostEstimate(flops=flops, bytes_accessed=0, transcendentals=0),
    )(*args)


def attn_forward(x_own, weight, q_width, head, seq):
    normed = pair_rows(norm_bf16(x_own))
    qkv = mixed("td,de->te", normed, weight[:, :q_width + 2 * head]).astype(jnp.bfloat16)
    o_act = by_sequence(attn_fwd_kernel, seq, q_width, head, (qkv,), q_width, 0, 20_000_000_000)
    o_weight = weight[:, q_width + 2 * head:]
    rows = x_own.shape[0]
    other = swap(mixed("te,de->td", o_act[rows:], o_weight))
    proj = mixed("te,de->td", o_act[:rows], o_weight) + other
    y_own = (x_own.astype(jnp.float32) + proj).astype(jnp.bfloat16)
    return y_own, (x_own, normed, qkv, o_act)


def attn_backward(saved, weight, q_width, head, seq, grad_own):
    x_own, normed, qkv, o_act = saved
    rows = grad_own.shape[0]
    grad_y = pair_rows(grad_own)
    d_o = mixed("td,de->te", grad_y, weight[:, q_width + 2 * head:]).astype(jnp.bfloat16)
    d_qkv = by_sequence(attn_bwd_kernel, seq, q_width, head, (qkv, d_o), qkv.shape[1], 2, 40_000_000_000)
    w_qkv = weight[:, :q_width + 2 * head]
    other = swap(mixed("te,de->td", d_qkv[rows:], w_qkv))
    d_norm = mixed("te,de->td", d_qkv[:rows], w_qkv) + other
    grad_x = (grad_own.astype(jnp.float32) + norm_back(x_own, d_norm)).astype(jnp.bfloat16)
    d_qkv_w = mixed("td,te->de", normed, d_qkv)
    return grad_x, d_qkv_w, mixed("td,te->de", grad_y, o_act)


def gelu_parts(hidden):
    square = hidden * hidden
    half = 0.5 + 0.5 * jnp.tanh(hidden * (GELU_A + GELU_A * GELU_B * square))
    value = hidden * half
    slope = half + value * (1.0 - half) * (2.0 * GELU_A + 6.0 * GELU_A * GELU_B * square)
    return value.astype(jnp.bfloat16), slope


def mlp_hidden(normed, up_weight):
    return lax.optimization_barrier(gelu_parts(mixed("td,df->tf", normed, up_weight)))


def mlp_output(x_own, gelu_act, down_weight):
    rows = x_own.shape[0]
    other = swap(mixed("tf,fd->td", gelu_act[rows:], down_weight))
    proj = mixed("tf,fd->td", gelu_act[:rows], down_weight) + other
    return (x_own.astype(jnp.float32) + proj).astype(jnp.bfloat16)


def mlp_backward(x_own, slope, up_weight, down_weight, grad_own):
    rows = grad_own.shape[0]
    grad_act = mixed("td,fd->tf", pair_rows(grad_own), down_weight)
    d_hid = (grad_act * slope).astype(jnp.bfloat16)
    other = swap(mixed("tf,df->td", d_hid[rows:], up_weight))
    d_norm = mixed("tf,df->td", d_hid[:rows], up_weight) + other
    return (grad_own.astype(jnp.float32) + norm_back(x_own, d_norm)).astype(jnp.bfloat16)


def all_rows(value):
    mine = gather(value)
    return mine, swap(mine)


def mlp_grads_kernel(half, place_ref, up_ref, down_ref, n0_ref, n1_ref, g0_ref, g1_ref, *rest):
    d_down_ref, parts, d_up_ref, flip_ref = rest[-2 * CHIPS - 3], rest[-2 * CHIPS - 2:-2], rest[-2], rest[-1]
    step = pl.program_id(0)
    normed = jnp.where(step < half, n0_ref[...], n1_ref[...])
    grad_y = jnp.where(step < half, g0_ref[...], g1_ref[...])

    @pl.when(step == 0)
    def _():
        d_down_ref[...] = jnp.zeros_like(d_down_ref)
        d_up_ref[...] = jnp.zeros_like(d_up_ref)

    gelu_act, slope = gelu_parts(dot(up_ref[...], normed, ((1,), (1,))))
    d_hid = (dot(down_ref[...], grad_y, ((1,), (1,))) * slope).astype(jnp.bfloat16)
    d_down_ref[0] += dot(gelu_act, grad_y, ((1,), (0,)))
    d_up_ref[...] += dot(d_hid, normed, ((1,), (0,)))

    @pl.when(step == pl.num_programs(0) - 1)
    def _():
        rows = parts[0].shape[0]
        for i in range(CHIPS):
            start = pl.multiple_of((place_ref[0] ^ i) * (CORES * rows), CORES * rows)
            flip_ref[...] = jnp.transpose(d_up_ref[:, pl.ds(start, CORES * rows)])
            for j in range(CORES):
                start = pl.multiple_of((place_ref[1] ^ j) * rows, rows)
                parts[CORES * i + j][...] = flip_ref[pl.ds(start, rows), :]


def mlp_weight_grads(place, layer, pairs, earlier, up_flip, down_block, norms, grads):
    block, width = down_block.shape
    half = norms[0].shape[0] // TOKEN_TILE
    rows = width // (CHIPS * CORES)
    once = pl.Buffered(1)
    whole = pl.BlockSpec((block, width), lambda i, p: (0, 0), pipeline_mode=once)
    mine = pl.BlockSpec((TOKEN_TILE, width), lambda i, p: (jnp.minimum(i, half - 1), 0))
    others = pl.BlockSpec((TOKEN_TILE, width), lambda i, p: (jnp.maximum(i - half, 0), 0))
    part = pl.BlockSpec((rows, block), lambda i, p: (0, 0), pipeline_mode=once)
    args = [place, up_flip, down_block, norms[0], norms[1], grads[0], grads[1]] + earlier
    outs = pl.pallas_call(
        functools.partial(mlp_grads_kernel, half),
        grid_spec=pltpu.PrefetchScalarGridSpec(
            num_scalar_prefetch=1,
            grid=(2 * half,),
            in_specs=[whole, whole, mine, others, mine, others] + [pl.BlockSpec(memory_space=pl.ANY)] * len(earlier),
            out_specs=[pl.BlockSpec((1, block, width), lambda i, p: (layer, 0, 0), pipeline_mode=once)]
            + [part] * (CHIPS * CORES),
            scratch_shapes=[pltpu.VMEM((block, width), jnp.float32), pltpu.VMEM((CORES * rows, block), jnp.float32)],
        ),
        out_shape=[jax.ShapeDtypeStruct((pairs, block, width), jnp.float32)]
        + [jax.ShapeDtypeStruct((rows, block), jnp.float32)] * (CHIPS * CORES),
        input_output_aliases={7: 0} if earlier else {},
        compiler_params=pltpu.CompilerParams(vmem_limit_bytes=60 * 1024 * 1024),
        cost_estimate=pl.CostEstimate(flops=8 * 2 * norms[0].shape[0] * block * width, bytes_accessed=0,
                                      transcendentals=0),
        name="mlp_grads",
    )(*args)
    return outs[0], outs[1:]


def exchange(parts):
    devices = range(CHIPS * CORES)
    return [lax.ppermute(part, AXES, [(d, d ^ i) for d in devices]) if i else part for i, part in enumerate(parts)]


def assemble_kernel(place_ref, *refs):
    parts, out_ref = [ref[...] for ref in refs[:CHIPS * CORES]], refs[-1]
    for bit in range(3):
        swapped = ((place_ref[0] * CORES + place_ref[1]) >> bit) % 2 == 1
        parts = [jnp.where(swapped, parts[i ^ (1 << bit)], part) for i, part in enumerate(parts)]
    for i, part in enumerate(parts):
        out_ref[0, :, i * part.shape[1]:(i + 1) * part.shape[1]] = part


def assemble(place, layer, pairs, earlier, parts):
    rows, block = parts[0].shape
    out_width = block * len(parts)
    return pl.pallas_call(
        assemble_kernel,
        grid_spec=pltpu.PrefetchScalarGridSpec(
            num_scalar_prefetch=1,
            grid=(rows // ROW_TILE,),
            in_specs=[pl.BlockSpec((ROW_TILE, block), lambda i, p: (i, 0))] * len(parts)
            + [pl.BlockSpec(memory_space=pl.ANY)] * len(earlier),
            out_specs=pl.BlockSpec((1, ROW_TILE, out_width), lambda i, p: (layer, i, 0)),
        ),
        out_shape=jax.ShapeDtypeStruct((pairs, rows, out_width), jnp.float32),
        input_output_aliases={1 + len(parts): 0} if earlier else {},
        cost_estimate=pl.CostEstimate(flops=5_000_000_000, bytes_accessed=0, transcendentals=0),
        name="assemble",
    )(place, *parts, *earlier)


def solution(mesh):
    row_spec = P(AXES)
    weight_spec = P(None, AXES)
    chips = mesh.shape["sub"]

    def body(x_loc, w_q, w_k, w_v, w_o, w_up, w_down, grad_out):
        core = lax.axis_index("fsdp")
        chip = lax.axis_index("sub")
        pairs, shard, heads, head = w_q.shape
        seqs, seq, width = x_loc.shape
        q_width = heads // CORES * head
        block = w_down.shape[1]

        def attn_piece(layer):
            halves = []
            for part in range(CORES):
                cols = [w[layer].reshape(shard, CORES, -1)[:, part] for w in (w_q, w_k, w_v, w_o)]
                halves.append(jnp.concatenate(cols, axis=1))
            return to_columns(core, halves)

        def up_piece(layer):
            grid = w_up[layer].reshape(shard, chips, CORES, block)
            return to_columns(core, [grid[:, :, part].reshape(shard, chips * block) for part in range(CORES)])

        attn_full, up_full, down_full, up_flip = [], [], [], []
        for layer in range(pairs):
            attn_full.append(gather(attn_piece(layer)))
            up_full.append(gather(up_piece(layer)))
            down_full.append(gather(w_down[layer]))
            up_flip.append(lax.select_n(chip, *[up_full[layer][:, i * block:(i + 1) * block] for i in range(chips)]).T)
        place = jnp.stack([chip, core]).astype(jnp.int32)
        carry_x = x_loc.reshape(seqs * seq, width)
        grad_x = grad_out.reshape(seqs * seq, width)
        attn_saved, mlp_saved, d_up, d_down = [], [], [], []

        def weight_grads(layer, norms, grads, d_down):
            down, parts = mlp_weight_grads(place, layer, pairs, d_down, up_flip[layer], w_down[layer], norms, grads)
            return exchange(parts), [down]

        for layer in range(pairs):
            x_own, saved = attn_forward(carry_x, attn_full[layer], q_width, head, seq)
            attn_saved.append(saved)
            n_own = norm_bf16(x_own)
            gelu_act, slope = mlp_hidden(pair_rows(n_own), up_full[layer])
            norms = all_rows(n_own)
            if layer == pairs - 1:
                parts, d_down = weight_grads(layer, norms, all_rows(grad_x), d_down)
            carry_x = mlp_output(x_own, gelu_act, down_full[layer])
            mlp_saved.append((x_own, norms, slope))
        y_loc = carry_x.reshape(x_loc.shape)
        grad_lists = ([], [], [], [])
        for layer in reversed(range(pairs)):
            x_own, norms, slope = mlp_saved[layer]
            if layer < pairs - 1:
                parts, d_down = weight_grads(layer, norms, all_rows(grad_x), d_down)
            d_up = [assemble(place, layer, pairs, d_up, parts)]
            grad_x = mlp_backward(x_own, slope, up_full[layer], down_full[layer], grad_x)
            grad_x, d_qkv, d_o = attn_backward(attn_saved[layer], attn_full[layer], q_width, head, seq, grad_x)
            parts = to_rows(core, scatter_sum(d_o))
            grad_lists[3].append(jnp.concatenate(parts, axis=1).reshape(shard, heads, head))
            parts = to_rows(core, scatter_sum(d_qkv))
            grad_lists[0].append(jnp.concatenate([part[:, :q_width] for part in parts], axis=1)
                                 .reshape(shard, heads, head))
            grad_lists[1].append(jnp.stack([part[:, q_width:q_width + head] for part in parts], axis=1))
            grad_lists[2].append(jnp.stack([part[:, q_width + head:] for part in parts], axis=1))
        stacked = tuple(jnp.stack(grad_list[::-1]) for grad_list in grad_lists)
        return (y_loc, grad_x.reshape(x_loc.shape)) + stacked + (d_up[0], d_down[0])

    return jax.shard_map(body, mesh=mesh, in_specs=(row_spec,) + (weight_spec,) * 6 + (row_spec,),
                         out_specs=(row_spec, row_spec) + (weight_spec,) * 6, check_vma=False)
```

```python
import functools

import jax
import jax.numpy as jnp
from jax import lax
from jax.experimental import pallas as pl
from jax.experimental.pallas import tpu as pltpu
from jax.sharding import PartitionSpec as P


AXES = ("sub", "fsdp")
EPS = 1e-6
MASK_FILL = -1e30
GELU_A = (2.0 / 3.141592653589793) ** 0.5
GELU_B = 0.044715
CHIPS = 4
CORES = 2
QUERY_BLOCK = 256
TOKEN_TILE = 512
ROW_TILE = 48


def rms_norm(values):
    return values * lax.rsqrt(jnp.mean(values * values, axis=-1, keepdims=True) + EPS)


def norm_bf16(x_loc):
    return rms_norm(x_loc.astype(jnp.float32)).astype(jnp.bfloat16)


def norm_back(x_loc, grad_norm):
    _, pull_back = jax.vjp(rms_norm, x_loc.astype(jnp.float32))
    return pull_back(grad_norm)[0]


def mixed(form, left, right):
    return jnp.einsum(form, left, right, preferred_element_type=jnp.float32)


def swap(value):
    return lax.ppermute(value, "fsdp", [(0, 1), (1, 0)])


def by_core(core, mine, other):
    return jnp.where(core == 0, mine, other), jnp.where(core == 0, other, mine)


def to_columns(core, halves):
    keep = jnp.where(core == 0, halves[0], halves[1])
    send = jnp.where(core == 0, halves[1], halves[0])
    first, second = by_core(core, keep, swap(send))
    return jnp.concatenate([first, second], axis=0)


def to_rows(core, grad):
    rows = grad.shape[0] // CORES
    grad = grad.reshape((CORES, rows) + grad.shape[1:])
    keep = lax.dynamic_index_in_dim(grad, core, 0, keepdims=False)
    send = lax.dynamic_index_in_dim(grad, 1 - core, 0, keepdims=False)
    return by_core(core, keep, swap(send))


def gather(piece):
    return lax.all_gather(piece, "sub", axis=0, tiled=True)


def scatter_sum(grad_full):
    return lax.psum_scatter(grad_full, "sub", scatter_dimension=0, tiled=True)


def both_halves(left, right, rows, form):
    other = swap(mixed(form, left[rows:], right))
    own = lax.optimization_barrier(mixed(form, left[:rows], right))
    return own + other


def pair_rows(value):
    return jnp.concatenate([value, swap(value)], axis=0)


def causal_blocks(seq):
    return [(start, start + QUERY_BLOCK) for start in range(0, seq, QUERY_BLOCK)]


def dot(left, right, contract):
    return lax.dot_general(left, right, (contract, ((), ())), preferred_element_type=jnp.float32)


def probabilities(k_blk, q_blk, scale):
    scores = dot(k_blk, q_blk, ((1,), (1,))) * scale
    keys, queries = scores.shape
    key = lax.broadcasted_iota(jnp.int32, (queries, queries), 0)
    query = lax.broadcasted_iota(jnp.int32, (queries, queries), 1)
    last = jnp.where(key <= query, scores[keys - queries:], MASK_FILL)
    scores = last if keys == queries else jnp.concatenate([scores[:keys - queries], last], axis=0)
    powers = jnp.exp(scores - jnp.max(scores, axis=0, keepdims=True))
    return powers * (1.0 / jnp.sum(powers, axis=0, keepdims=True))


def attn_fwd_kernel(q_width, head, qkv_ref, o_ref):
    seq = qkv_ref.shape[0]
    k_all = qkv_ref[:, q_width:q_width + head]
    v_flip = jnp.transpose(qkv_ref[:, q_width + head:].astype(jnp.float32)).astype(jnp.bfloat16)
    for col in range(0, q_width, head):
        for start, end in causal_blocks(seq):
            probs = probabilities(k_all[:end], qkv_ref[start:end, col:col + head], head ** -0.5)
            o_flip = dot(v_flip[:, :end], probs.astype(jnp.bfloat16), ((1,), (0,)))
            o_ref[start:end, col:col + head] = jnp.transpose(o_flip).astype(jnp.bfloat16)


def attn_bwd_kernel(q_width, head, qkv_ref, d_o_ref, out_ref, d_k_ref, d_v_ref):
    seq = qkv_ref.shape[0]
    scale = head ** -0.5
    k_all = qkv_ref[:, q_width:q_width + head]
    v_all = qkv_ref[:, q_width + head:]
    k_flip = jnp.transpose(k_all.astype(jnp.float32)).astype(jnp.bfloat16)
    d_k_ref[...] = jnp.zeros_like(d_k_ref)
    d_v_ref[...] = jnp.zeros_like(d_v_ref)
    for col in range(0, q_width, head):
        for start, end in causal_blocks(seq):
            q_blk = qkv_ref[start:end, col:col + head]
            d_o_blk = d_o_ref[start:end, col:col + head]
            probs = probabilities(k_all[:end], q_blk, scale)
            d_p = dot(v_all[:end], d_o_blk, ((1,), (1,)))
            d_v_ref[:end] += dot(probs.astype(jnp.bfloat16), d_o_blk, ((1,), (0,)))
            d_s = probs * (d_p - jnp.sum(probs * d_p, axis=0, keepdims=True))
            d_s = (d_s * scale).astype(jnp.bfloat16)
            d_k_ref[:end] += dot(d_s, q_blk, ((1,), (0,)))
            d_q_flip = dot(k_flip[:, :end], d_s, ((1,), (0,)))
            out_ref[start:end, col:col + head] = jnp.transpose(d_q_flip).astype(jnp.bfloat16)
    out_ref[:, q_width:q_width + head] = d_k_ref[...].astype(jnp.bfloat16)
    out_ref[:, q_width + head:] = d_v_ref[...].astype(jnp.bfloat16)


def by_sequence(kernel, seq, q_width, head, args, width, scratch, flops):
    rows = args[0].shape[0]
    return pl.pallas_call(
        functools.partial(kernel, q_width, head),
        grid=(rows // seq,),
        in_specs=[pl.BlockSpec((seq, arg.shape[1]), lambda i: (i, 0)) for arg in args],
        out_specs=pl.BlockSpec((seq, width), lambda i: (i, 0)),
        out_shape=jax.ShapeDtypeStruct((rows, width), jnp.bfloat16),
        scratch_shapes=[pltpu.VMEM((seq, head), jnp.float32)] * scratch,
        cost_estimate=pl.CostEstimate(flops=flops, bytes_accessed=0, transcendentals=0),
    )(*args)


def attn_forward(x_own, weight, q_width, head, seq):
    normed = pair_rows(norm_bf16(x_own))
    qkv = mixed("td,de->te", normed, weight[:, :q_width + 2 * head]).astype(jnp.bfloat16)
    o_act = by_sequence(attn_fwd_kernel, seq, q_width, head, (qkv,), q_width, 0, 20_000_000_000)
    o_weight = weight[:, q_width + 2 * head:]
    rows = x_own.shape[0]
    proj = both_halves(o_act, o_weight, rows, "te,de->td")
    y_own = (x_own.astype(jnp.float32) + proj).astype(jnp.bfloat16)
    return y_own, (x_own, normed, qkv, o_act)


def attn_backward(saved, weight, q_width, head, seq, grad_own):
    x_own, normed, qkv, o_act = saved
    rows = grad_own.shape[0]
    grad_y = pair_rows(grad_own)
    d_o = mixed("td,de->te", grad_y, weight[:, q_width + 2 * head:]).astype(jnp.bfloat16)
    d_qkv = by_sequence(attn_bwd_kernel, seq, q_width, head, (qkv, d_o), qkv.shape[1], 2, 40_000_000_000)
    w_qkv = weight[:, :q_width + 2 * head]
    d_norm = both_halves(d_qkv, w_qkv, rows, "te,de->td")
    grad_x = (grad_own.astype(jnp.float32) + norm_back(x_own, d_norm)).astype(jnp.bfloat16)
    d_qkv_w = mixed("td,te->de", normed, d_qkv)
    return grad_x, d_qkv_w, mixed("td,te->de", grad_y, o_act)


def gelu_parts(hidden):
    square = hidden * hidden
    half = 0.5 + 0.5 * jnp.tanh(hidden * (GELU_A + GELU_A * GELU_B * square))
    value = hidden * half
    slope = half + value * (1.0 - half) * (2.0 * GELU_A + 6.0 * GELU_A * GELU_B * square)
    return value.astype(jnp.bfloat16), slope


def mlp_hidden(normed, up_weight):
    return lax.optimization_barrier(gelu_parts(mixed("td,df->tf", normed, up_weight)))


def mlp_output(x_own, gelu_act, down_weight):
    rows = x_own.shape[0]
    proj = both_halves(gelu_act, down_weight, rows, "tf,fd->td")
    return (x_own.astype(jnp.float32) + proj).astype(jnp.bfloat16)


def mlp_backward(x_own, slope, up_weight, down_weight, grad_own):
    rows = grad_own.shape[0]
    grad_act = mixed("td,fd->tf", pair_rows(grad_own), down_weight)
    d_hid = (grad_act * slope).astype(jnp.bfloat16)
    d_norm = both_halves(d_hid, up_weight, rows, "tf,df->td")
    return (grad_own.astype(jnp.float32) + norm_back(x_own, d_norm)).astype(jnp.bfloat16)


def all_rows(value):
    mine = gather(value)
    return mine, swap(mine)


def mlp_grads_kernel(half, place_ref, up_ref, down_ref, n0_ref, n1_ref, g0_ref, g1_ref, *rest):
    d_down_ref, parts, d_up_ref, flip_ref = rest[-2 * CHIPS - 3], rest[-2 * CHIPS - 2:-2], rest[-2], rest[-1]
    step = pl.program_id(0)
    normed = jnp.where(step < half, n0_ref[...], n1_ref[...])
    grad_y = jnp.where(step < half, g0_ref[...], g1_ref[...])

    @pl.when(step == 0)
    def _():
        d_down_ref[...] = jnp.zeros_like(d_down_ref)
        d_up_ref[...] = jnp.zeros_like(d_up_ref)

    gelu_act, slope = gelu_parts(dot(up_ref[...], normed, ((1,), (1,))))
    d_hid = (dot(down_ref[...], grad_y, ((1,), (1,))) * slope).astype(jnp.bfloat16)
    d_down_ref[0] += dot(gelu_act, grad_y, ((1,), (0,)))
    d_up_ref[...] += dot(d_hid, normed, ((1,), (0,)))

    @pl.when(step == pl.num_programs(0) - 1)
    def _():
        rows = parts[0].shape[0]
        for i in range(CHIPS):
            start = pl.multiple_of((place_ref[0] ^ i) * (CORES * rows), CORES * rows)
            flip_ref[...] = jnp.transpose(d_up_ref[:, pl.ds(start, CORES * rows)])
            for j in range(CORES):
                start = pl.multiple_of((place_ref[1] ^ j) * rows, rows)
                parts[CORES * i + j][...] = flip_ref[pl.ds(start, rows), :]


def mlp_weight_grads(place, layer, pairs, earlier, up_flip, down_block, norms, grads):
    block, width = down_block.shape
    half = norms[0].shape[0] // TOKEN_TILE
    rows = width // (CHIPS * CORES)
    once = pl.Buffered(1)
    whole = pl.BlockSpec((block, width), lambda i, p: (0, 0), pipeline_mode=once)
    mine = pl.BlockSpec((TOKEN_TILE, width), lambda i, p: (jnp.minimum(i, half - 1), 0))
    others = pl.BlockSpec((TOKEN_TILE, width), lambda i, p: (jnp.maximum(i - half, 0), 0))
    part = pl.BlockSpec((rows, block), lambda i, p: (0, 0), pipeline_mode=once)
    args = [place, up_flip, down_block, norms[0], norms[1], grads[0], grads[1]] + earlier
    outs = pl.pallas_call(
        functools.partial(mlp_grads_kernel, half),
        grid_spec=pltpu.PrefetchScalarGridSpec(
            num_scalar_prefetch=1,
            grid=(2 * half,),
            in_specs=[whole, whole, mine, others, mine, others] + [pl.BlockSpec(memory_space=pl.ANY)] * len(earlier),
            out_specs=[pl.BlockSpec((1, block, width), lambda i, p: (layer, 0, 0), pipeline_mode=once)]
            + [part] * (CHIPS * CORES),
            scratch_shapes=[pltpu.VMEM((block, width), jnp.float32), pltpu.VMEM((CORES * rows, block), jnp.float32)],
        ),
        out_shape=[jax.ShapeDtypeStruct((pairs, block, width), jnp.float32)]
        + [jax.ShapeDtypeStruct((rows, block), jnp.float32)] * (CHIPS * CORES),
        input_output_aliases={7: 0} if earlier else {},
        compiler_params=pltpu.CompilerParams(vmem_limit_bytes=60 * 1024 * 1024),
        cost_estimate=pl.CostEstimate(flops=8 * 2 * norms[0].shape[0] * block * width, bytes_accessed=0,
                                      transcendentals=0),
        name="mlp_grads",
    )(*args)
    return outs[0], outs[1:]


def exchange(parts):
    devices = range(CHIPS * CORES)
    return [lax.ppermute(part, AXES, [(d, d ^ i) for d in devices]) if i else part for i, part in enumerate(parts)]


def assemble_kernel(place_ref, *refs):
    parts, out_ref = [ref[...] for ref in refs[:CHIPS * CORES]], refs[-1]
    for bit in range(3):
        swapped = ((place_ref[0] * CORES + place_ref[1]) >> bit) % 2 == 1
        parts = [jnp.where(swapped, parts[i ^ (1 << bit)], part) for i, part in enumerate(parts)]
    for i, part in enumerate(parts):
        out_ref[0, :, i * part.shape[1]:(i + 1) * part.shape[1]] = part


def assemble(place, layer, pairs, earlier, parts):
    rows, block = parts[0].shape
    out_width = block * len(parts)
    return pl.pallas_call(
        assemble_kernel,
        grid_spec=pltpu.PrefetchScalarGridSpec(
            num_scalar_prefetch=1,
            grid=(rows // ROW_TILE,),
            in_specs=[pl.BlockSpec((ROW_TILE, block), lambda i, p: (i, 0))] * len(parts)
            + [pl.BlockSpec(memory_space=pl.ANY)] * len(earlier),
            out_specs=pl.BlockSpec((1, ROW_TILE, out_width), lambda i, p: (layer, i, 0)),
        ),
        out_shape=jax.ShapeDtypeStruct((pairs, rows, out_width), jnp.float32),
        input_output_aliases={1 + len(parts): 0} if earlier else {},
        cost_estimate=pl.CostEstimate(flops=5_000_000_000, bytes_accessed=0, transcendentals=0),
        name="assemble",
    )(place, *parts, *earlier)


def solution(mesh):
    row_spec = P(AXES)
    weight_spec = P(None, AXES)
    chips = mesh.shape["sub"]

    def body(x_loc, w_q, w_k, w_v, w_o, w_up, w_down, grad_out):
        core = lax.axis_index("fsdp")
        chip = lax.axis_index("sub")
        pairs, shard, heads, head = w_q.shape
        seqs, seq, width = x_loc.shape
        q_width = heads // CORES * head
        block = w_down.shape[1]

        def attn_piece(layer):
            halves = []
            for part in range(CORES):
                cols = [w[layer].reshape(shard, CORES, -1)[:, part] for w in (w_q, w_k, w_v, w_o)]
                halves.append(jnp.concatenate(cols, axis=1))
            return to_columns(core, halves)

        def up_piece(layer):
            grid = w_up[layer].reshape(shard, chips, CORES, block)
            return to_columns(core, [grid[:, :, part].reshape(shard, chips * block) for part in range(CORES)])

        attn_full, up_full, down_full, up_flip = [], [], [], []
        for layer in range(pairs):
            attn_full.append(gather(attn_piece(layer)))
            up_full.append(gather(up_piece(layer)))
            down_full.append(gather(w_down[layer]))
            cols = [up_full[layer][:, i * block:(i + 1) * block] for i in range(chips)]
            up_flip.append(lax.select_n(chip, *cols).T)
        place = jnp.stack([chip, core]).astype(jnp.int32)
        carry_x = x_loc.reshape(seqs * seq, width)
        grad_x = grad_out.reshape(seqs * seq, width)
        attn_saved, mlp_saved, d_up, d_down = [], [], [], []

        def weight_grads(layer, norms, grads, d_down):
            down, parts = mlp_weight_grads(place, layer, pairs, d_down, up_flip[layer], w_down[layer], norms, grads)
            return exchange(parts), [down]

        for layer in range(pairs):
            x_own, saved = attn_forward(carry_x, attn_full[layer], q_width, head, seq)
            attn_saved.append(saved)
            n_own = norm_bf16(x_own)
            gelu_act, slope = mlp_hidden(pair_rows(n_own), up_full[layer])
            norms = all_rows(n_own)
            if layer == pairs - 1:
                parts, d_down = weight_grads(layer, norms, all_rows(grad_x), d_down)
            mlp_saved.append((x_own, norms, slope))
            if layer < pairs - 1:
                carry_x = mlp_output(x_own, gelu_act, down_full[layer])
        last = (x_own, gelu_act, down_full[-1])
        grad_lists = ([], [], [], [])
        for layer in reversed(range(pairs)):
            x_own, norms, slope = mlp_saved[layer]
            if layer < pairs - 1:
                parts, d_down = weight_grads(layer, norms, all_rows(grad_x), d_down)
            d_up = [assemble(place, layer, pairs, d_up, parts)]
            grad_x = mlp_backward(x_own, slope, up_full[layer], down_full[layer], grad_x)
            grad_x, d_qkv, d_o = attn_backward(attn_saved[layer], attn_full[layer], q_width, head, seq, grad_x)
            parts = to_rows(core, scatter_sum(d_o))
            grad_lists[3].append(jnp.concatenate(parts, axis=1).reshape(shard, heads, head))
            parts = to_rows(core, scatter_sum(d_qkv))
            grad_lists[0].append(jnp.concatenate([part[:, :q_width] for part in parts], axis=1)
                                 .reshape(shard, heads, head))
            grad_lists[1].append(jnp.stack([part[:, q_width:q_width + head] for part in parts], axis=1))
            grad_lists[2].append(jnp.stack([part[:, q_width + head:] for part in parts], axis=1))
        last, d_down = lax.optimization_barrier((last, d_down))
        y_loc = mlp_output(*last).reshape(x_loc.shape)
        stacked = tuple(jnp.stack(grad_list[::-1]) for grad_list in grad_lists)
        return (y_loc, grad_x.reshape(x_loc.shape)) + stacked + (d_up[0], d_down[0])

    return jax.shard_map(body, mesh=mesh, in_specs=(row_spec,) + (weight_spec,) * 6 + (row_spec,),
                         out_specs=(row_spec, row_spec) + (weight_spec,) * 6, check_vma=False)
```

```python
import functools

import jax
import jax.numpy as jnp
from jax import lax
from jax.experimental import pallas as pl
from jax.experimental.pallas import tpu as pltpu
from jax.sharding import PartitionSpec as P


CHIP, CORE = AXES = ("sub", "fsdp")
EPS = 1e-6
MASK_FILL = -1e30
GELU_A = (2.0 / 3.141592653589793) ** 0.5
GELU_B = 0.044715
CHIPS = 4
CORES = 2
QUERY_BLOCK = 256
TOKEN_TILE = 512
ROW_TILE = 48
NEIGHBOURS = (1, 2)


def rms_norm(values):
    return values * lax.rsqrt(jnp.mean(values * values, axis=-1, keepdims=True) + EPS)


def norm_bf16(x_loc):
    return rms_norm(x_loc.astype(jnp.float32)).astype(jnp.bfloat16)


def norm_back(x_loc, grad_norm):
    _, pull_back = jax.vjp(rms_norm, x_loc.astype(jnp.float32))
    return pull_back(grad_norm)[0]


def dot(left, right, contract):
    return lax.dot_general(left, right, (contract, ((), ())), preferred_element_type=jnp.float32)


def times(left, right):
    return dot(left, right, ((1,), (0,)))


def times_flipped(left, right):
    return dot(left, right, ((1,), (1,)))


def over_rows(left, right):
    return dot(left, right, ((0,), (0,)))


def swap(value):
    return lax.ppermute(value, CORE, [(0, 1), (1, 0)])


def hop(value, step):
    return lax.ppermute(value, CHIP, [(chip, chip ^ step) for chip in range(CHIPS)])


def by_core(core, mine, other):
    return jnp.where(core == 0, mine, other), jnp.where(core == 0, other, mine)


def to_columns(core, halves):
    keep = jnp.where(core == 0, halves[0], halves[1])
    send = jnp.where(core == 0, halves[1], halves[0])
    first, second = by_core(core, keep, swap(send))
    return jnp.concatenate([first, second], axis=0)


def to_rows(core, grad):
    rows = grad.shape[0] // CORES
    grad = grad.reshape((CORES, rows) + grad.shape[1:])
    keep = lax.dynamic_index_in_dim(grad, core, 0, keepdims=False)
    send = lax.dynamic_index_in_dim(grad, 1 - core, 0, keepdims=False)
    return by_core(core, keep, swap(send))


def blank_kernel(_, out_ref):
    del out_ref


def blank(piece):
    anywhere = pl.BlockSpec(memory_space=pl.ANY)
    return pl.pallas_call(blank_kernel, in_specs=[anywhere], out_specs=anywhere, name="blank",
                          out_shape=jax.ShapeDtypeStruct((CHIPS,) + piece.shape, piece.dtype))(piece)


def gather_weight(chip, piece):
    half = piece.shape[0] // 2
    near = [hop(piece, step) for step in NEIGHBOURS]
    opposite = [hop(near[0][:half], NEIGHBOURS[1]),
                hop(near[1][half:], NEIGHBOURS[0])]
    full = blank(piece)
    parts = [(piece, 0, 0), (near[0], NEIGHBOURS[0], 0), (near[1], NEIGHBOURS[1], 0),
             (opposite[0], sum(NEIGHBOURS), 0), (opposite[1], sum(NEIGHBOURS), half)]
    for part, step, row in parts:
        full = lax.dynamic_update_slice(full, part[None], (chip ^ step, row, 0))
    return full.reshape(-1, piece.shape[1])


def gather(value):
    return functools.partial(lax.all_gather, axis=0, tiled=True)(value, CHIP)


def gather_rows(value):
    mine = gather(value)
    return mine, swap(mine)


def scatter_sum(grad_full):
    return lax.psum_scatter(grad_full, CHIP, scatter_dimension=0, tiled=True)


def both_halves(left, right, rows, product):
    other = swap(product(left[rows:], right))
    own = lax.optimization_barrier(product(left[:rows], right))
    return own + other


def pair_rows(value):
    return jnp.concatenate([value, swap(value)], axis=0)


def causal_blocks(seq):
    return [(start, start + QUERY_BLOCK) for start in range(0, seq, QUERY_BLOCK)]


def probabilities(k_blk, q_blk, scale):
    scores = dot(k_blk, q_blk, ((1,), (1,))) * scale
    keys, queries = scores.shape
    key = lax.broadcasted_iota(jnp.int32, (queries, queries), 0)
    query = lax.broadcasted_iota(jnp.int32, (queries, queries), 1)
    last = jnp.where(key <= query, scores[keys - queries:], MASK_FILL)
    scores = last if keys == queries else jnp.concatenate([scores[:keys - queries], last], axis=0)
    powers = jnp.exp(scores - jnp.max(scores, axis=0, keepdims=True))
    return powers * (1.0 / jnp.sum(powers, axis=0, keepdims=True))


def attn_fwd_kernel(q_width, head, qkv_ref, o_ref):
    seq = qkv_ref.shape[0]
    k_all = qkv_ref[:, q_width:q_width + head]
    v_flip = jnp.transpose(qkv_ref[:, q_width + head:].astype(jnp.float32)).astype(jnp.bfloat16)
    for col in range(0, q_width, head):
        for start, end in causal_blocks(seq):
            probs = probabilities(k_all[:end], qkv_ref[start:end, col:col + head], head ** -0.5)
            o_flip = dot(v_flip[:, :end], probs.astype(jnp.bfloat16), ((1,), (0,)))
            o_ref[start:end, col:col + head] = jnp.transpose(o_flip).astype(jnp.bfloat16)


def attn_bwd_kernel(q_width, head, qkv_ref, d_o_ref, out_ref, d_k_ref, d_v_ref):
    seq = qkv_ref.shape[0]
    scale = head ** -0.5
    k_all = qkv_ref[:, q_width:q_width + head]
    v_all = qkv_ref[:, q_width + head:]
    k_flip = jnp.transpose(k_all.astype(jnp.float32)).astype(jnp.bfloat16)
    d_k_ref[...] = jnp.zeros_like(d_k_ref)
    d_v_ref[...] = jnp.zeros_like(d_v_ref)
    for col in range(0, q_width, head):
        for start, end in causal_blocks(seq):
            q_blk = qkv_ref[start:end, col:col + head]
            d_o_blk = d_o_ref[start:end, col:col + head]
            probs = probabilities(k_all[:end], q_blk, scale)
            d_p = dot(v_all[:end], d_o_blk, ((1,), (1,)))
            d_v_ref[:end] += dot(probs.astype(jnp.bfloat16), d_o_blk, ((1,), (0,)))
            d_s = probs * (d_p - jnp.sum(probs * d_p, axis=0, keepdims=True))
            d_s = (d_s * scale).astype(jnp.bfloat16)
            d_k_ref[:end] += dot(d_s, q_blk, ((1,), (0,)))
            d_q_flip = dot(k_flip[:, :end], d_s, ((1,), (0,)))
            out_ref[start:end, col:col + head] = jnp.transpose(d_q_flip).astype(jnp.bfloat16)
    out_ref[:, q_width:q_width + head] = d_k_ref[...].astype(jnp.bfloat16)
    out_ref[:, q_width + head:] = d_v_ref[...].astype(jnp.bfloat16)


def by_sequence(kernel, seq, q_width, head, args, width, scratch, flops):
    rows = args[0].shape[0]
    return pl.pallas_call(
        functools.partial(kernel, q_width, head),
        grid=(rows // seq,),
        in_specs=[pl.BlockSpec((seq, arg.shape[1]), lambda i: (i, 0)) for arg in args],
        out_specs=pl.BlockSpec((seq, width), lambda i: (i, 0)),
        out_shape=jax.ShapeDtypeStruct((rows, width), jnp.bfloat16),
        scratch_shapes=[pltpu.VMEM((seq, head), jnp.float32)] * scratch,
        cost_estimate=pl.CostEstimate(flops=flops, bytes_accessed=0, transcendentals=0),
    )(*args)


def attn_forward(x_own, weight, q_width, head, seq):
    normed = pair_rows(norm_bf16(x_own))
    qkv = times(normed, weight[:, :q_width + 2 * head]).astype(jnp.bfloat16)
    o_act = by_sequence(attn_fwd_kernel, seq, q_width, head, (qkv,), q_width, 0,
                  20_000_000_000)
    proj = both_halves(o_act, weight[:, q_width + 2 * head:], x_own.shape[0], times_flipped)
    y_own = (x_own.astype(jnp.float32) + proj).astype(jnp.bfloat16)
    return y_own, (x_own, normed, qkv, o_act)


def attn_backward(saved, weight, q_width, head, seq, grad_own):
    x_own, normed, qkv, o_act = saved
    grad_y = pair_rows(grad_own)
    d_o = times(grad_y, weight[:, q_width + 2 * head:]).astype(jnp.bfloat16)
    d_qkv = by_sequence(attn_bwd_kernel, seq, q_width, head, (qkv, d_o), qkv.shape[1], 2,
                  40_000_000_000)
    d_norm = both_halves(d_qkv, weight[:, :q_width + 2 * head], grad_own.shape[0], times_flipped)
    grad_x = (grad_own.astype(jnp.float32) + norm_back(x_own, d_norm)).astype(jnp.bfloat16)
    return grad_x, over_rows(normed, d_qkv), over_rows(grad_y, o_act)


def gelu_parts(hidden):
    square = hidden * hidden
    half = 0.5 + 0.5 * jnp.tanh(hidden * (GELU_A + GELU_A * GELU_B * square))
    value = hidden * half
    slope = half + value * (1.0 - half) * (2.0 * GELU_A + 6.0 * GELU_A * GELU_B * square)
    return value.astype(jnp.bfloat16), slope


def mlp_hidden(normed, up_weight):
    return lax.optimization_barrier(gelu_parts(times(normed, up_weight)))


def mlp_output(x_own, gelu_act, down_weight):
    proj = both_halves(gelu_act, down_weight, x_own.shape[0], times)
    return (x_own.astype(jnp.float32) + proj).astype(jnp.bfloat16)


def mlp_backward(x_own, slope, up_weight, down_weight, grad_own):
    grad_act = times_flipped(pair_rows(grad_own), down_weight)
    d_hid = (grad_act * slope).astype(jnp.bfloat16)
    d_norm = both_halves(d_hid, up_weight, grad_own.shape[0], times_flipped)
    return (grad_own.astype(jnp.float32) + norm_back(x_own, d_norm)).astype(jnp.bfloat16)


def mlp_grads_kernel(half, place_ref, up_ref, down_ref, n0_ref, n1_ref, g0_ref, g1_ref, *rest):
    d_down_ref, parts, d_up_ref, flip_ref = rest[-2 * CHIPS - 3], rest[-2 * CHIPS - 2:-2], rest[-2], rest[-1]
    step = pl.program_id(0)
    normed = jnp.where(step < half, n0_ref[...], n1_ref[...])
    grad_y = jnp.where(step < half, g0_ref[...], g1_ref[...])

    @pl.when(step == 0)
    def _():
        d_down_ref[...] = jnp.zeros_like(d_down_ref)
        d_up_ref[...] = jnp.zeros_like(d_up_ref)

    gelu_act, slope = gelu_parts(dot(up_ref[...], normed, ((1,), (1,))))
    d_hid = (dot(down_ref[...], grad_y, ((1,), (1,))) * slope).astype(jnp.bfloat16)
    d_down_ref[0] += dot(gelu_act, grad_y, ((1,), (0,)))
    d_up_ref[...] += dot(d_hid, normed, ((1,), (0,)))

    @pl.when(step == pl.num_programs(0) - 1)
    def _():
        rows = parts[0].shape[0]
        for i in range(CHIPS):
            start = pl.multiple_of((place_ref[0] ^ i) * (CORES * rows), CORES * rows)
            flip_ref[...] = jnp.transpose(d_up_ref[:, pl.ds(start, CORES * rows)])
            for j in range(CORES):
                start = pl.multiple_of((place_ref[1] ^ j) * rows, rows)
                parts[CORES * i + j][...] = flip_ref[pl.ds(start, rows), :]


def mlp_weight_grads(place, layer, pairs, earlier, up_flip, down_block, norms, grads):
    block, width = down_block.shape
    half = norms[0].shape[0] // TOKEN_TILE
    rows = width // (CHIPS * CORES)
    once = pl.Buffered(1)
    whole = pl.BlockSpec((block, width), lambda i, p: (0, 0), pipeline_mode=once)
    mine = pl.BlockSpec((TOKEN_TILE, width), lambda i, p: (jnp.minimum(i, half - 1), 0))
    others = pl.BlockSpec((TOKEN_TILE, width), lambda i, p: (jnp.maximum(i - half, 0), 0))
    part = pl.BlockSpec((rows, block), lambda i, p: (0, 0), pipeline_mode=once)
    args = [place, up_flip, down_block, norms[0], norms[1], grads[0], grads[1]] + earlier
    outs = pl.pallas_call(
        functools.partial(mlp_grads_kernel, half),
        grid_spec=pltpu.PrefetchScalarGridSpec(
            num_scalar_prefetch=1,
            grid=(2 * half,),
            in_specs=[whole, whole, mine, others, mine, others] + [pl.BlockSpec(memory_space=pl.ANY)] * len(earlier),
            out_specs=[pl.BlockSpec((1, block, width), lambda i, p: (layer, 0, 0), pipeline_mode=once)]
            + [part] * (CHIPS * CORES),
            scratch_shapes=[pltpu.VMEM((block, width), jnp.float32), pltpu.VMEM((CORES * rows, block), jnp.float32)],
        ),
        out_shape=[jax.ShapeDtypeStruct((pairs, block, width), jnp.float32)]
        + [jax.ShapeDtypeStruct((rows, block), jnp.float32)] * (CHIPS * CORES),
        input_output_aliases={7: 0} if earlier else {},
        compiler_params=pltpu.CompilerParams(vmem_limit_bytes=60 * 1024 * 1024),
        cost_estimate=pl.CostEstimate(flops=8 * 2 * norms[0].shape[0] * block * width, bytes_accessed=0,
                                      transcendentals=0),
        name="mlp_grads",
    )(*args)
    return outs[0], outs[1:]


def exchange(parts):
    devices = range(CHIPS * CORES)
    return [lax.ppermute(part, AXES, [(d, d ^ i) for d in devices]) if i else part for i, part in enumerate(parts)]


def assemble_kernel(place_ref, *refs):
    parts, out_ref = [ref[...] for ref in refs[:CHIPS * CORES]], refs[-1]
    for bit in range(3):
        swapped = ((place_ref[0] * CORES + place_ref[1]) >> bit) % 2 == 1
        parts = [jnp.where(swapped, parts[i ^ (1 << bit)], part) for i, part in enumerate(parts)]
    for i, part in enumerate(parts):
        out_ref[0, :, i * part.shape[1]:(i + 1) * part.shape[1]] = part


def assemble(place, layer, pairs, earlier, parts):
    rows, block = parts[0].shape
    out_width = block * len(parts)
    return pl.pallas_call(
        assemble_kernel,
        grid_spec=pltpu.PrefetchScalarGridSpec(
            num_scalar_prefetch=1,
            grid=(rows // ROW_TILE,),
            in_specs=[pl.BlockSpec((ROW_TILE, block), lambda i, p: (i, 0))] * len(parts)
            + [pl.BlockSpec(memory_space=pl.ANY)] * len(earlier),
            out_specs=pl.BlockSpec((1, ROW_TILE, out_width), lambda i, p: (layer, i, 0)),
        ),
        out_shape=jax.ShapeDtypeStruct((pairs, rows, out_width), jnp.float32),
        input_output_aliases={1 + len(parts): 0} if earlier else {},
        cost_estimate=pl.CostEstimate(flops=5_000_000_000, bytes_accessed=0, transcendentals=0),
        name="assemble",
    )(place, *parts, *earlier)


def solution(mesh):
    row_spec = P(AXES)
    weight_spec = P(None, AXES)
    chips = mesh.shape[CHIP]

    def body(x_loc, w_q, w_k, w_v, w_o, w_up, w_down, grad_out):
        core = lax.axis_index(CORE)
        chip = lax.axis_index(CHIP)
        pairs, shard, heads, head = w_q.shape
        seqs, seq, width = x_loc.shape
        q_width = heads // CORES * head
        block = w_down.shape[1]

        def attn_piece(layer):
            halves = []
            for part in range(CORES):
                cols = [w[layer].reshape(shard, CORES, -1)[:, part] for w in (w_q, w_k, w_v, w_o)]
                halves.append(jnp.concatenate(cols, axis=1))
            return to_columns(core, halves)

        def up_piece(layer):
            grid = w_up[layer].reshape(shard, chips, CORES, block)
            return to_columns(core, [grid[:, :, part].reshape(shard, chips * block) for part in range(CORES)])

        attn_full, up_full, down_full, up_flip = [], [], [], []
        for layer in range(pairs):
            attn_full.append(gather_weight(chip, attn_piece(layer)))
            up_full.append(gather_weight(chip, up_piece(layer)))
            down_full.append(gather_weight(chip, w_down[layer]) if layer < pairs - 1 else gather(w_down[layer]))
            cols = [up_full[layer][:, i * block:(i + 1) * block] for i in range(chips)]
            up_flip.append(lax.select_n(chip, *cols).T)
        place = jnp.stack([chip, core]).astype(jnp.int32)
        carry_x = x_loc.reshape(seqs * seq, width)
        grad_x = grad_out.reshape(seqs * seq, width)
        attn_saved, mlp_saved, d_up, d_down = [], [], [], []

        def weight_grads(layer, norms, grads, d_down):
            down, parts = mlp_weight_grads(place, layer, pairs, d_down, up_flip[layer], w_down[layer], norms, grads)
            return exchange(parts), [down]

        for layer in range(pairs):
            x_own, saved = attn_forward(carry_x, attn_full[layer], q_width, head, seq)
            attn_saved.append(saved)
            n_own = norm_bf16(x_own)
            gelu_act, slope = mlp_hidden(pair_rows(n_own), up_full[layer])
            norms = gather_rows(n_own)
            if layer == pairs - 1:
                parts, d_down = weight_grads(layer, norms, gather_rows(grad_x), d_down)
            mlp_saved.append((x_own, norms, slope))
            if layer < pairs - 1:
                carry_x = mlp_output(x_own, gelu_act, down_full[layer])
        last = (x_own, gelu_act, down_full[-1])
        grad_lists = ([], [], [], [])
        for layer in reversed(range(pairs)):
            x_own, norms, slope = mlp_saved[layer]
            if layer < pairs - 1:
                parts, d_down = weight_grads(layer, norms, gather_rows(grad_x), d_down)
            d_up = [assemble(place, layer, pairs, d_up, parts)]
            grad_x = mlp_backward(x_own, slope, up_full[layer], down_full[layer], grad_x)
            grad_x, d_qkv, d_o = attn_backward(attn_saved[layer], attn_full[layer], q_width, head, seq, grad_x)
            parts = to_rows(core, scatter_sum(d_o))
            grad_lists[3].append(jnp.concatenate(parts, axis=1).reshape(shard, heads, head))
            parts = to_rows(core, scatter_sum(d_qkv))
            grad_lists[0].append(jnp.concatenate([part[:, :q_width] for part in parts], axis=1)
                                 .reshape(shard, heads, head))
            grad_lists[1].append(jnp.stack([part[:, q_width:q_width + head] for part in parts], axis=1))
            grad_lists[2].append(jnp.stack([part[:, q_width + head:] for part in parts], axis=1))
        last, d_down = lax.optimization_barrier((last, d_down))
        y_loc = mlp_output(*last).reshape(x_loc.shape)
        stacked = tuple(jnp.stack(grad_list[::-1]) for grad_list in grad_lists)
        return (y_loc, grad_x.reshape(x_loc.shape)) + stacked + (d_up[0], d_down[0])

    return jax.shard_map(body, mesh=mesh, in_specs=(row_spec,) + (weight_spec,) * 6 + (row_spec,),
                         out_specs=(row_spec, row_spec) + (weight_spec,) * 6, check_vma=False)
```

```python
import functools

import jax
import jax.numpy as jnp
from jax import lax
from jax.experimental import pallas as pl
from jax.experimental.pallas import tpu as pltpu
from jax.sharding import PartitionSpec as P


CHIP, CORE = AXES = ("sub", "fsdp")
EPS = 1e-6
MASK_FILL = -1e30
GELU_A = (2.0 / 3.141592653589793) ** 0.5
GELU_B = 0.044715
CHIPS = 4
CORES = 2
QUERY_BLOCK = 256
TOKEN_TILE = 512
ROW_TILE = 48
FLIP_TILE = 256
NEIGHBOURS = (1, 2)


def rms_norm(values):
    return values * lax.rsqrt(jnp.mean(values * values, axis=-1, keepdims=True) + EPS)


def norm_bf16(x_loc):
    return rms_norm(x_loc.astype(jnp.float32)).astype(jnp.bfloat16)


def norm_back(x_loc, grad_norm):
    _, pull_back = jax.vjp(rms_norm, x_loc.astype(jnp.float32))
    return pull_back(grad_norm)[0]


def dot(left, right, contract):
    return lax.dot_general(left, right, (contract, ((), ())), preferred_element_type=jnp.float32)


def times(left, right):
    return dot(left, right, ((1,), (0,)))


def times_flipped(left, right):
    return dot(left, right, ((1,), (1,)))


def over_rows(left, right):
    return dot(left, right, ((0,), (0,)))


def swap(value):
    return lax.ppermute(value, CORE, [(0, 1), (1, 0)])


def hop(value, step):
    return lax.ppermute(value, CHIP, [(chip, chip ^ step) for chip in range(CHIPS)])


def by_core(core, mine, other):
    return jnp.where(core == 0, mine, other), jnp.where(core == 0, other, mine)


def to_columns(core, halves):
    keep = jnp.where(core == 0, halves[0], halves[1])
    send = jnp.where(core == 0, halves[1], halves[0])
    first, second = by_core(core, keep, swap(send))
    return jnp.concatenate([first, second], axis=0)


def to_rows(core, grad):
    rows = grad.shape[0] // CORES
    grad = grad.reshape((CORES, rows) + grad.shape[1:])
    keep = lax.dynamic_index_in_dim(grad, core, 0, keepdims=False)
    send = lax.dynamic_index_in_dim(grad, 1 - core, 0, keepdims=False)
    return by_core(core, keep, swap(send))


def blank_kernel(_, out_ref):
    del out_ref


def blank(piece):
    anywhere = pl.BlockSpec(memory_space=pl.ANY)
    return pl.pallas_call(blank_kernel, in_specs=[anywhere], out_specs=anywhere, name="blank",
                          out_shape=jax.ShapeDtypeStruct((CHIPS,) + piece.shape, piece.dtype))(piece)


def gather_weight(chip, piece):
    half = piece.shape[0] // 2
    near = [hop(piece, step) for step in NEIGHBOURS]
    opposite = [hop(near[0][:half], NEIGHBOURS[1]),
                hop(near[1][half:], NEIGHBOURS[0])]
    full = blank(piece)
    parts = [(piece, 0, 0), (near[0], NEIGHBOURS[0], 0), (near[1], NEIGHBOURS[1], 0),
             (opposite[0], sum(NEIGHBOURS), 0), (opposite[1], sum(NEIGHBOURS), half)]
    for part, step, row in parts:
        full = lax.dynamic_update_slice(full, part[None], (chip ^ step, row, 0))
    return full.reshape(-1, piece.shape[1])


def gather(value, axes):
    return functools.partial(lax.all_gather, axis=0, tiled=True)(value, axes)


def gather_rows(value, swapped):
    if not swapped:
        return (gather(value, AXES),)
    mine = gather(value, CHIP)
    return mine, swap(mine)


def scatter_sum(grad_full):
    return lax.psum_scatter(grad_full, CHIP, scatter_dimension=0, tiled=True)


def both_halves(left, right, rows, product):
    other = swap(product(left[rows:], right))
    own = lax.optimization_barrier(product(left[:rows], right))
    return own + other


def pair_rows(value):
    return jnp.concatenate([value, swap(value)], axis=0)


def causal_blocks(seq):
    return [(start, start + QUERY_BLOCK) for start in range(0, seq, QUERY_BLOCK)]


def probabilities(k_blk, q_blk, scale):
    scores = dot(k_blk, q_blk, ((1,), (1,))) * scale
    keys, queries = scores.shape
    key = lax.broadcasted_iota(jnp.int32, (queries, queries), 0)
    query = lax.broadcasted_iota(jnp.int32, (queries, queries), 1)
    last = jnp.where(key <= query, scores[keys - queries:], MASK_FILL)
    scores = last if keys == queries else jnp.concatenate([scores[:keys - queries], last], axis=0)
    powers = jnp.exp(scores - jnp.max(scores, axis=0, keepdims=True))
    return powers * (1.0 / jnp.sum(powers, axis=0, keepdims=True))


def attn_fwd_kernel(q_width, head, qkv_ref, o_ref):
    seq = qkv_ref.shape[0]
    k_all = qkv_ref[:, q_width:q_width + head]
    v_flip = jnp.transpose(qkv_ref[:, q_width + head:].astype(jnp.float32)).astype(jnp.bfloat16)
    for col in range(0, q_width, head):
        for start, end in causal_blocks(seq):
            probs = probabilities(k_all[:end], qkv_ref[start:end, col:col + head], head ** -0.5)
            o_flip = dot(v_flip[:, :end], probs.astype(jnp.bfloat16), ((1,), (0,)))
            o_ref[start:end, col:col + head] = jnp.transpose(o_flip).astype(jnp.bfloat16)


def attn_bwd_kernel(q_width, head, qkv_ref, d_o_ref, out_ref, d_k_ref, d_v_ref):
    seq = qkv_ref.shape[0]
    scale = head ** -0.5
    k_all = qkv_ref[:, q_width:q_width + head]
    v_all = qkv_ref[:, q_width + head:]
    k_flip = jnp.transpose(k_all.astype(jnp.float32)).astype(jnp.bfloat16)
    d_k_ref[...] = jnp.zeros_like(d_k_ref)
    d_v_ref[...] = jnp.zeros_like(d_v_ref)
    for col in range(0, q_width, head):
        for start, end in causal_blocks(seq):
            q_blk = qkv_ref[start:end, col:col + head]
            d_o_blk = d_o_ref[start:end, col:col + head]
            probs = probabilities(k_all[:end], q_blk, scale)
            d_p = dot(v_all[:end], d_o_blk, ((1,), (1,)))
            d_v_ref[:end] += dot(probs.astype(jnp.bfloat16), d_o_blk, ((1,), (0,)))
            d_s = probs * (d_p - jnp.sum(probs * d_p, axis=0, keepdims=True))
            d_s = (d_s * scale).astype(jnp.bfloat16)
            d_k_ref[:end] += dot(d_s, q_blk, ((1,), (0,)))
            d_q_flip = dot(k_flip[:, :end], d_s, ((1,), (0,)))
            out_ref[start:end, col:col + head] = jnp.transpose(d_q_flip).astype(jnp.bfloat16)
    out_ref[:, q_width:q_width + head] = d_k_ref[...].astype(jnp.bfloat16)
    out_ref[:, q_width + head:] = d_v_ref[...].astype(jnp.bfloat16)


def by_sequence(kernel, seq, q_width, head, args, width, scratch, flops):
    rows = args[0].shape[0]
    return pl.pallas_call(
        functools.partial(kernel, q_width, head),
        grid=(rows // seq,),
        in_specs=[pl.BlockSpec((seq, arg.shape[1]), lambda i: (i, 0)) for arg in args],
        out_specs=pl.BlockSpec((seq, width), lambda i: (i, 0)),
        out_shape=jax.ShapeDtypeStruct((rows, width), jnp.bfloat16),
        scratch_shapes=[pltpu.VMEM((seq, head), jnp.float32)] * scratch,
        cost_estimate=pl.CostEstimate(flops=flops, bytes_accessed=0, transcendentals=0),
    )(*args)


def attn_forward(x_own, weight, q_width, head, seq):
    normed = pair_rows(norm_bf16(x_own))
    qkv = times(normed, weight[:, :q_width + 2 * head]).astype(jnp.bfloat16)
    o_act = by_sequence(attn_fwd_kernel, seq, q_width, head, (qkv,), q_width, 0,
                  20_000_000_000)
    proj = both_halves(o_act, weight[:, q_width + 2 * head:], x_own.shape[0], times_flipped)
    y_own = (x_own.astype(jnp.float32) + proj).astype(jnp.bfloat16)
    return y_own, (x_own, normed, qkv, o_act)


def attn_backward(saved, weight, q_width, head, seq, grad_own):
    x_own, normed, qkv, o_act = saved
    grad_y = pair_rows(grad_own)
    d_o = times(grad_y, weight[:, q_width + 2 * head:]).astype(jnp.bfloat16)
    d_qkv = by_sequence(attn_bwd_kernel, seq, q_width, head, (qkv, d_o), qkv.shape[1], 2,
                  40_000_000_000)
    d_norm = both_halves(d_qkv, weight[:, :q_width + 2 * head], grad_own.shape[0], times_flipped)
    grad_x = (grad_own.astype(jnp.float32) + norm_back(x_own, d_norm)).astype(jnp.bfloat16)
    return grad_x, over_rows(normed, d_qkv), over_rows(grad_y, o_act)


def gelu_parts(hidden):
    square = hidden * hidden
    half = 0.5 + 0.5 * jnp.tanh(hidden * (GELU_A + GELU_A * GELU_B * square))
    value = hidden * half
    slope = half + value * (1.0 - half) * (2.0 * GELU_A + 6.0 * GELU_A * GELU_B * square)
    return value.astype(jnp.bfloat16), slope


def mlp_hidden(normed, up_weight):
    return lax.optimization_barrier(gelu_parts(times(normed, up_weight)))


def mlp_output(x_own, gelu_act, down_weight):
    proj = both_halves(gelu_act, down_weight, x_own.shape[0], times)
    return (x_own.astype(jnp.float32) + proj).astype(jnp.bfloat16)


def mlp_backward(x_own, slope, up_weight, down_weight, grad_own):
    grad_act = times_flipped(pair_rows(grad_own), down_weight)
    d_hid = (grad_act * slope).astype(jnp.bfloat16)
    d_norm = both_halves(d_hid, up_weight, grad_own.shape[0], times_flipped)
    return (grad_own.astype(jnp.float32) + norm_back(x_own, d_norm)).astype(jnp.bfloat16)


def mlp_grads_kernel(steps, arrays, place_ref, up_ref, down_ref, *rest):
    norms, grads = rest[:arrays], rest[arrays:2 * arrays]
    d_down_ref, parts, d_up_ref, flip_ref = rest[-2 * CHIPS - 3], rest[-2 * CHIPS - 2:-2], rest[-2], rest[-1]
    step = pl.program_id(0)
    normed, grad_y = norms[0][...], grads[0][...]
    if arrays > 1:
        normed = jnp.where(step < steps, normed, norms[1][...])
        grad_y = jnp.where(step < steps, grad_y, grads[1][...])

    @pl.when(step == 0)
    def _():
        d_down_ref[...] = jnp.zeros_like(d_down_ref)
        d_up_ref[...] = jnp.zeros_like(d_up_ref)

    gelu_act, slope = gelu_parts(dot(up_ref[...], normed, ((1,), (1,))))
    d_hid = (dot(down_ref[...], grad_y, ((1,), (1,))) * slope).astype(jnp.bfloat16)
    d_down_ref[0] += dot(gelu_act, grad_y, ((1,), (0,)))
    d_up_ref[...] += dot(d_hid, normed, ((1,), (0,)))

    @pl.when(step == pl.num_programs(0) - 1)
    def _():
        rows = parts[0].shape[0]
        for i in range(CHIPS):
            start = pl.multiple_of((place_ref[0] ^ i) * (CORES * rows), CORES * rows)
            flip_ref[...] = jnp.transpose(d_up_ref[:, pl.ds(start, CORES * rows)])
            for j in range(CORES):
                start = pl.multiple_of((place_ref[1] ^ j) * rows, rows)
                parts[CORES * i + j][...] = flip_ref[pl.ds(start, rows), :]


def mlp_weight_grads(place, layer, pairs, earlier, up_flip, down_block, norms, grads):
    block, width = down_block.shape
    steps = norms[0].shape[0] // TOKEN_TILE
    rows = width // (CHIPS * CORES)
    once = pl.Buffered(1)
    whole = pl.BlockSpec((block, width), lambda i, p: (0, 0), pipeline_mode=once)
    tokens = [pl.BlockSpec((TOKEN_TILE, width), lambda i, p: (jnp.minimum(i, steps - 1), 0)),
              pl.BlockSpec((TOKEN_TILE, width), lambda i, p: (jnp.maximum(i - steps, 0), 0))][:len(norms)]
    part = pl.BlockSpec((rows, block), lambda i, p: (0, 0), pipeline_mode=once)
    args = [place, up_flip, down_block, *norms, *grads, *earlier]
    outs = pl.pallas_call(
        functools.partial(mlp_grads_kernel, steps, len(norms)),
        grid_spec=pltpu.PrefetchScalarGridSpec(
            num_scalar_prefetch=1,
            grid=(steps * len(norms),),
            in_specs=[whole, whole] + tokens * 2 + [pl.BlockSpec(memory_space=pl.ANY)] * len(earlier),
            out_specs=[pl.BlockSpec((1, block, width), lambda i, p: (layer, 0, 0), pipeline_mode=once)]
            + [part] * (CHIPS * CORES),
            scratch_shapes=[pltpu.VMEM((block, width), jnp.float32), pltpu.VMEM((CORES * rows, block), jnp.float32)],
        ),
        out_shape=[jax.ShapeDtypeStruct((pairs, block, width), jnp.float32)]
        + [jax.ShapeDtypeStruct((rows, block), jnp.float32)] * (CHIPS * CORES),
        input_output_aliases={len(args) - 1: 0} if earlier else {},
        compiler_params=pltpu.CompilerParams(vmem_limit_bytes=60 * 1024 * 1024),
        cost_estimate=pl.CostEstimate(flops=8 * len(norms) * norms[0].shape[0] * block * width, bytes_accessed=0,
                                      transcendentals=0),
        name="mlp_grads",
    )(*args)
    return outs[0], outs[1:]


def exchange(parts):
    devices = range(CHIPS * CORES)
    return [lax.ppermute(part, AXES, [(d, d ^ i) for d in devices]) if i else part for i, part in enumerate(parts)]


def assemble_kernel(place_ref, *refs):
    parts, out_ref = [ref[...] for ref in refs[:CHIPS * CORES]], refs[-1]
    for bit in range(3):
        swapped = ((place_ref[0] * CORES + place_ref[1]) >> bit) % 2 == 1
        parts = [jnp.where(swapped, parts[i ^ (1 << bit)], part) for i, part in enumerate(parts)]
    for i, part in enumerate(parts):
        out_ref[0, :, i * part.shape[1]:(i + 1) * part.shape[1]] = part


def assemble(place, layer, pairs, earlier, parts):
    rows, block = parts[0].shape
    out_width = block * len(parts)
    return pl.pallas_call(
        assemble_kernel,
        grid_spec=pltpu.PrefetchScalarGridSpec(
            num_scalar_prefetch=1,
            grid=(rows // ROW_TILE,),
            in_specs=[pl.BlockSpec((ROW_TILE, block), lambda i, p: (i, 0))] * len(parts)
            + [pl.BlockSpec(memory_space=pl.ANY)] * len(earlier),
            out_specs=pl.BlockSpec((1, ROW_TILE, out_width), lambda i, p: (layer, i, 0)),
        ),
        out_shape=jax.ShapeDtypeStruct((pairs, rows, out_width), jnp.float32),
        input_output_aliases={1 + len(parts): 0} if earlier else {},
        cost_estimate=pl.CostEstimate(flops=5_000_000_000, bytes_accessed=0, transcendentals=0),
        name="assemble",
    )(place, *parts, *earlier)


def flip_kernel(place_ref, up_ref, out_ref):
    block = out_ref.shape[0]
    cols = up_ref[:, :block]
    for i in range(1, CHIPS):
        cols = jnp.where(place_ref[0] == i, up_ref[:, i * block:(i + 1) * block], cols)
    out_ref[...] = jnp.transpose(cols.astype(jnp.float32)).astype(jnp.bfloat16)


def flip(place, up_weight):
    width, cols = up_weight.shape
    return pl.pallas_call(
        flip_kernel,
        grid_spec=pltpu.PrefetchScalarGridSpec(
            num_scalar_prefetch=1,
            grid=(width // FLIP_TILE,),
            in_specs=[pl.BlockSpec((FLIP_TILE, cols), lambda i, p: (i, 0))],
            out_specs=pl.BlockSpec((cols // CHIPS, FLIP_TILE), lambda i, p: (0, i)),
        ),
        out_shape=jax.ShapeDtypeStruct((cols // CHIPS, width), jnp.bfloat16),
        cost_estimate=pl.CostEstimate(flops=5_000_000_000, bytes_accessed=0, transcendentals=0),
        name="flip",
    )(place, up_weight)


def solution(mesh):
    row_spec = P(AXES)
    weight_spec = P(None, AXES)
    chips = mesh.shape[CHIP]

    def body(x_loc, w_q, w_k, w_v, w_o, w_up, w_down, grad_out):
        core = lax.axis_index(CORE)
        chip = lax.axis_index(CHIP)
        pairs, shard, heads, head = w_q.shape
        seqs, seq, width = x_loc.shape
        q_width = heads // CORES * head
        block = w_down.shape[1]

        def attn_piece(layer):
            halves = []
            for part in range(CORES):
                cols = [w[layer].reshape(shard, CORES, -1)[:, part] for w in (w_q, w_k, w_v, w_o)]
                halves.append(jnp.concatenate(cols, axis=1))
            return to_columns(core, halves)

        def up_piece(layer):
            grid = w_up[layer].reshape(shard, chips, CORES, block)
            return to_columns(core, [grid[:, :, part].reshape(shard, chips * block) for part in range(CORES)])

        place = jnp.stack([chip, core]).astype(jnp.int32)
        attn_full, up_full, down_full, up_flip = [], [], [], []
        for layer in range(pairs):
            attn_full.append(gather_weight(chip, attn_piece(layer)))
            up_full.append(gather_weight(chip, up_piece(layer)))
            down_full.append(gather_weight(chip, w_down[layer]))
            up_flip.append(flip(place, up_full[layer]))
        carry_x = x_loc.reshape(seqs * seq, width)
        grad_x = grad_out.reshape(seqs * seq, width)
        attn_saved, mlp_saved, d_up, d_down = [], [], [], []

        def weight_grads(layer, norms, grads, d_down):
            down, parts = mlp_weight_grads(place, layer, pairs, d_down, up_flip[layer], w_down[layer], norms, grads)
            return exchange(parts), [down]

        for layer in range(pairs):
            x_own, saved = attn_forward(carry_x, attn_full[layer], q_width, head, seq)
            attn_saved.append(saved)
            n_own = norm_bf16(x_own)
            gelu_act, slope = mlp_hidden(pair_rows(n_own), up_full[layer])
            norms = gather_rows(n_own, layer == pairs - 1)
            if layer == pairs - 1:
                parts, d_down = weight_grads(layer, norms, gather_rows(grad_x, layer == pairs - 1), d_down)
            mlp_saved.append((x_own, norms, slope))
            if layer < pairs - 1:
                carry_x = mlp_output(x_own, gelu_act, down_full[layer])
        last = (x_own, gelu_act, down_full[-1])
        grad_lists = ([], [], [], [])
        for layer in reversed(range(pairs)):
            x_own, norms, slope = mlp_saved[layer]
            if layer < pairs - 1:
                parts, d_down = weight_grads(layer, norms, gather_rows(grad_x, layer == pairs - 1), d_down)
            d_up = [assemble(place, layer, pairs, d_up, parts)]
            grad_x = mlp_backward(x_own, slope, up_full[layer], down_full[layer], grad_x)
            grad_x, d_qkv, d_o = attn_backward(attn_saved[layer], attn_full[layer], q_width, head, seq, grad_x)
            parts = to_rows(core, scatter_sum(d_o))
            grad_lists[3].append(jnp.concatenate(parts, axis=1).reshape(shard, heads, head))
            parts = to_rows(core, scatter_sum(d_qkv))
            grad_lists[0].append(jnp.concatenate([part[:, :q_width] for part in parts], axis=1)
                                 .reshape(shard, heads, head))
            grad_lists[1].append(jnp.stack([part[:, q_width:q_width + head] for part in parts], axis=1))
            grad_lists[2].append(jnp.stack([part[:, q_width + head:] for part in parts], axis=1))
        last, d_down = lax.optimization_barrier((last, d_down))
        y_loc = mlp_output(*last).reshape(x_loc.shape)
        stacked = tuple(jnp.stack(grad_list[::-1]) for grad_list in grad_lists)
        return (y_loc, grad_x.reshape(x_loc.shape)) + stacked + (d_up[0], d_down[0])

    return jax.shard_map(body, mesh=mesh, in_specs=(row_spec,) + (weight_spec,) * 6 + (row_spec,),
                         out_specs=(row_spec, row_spec) + (weight_spec,) * 6, check_vma=False)
```

```python
import functools

import jax
import jax.numpy as jnp
from jax import lax
from jax.experimental import pallas as pl
from jax.experimental.pallas import tpu as pltpu
from jax.sharding import PartitionSpec as P


CHIP, CORE = AXES = ("sub", "fsdp")
EPS = 1e-6
MASK_FILL = -1e30
GELU_A = (2.0 / 3.141592653589793) ** 0.5
GELU_B = 0.044715
CHIPS = 4
CORES = 2
QUERY_BLOCK = 256
TOKEN_TILE = 512
ROW_TILE = 48
FLIP_TILE = 256
NEIGHBOURS = (1, 2)


def rms_norm(values):
    return values * lax.rsqrt(jnp.mean(values * values, axis=-1, keepdims=True) + EPS)


def norm_bf16(x_loc):
    return rms_norm(x_loc.astype(jnp.float32)).astype(jnp.bfloat16)


def norm_back(x_loc, grad_norm):
    _, pull_back = jax.vjp(rms_norm, x_loc.astype(jnp.float32))
    return pull_back(grad_norm)[0]


def dot(left, right, contract):
    return lax.dot_general(left, right, (contract, ((), ())), preferred_element_type=jnp.float32)


def times(left, right):
    return dot(left, right, ((1,), (0,)))


def times_flipped(left, right):
    return dot(left, right, ((1,), (1,)))


def over_rows(left, right):
    return dot(left, right, ((0,), (0,)))


def swap(value):
    return lax.ppermute(value, CORE, [(0, 1), (1, 0)])


def hop(value, step):
    return lax.ppermute(value, CHIP, [(chip, chip ^ step) for chip in range(CHIPS)])


def by_core(core, mine, other):
    return jnp.where(core == 0, mine, other), jnp.where(core == 0, other, mine)


def to_columns(core, keep, send):
    first, second = by_core(core, keep, swap(send))
    return jnp.concatenate([first, second], axis=0)


def to_rows(core, grad):
    rows = grad.shape[0] // CORES
    grad = grad.reshape((CORES, rows) + grad.shape[1:])
    keep = lax.dynamic_index_in_dim(grad, core, 0, keepdims=False)
    send = lax.dynamic_index_in_dim(grad, 1 - core, 0, keepdims=False)
    return by_core(core, keep, swap(send))


def blank_kernel(_, out_ref):
    del out_ref


def blank(piece):
    anywhere = pl.BlockSpec(memory_space=pl.ANY)
    return pl.pallas_call(blank_kernel, in_specs=[anywhere], out_specs=anywhere, name="blank",
                          out_shape=jax.ShapeDtypeStruct((CHIPS,) + piece.shape, piece.dtype))(piece)


def gather_weight(chip, piece):
    half = piece.shape[0] // 2
    near = [hop(piece, step) for step in NEIGHBOURS]
    opposite = [hop(near[0][:half], NEIGHBOURS[1]),
                hop(near[1][half:], NEIGHBOURS[0])]
    full = blank(piece)
    parts = [(piece, 0, 0), (near[0], NEIGHBOURS[0], 0), (near[1], NEIGHBOURS[1], 0),
             (opposite[0], sum(NEIGHBOURS), 0), (opposite[1], sum(NEIGHBOURS), half)]
    for part, step, row in parts:
        full = lax.dynamic_update_slice(full, part[None], (chip ^ step, row, 0))
    return full.reshape(-1, piece.shape[1])


def gather_rows(value):
    return functools.partial(lax.all_gather, axis=0, tiled=True)(value, AXES)


def scatter_sum(grad_full):
    return lax.psum_scatter(grad_full, CHIP, scatter_dimension=0, tiled=True)


def both_halves(left, right, rows, product):
    other = swap(product(left[rows:], right))
    own = lax.optimization_barrier(product(left[:rows], right))
    return own + other


def pair_rows(value):
    return jnp.concatenate([value, swap(value)], axis=0)


def causal_blocks(seq):
    return [(start, start + QUERY_BLOCK) for start in range(0, seq, QUERY_BLOCK)]


def probabilities(k_blk, q_blk, scale):
    scores = dot(k_blk, q_blk, ((1,), (1,))) * scale
    keys, queries = scores.shape
    key = lax.broadcasted_iota(jnp.int32, (queries, queries), 0)
    query = lax.broadcasted_iota(jnp.int32, (queries, queries), 1)
    last = jnp.where(key <= query, scores[keys - queries:], MASK_FILL)
    scores = last if keys == queries else jnp.concatenate([scores[:keys - queries], last], axis=0)
    powers = jnp.exp(scores - jnp.max(scores, axis=0, keepdims=True))
    return powers * (1.0 / jnp.sum(powers, axis=0, keepdims=True))


def attn_fwd_kernel(q_width, head, qkv_ref, o_ref):
    seq = qkv_ref.shape[0]
    k_all = qkv_ref[:, q_width:q_width + head]
    v_flip = jnp.transpose(qkv_ref[:, q_width + head:].astype(jnp.float32)).astype(jnp.bfloat16)
    for col in range(0, q_width, head):
        for start, end in causal_blocks(seq):
            probs = probabilities(k_all[:end], qkv_ref[start:end, col:col + head], head ** -0.5)
            o_flip = dot(v_flip[:, :end], probs.astype(jnp.bfloat16), ((1,), (0,)))
            o_ref[start:end, col:col + head] = jnp.transpose(o_flip).astype(jnp.bfloat16)


def attn_bwd_kernel(q_width, head, qkv_ref, d_o_ref, out_ref, d_k_ref, d_v_ref):
    seq = qkv_ref.shape[0]
    scale = head ** -0.5
    k_all = qkv_ref[:, q_width:q_width + head]
    v_all = qkv_ref[:, q_width + head:]
    k_flip = jnp.transpose(k_all.astype(jnp.float32)).astype(jnp.bfloat16)
    d_k_ref[...] = jnp.zeros_like(d_k_ref)
    d_v_ref[...] = jnp.zeros_like(d_v_ref)
    for col in range(0, q_width, head):
        for start, end in causal_blocks(seq):
            q_blk = qkv_ref[start:end, col:col + head]
            d_o_blk = d_o_ref[start:end, col:col + head]
            probs = probabilities(k_all[:end], q_blk, scale)
            d_p = dot(v_all[:end], d_o_blk, ((1,), (1,)))
            d_v_ref[:end] += dot(probs.astype(jnp.bfloat16), d_o_blk, ((1,), (0,)))
            d_s = probs * (d_p - jnp.sum(probs * d_p, axis=0, keepdims=True))
            d_s = (d_s * scale).astype(jnp.bfloat16)
            d_k_ref[:end] += dot(d_s, q_blk, ((1,), (0,)))
            d_q_flip = dot(k_flip[:, :end], d_s, ((1,), (0,)))
            out_ref[start:end, col:col + head] = jnp.transpose(d_q_flip).astype(jnp.bfloat16)
    out_ref[:, q_width:q_width + head] = d_k_ref[...].astype(jnp.bfloat16)
    out_ref[:, q_width + head:] = d_v_ref[...].astype(jnp.bfloat16)


def by_sequence(kernel, seq, q_width, head, args, width, scratch, flops):
    rows = args[0].shape[0]
    return pl.pallas_call(
        functools.partial(kernel, q_width, head),
        grid=(rows // seq,),
        in_specs=[pl.BlockSpec((seq, arg.shape[1]), lambda i: (i, 0)) for arg in args],
        out_specs=pl.BlockSpec((seq, width), lambda i: (i, 0)),
        out_shape=jax.ShapeDtypeStruct((rows, width), jnp.bfloat16),
        scratch_shapes=[pltpu.VMEM((seq, head), jnp.float32)] * scratch,
        cost_estimate=pl.CostEstimate(flops=flops, bytes_accessed=0, transcendentals=0),
    )(*args)


def attn_forward(x_own, weight, q_width, head, seq):
    normed = pair_rows(norm_bf16(x_own))
    qkv = times(normed, weight[:, :q_width + 2 * head]).astype(jnp.bfloat16)
    o_act = by_sequence(attn_fwd_kernel, seq, q_width, head, (qkv,), q_width, 0,
                  20_000_000_000)
    proj = both_halves(o_act, weight[:, q_width + 2 * head:], x_own.shape[0], times_flipped)
    y_own = (x_own.astype(jnp.float32) + proj).astype(jnp.bfloat16)
    return y_own, (x_own, normed, qkv, o_act)


def attn_backward(saved, weight, q_width, head, seq, grad_own):
    x_own, normed, qkv, o_act = saved
    grad_y = pair_rows(grad_own)
    d_o = times(grad_y, weight[:, q_width + 2 * head:]).astype(jnp.bfloat16)
    d_qkv = by_sequence(attn_bwd_kernel, seq, q_width, head, (qkv, d_o), qkv.shape[1], 2,
                  40_000_000_000)
    d_norm = both_halves(d_qkv, weight[:, :q_width + 2 * head], grad_own.shape[0], times_flipped)
    grad_x = (grad_own.astype(jnp.float32) + norm_back(x_own, d_norm)).astype(jnp.bfloat16)
    return grad_x, over_rows(normed, d_qkv), over_rows(grad_y, o_act)


def gelu_parts(hidden):
    square = hidden * hidden
    half = 0.5 + 0.5 * jnp.tanh(hidden * (GELU_A + GELU_A * GELU_B * square))
    value = hidden * half
    slope = half + value * (1.0 - half) * (2.0 * GELU_A + 6.0 * GELU_A * GELU_B * square)
    return value.astype(jnp.bfloat16), slope


def mlp_hidden(normed, up_weight):
    return lax.optimization_barrier(gelu_parts(times(normed, up_weight)))


def mlp_output(x_own, gelu_act, down_weight):
    proj = both_halves(gelu_act, down_weight, x_own.shape[0], times)
    return (x_own.astype(jnp.float32) + proj).astype(jnp.bfloat16)


def mlp_backward(x_own, slope, up_weight, down_weight, grad_own):
    grad_act = times_flipped(pair_rows(grad_own), down_weight)
    d_hid = (grad_act * slope).astype(jnp.bfloat16)
    d_norm = both_halves(d_hid, up_weight, grad_own.shape[0], times_flipped)
    return (grad_own.astype(jnp.float32) + norm_back(x_own, d_norm)).astype(jnp.bfloat16)


def mlp_grads_kernel(place_ref, up_ref, down_ref, norm_ref, grad_ref, *rest):
    d_down_ref, parts, d_up_ref, flip_ref = rest[-2 * CHIPS - 3], rest[-2 * CHIPS - 2:-2], rest[-2], rest[-1]
    step = pl.program_id(0)
    normed, grad_y = norm_ref[...], grad_ref[...]

    @pl.when(step == 0)
    def _():
        d_down_ref[...] = jnp.zeros_like(d_down_ref)
        d_up_ref[...] = jnp.zeros_like(d_up_ref)

    gelu_act, slope = gelu_parts(dot(up_ref[...], normed, ((1,), (1,))))
    d_hid = (dot(down_ref[...], grad_y, ((1,), (1,))) * slope).astype(jnp.bfloat16)
    d_down_ref[0] += dot(gelu_act, grad_y, ((1,), (0,)))
    d_up_ref[...] += dot(d_hid, normed, ((1,), (0,)))

    @pl.when(step == pl.num_programs(0) - 1)
    def _():
        rows = parts[0].shape[0]
        for i in range(CHIPS):
            start = pl.multiple_of((place_ref[0] ^ i) * (CORES * rows), CORES * rows)
            flip_ref[...] = jnp.transpose(d_up_ref[:, pl.ds(start, CORES * rows)])
            for j in range(CORES):
                start = pl.multiple_of((place_ref[1] ^ j) * rows, rows)
                parts[CORES * i + j][...] = flip_ref[pl.ds(start, rows), :]


def mlp_weight_grads(place, layer, pairs, earlier, up_flip, down_block, norms, grads):
    block, width = down_block.shape
    rows = width // (CHIPS * CORES)
    once = pl.Buffered(1)
    whole = pl.BlockSpec((block, width), lambda i, p: (0, 0), pipeline_mode=once)
    tokens = pl.BlockSpec((TOKEN_TILE, width), lambda i, p: (i, 0))
    part = pl.BlockSpec((rows, block), lambda i, p: (0, 0), pipeline_mode=once)
    args = [place, up_flip, down_block, norms, grads, *earlier]
    outs = pl.pallas_call(
        mlp_grads_kernel,
        grid_spec=pltpu.PrefetchScalarGridSpec(
            num_scalar_prefetch=1,
            grid=(norms.shape[0] // TOKEN_TILE,),
            in_specs=[whole, whole, tokens, tokens] + [pl.BlockSpec(memory_space=pl.ANY)] * len(earlier),
            out_specs=[pl.BlockSpec((1, block, width), lambda i, p: (layer, 0, 0), pipeline_mode=once)]
            + [part] * (CHIPS * CORES),
            scratch_shapes=[pltpu.VMEM((block, width), jnp.float32), pltpu.VMEM((CORES * rows, block), jnp.float32)],
        ),
        out_shape=[jax.ShapeDtypeStruct((pairs, block, width), jnp.float32)]
        + [jax.ShapeDtypeStruct((rows, block), jnp.float32)] * (CHIPS * CORES),
        input_output_aliases={len(args) - 1: 0} if earlier else {},
        compiler_params=pltpu.CompilerParams(vmem_limit_bytes=60 * 1024 * 1024),
        cost_estimate=pl.CostEstimate(flops=8 * norms.shape[0] * block * width, bytes_accessed=0,
                                      transcendentals=0),
        name="mlp_grads",
    )(*args)
    return outs[0], outs[1:]


def exchange(parts):
    devices = range(CHIPS * CORES)
    return [lax.ppermute(part, AXES, [(d, d ^ i) for d in devices]) if i else part for i, part in enumerate(parts)]


def assemble_kernel(place_ref, *refs):
    parts, out_ref = [ref[...] for ref in refs[:CHIPS * CORES]], refs[-1]
    for bit in range(3):
        swapped = ((place_ref[0] * CORES + place_ref[1]) >> bit) % 2 == 1
        parts = [jnp.where(swapped, parts[i ^ (1 << bit)], part) for i, part in enumerate(parts)]
    for i, part in enumerate(parts):
        out_ref[0, :, i * part.shape[1]:(i + 1) * part.shape[1]] = part


def assemble(place, layer, pairs, earlier, parts):
    rows, block = parts[0].shape
    out_width = block * len(parts)
    return pl.pallas_call(
        assemble_kernel,
        grid_spec=pltpu.PrefetchScalarGridSpec(
            num_scalar_prefetch=1,
            grid=(rows // ROW_TILE,),
            in_specs=[pl.BlockSpec((ROW_TILE, block), lambda i, p: (i, 0))] * len(parts)
            + [pl.BlockSpec(memory_space=pl.ANY)] * len(earlier),
            out_specs=pl.BlockSpec((1, ROW_TILE, out_width), lambda i, p: (layer, i, 0)),
        ),
        out_shape=jax.ShapeDtypeStruct((pairs, rows, out_width), jnp.float32),
        input_output_aliases={1 + len(parts): 0} if earlier else {},
        cost_estimate=pl.CostEstimate(flops=5_000_000_000, bytes_accessed=0, transcendentals=0),
        name="assemble",
    )(place, *parts, *earlier)


def split_kernel(place_ref, rows_ref, keep_ref, send_ref):
    block = rows_ref.shape[2] // (CHIPS * CORES)
    for i in range(CHIPS):
        pair = [rows_ref[0, :, (CORES * i + j) * block:(CORES * i + j + 1) * block] for j in range(CORES)]
        cols = slice(i * block, (i + 1) * block)
        keep_ref[:, cols] = jnp.where(place_ref[1] == 0, pair[0], pair[1])
        send_ref[:, cols] = jnp.where(place_ref[1] == 0, pair[1], pair[0])


def split_columns(place, layer, weight):
    rows, cols = weight.shape[1:]
    half = jax.ShapeDtypeStruct((rows, cols // CORES), weight.dtype)
    return pl.pallas_call(
        split_kernel,
        grid_spec=pltpu.PrefetchScalarGridSpec(
            num_scalar_prefetch=1,
            grid=(rows // ROW_TILE,),
            in_specs=[pl.BlockSpec((1, ROW_TILE, cols), lambda i, p: (layer, i, 0))],
            out_specs=[pl.BlockSpec((ROW_TILE, cols // CORES), lambda i, p: (i, 0))] * CORES,
        ),
        out_shape=[half] * CORES,
        cost_estimate=pl.CostEstimate(flops=5_000_000_000, bytes_accessed=0, transcendentals=0),
        name="split",
    )(place, weight)


def flip_kernel(place_ref, up_ref, out_ref):
    block = out_ref.shape[0]
    cols = up_ref[:, :block]
    for i in range(1, CHIPS):
        cols = jnp.where(place_ref[0] == i, up_ref[:, i * block:(i + 1) * block], cols)
    out_ref[...] = jnp.transpose(cols.astype(jnp.float32)).astype(jnp.bfloat16)


def flip(place, up_weight):
    width, cols = up_weight.shape
    return pl.pallas_call(
        flip_kernel,
        grid_spec=pltpu.PrefetchScalarGridSpec(
            num_scalar_prefetch=1,
            grid=(width // FLIP_TILE,),
            in_specs=[pl.BlockSpec((FLIP_TILE, cols), lambda i, p: (i, 0))],
            out_specs=pl.BlockSpec((cols // CHIPS, FLIP_TILE), lambda i, p: (0, i)),
        ),
        out_shape=jax.ShapeDtypeStruct((cols // CHIPS, width), jnp.bfloat16),
        cost_estimate=pl.CostEstimate(flops=5_000_000_000, bytes_accessed=0, transcendentals=0),
        name="flip",
    )(place, up_weight)


def solution(mesh):
    row_spec = P(AXES)
    weight_spec = P(None, AXES)

    def body(x_loc, w_q, w_k, w_v, w_o, w_up, w_down, grad_out):
        core = lax.axis_index(CORE)
        chip = lax.axis_index(CHIP)
        pairs, shard, heads, head = w_q.shape
        seqs, seq, width = x_loc.shape
        q_width = heads // CORES * head

        place = jnp.stack([chip, core]).astype(jnp.int32)

        def attn_piece(layer, core):
            halves = []
            for part in range(CORES):
                cols = [w[layer].reshape(shard, CORES, -1)[:, part] for w in (w_q, w_k, w_v, w_o)]
                halves.append(jnp.concatenate(cols, axis=1))
            return to_columns(core, *by_core(core, *halves))

        def up_piece(layer, core, place):
            return to_columns(core, *split_columns(place, layer, w_up))

        attn_full, up_full, down_full, up_flip = [], [], [], []

        def gather_weights(layer, core, place):
            attn_full.append(gather_weight(chip, attn_piece(layer, core)))
            up_full.append(gather_weight(chip, up_piece(layer, core, place)))
            down_full.append(gather_weight(chip, w_down[layer]))
            up_flip.append(flip(place, up_full[layer]))

        gather_weights(0, core, place)
        carry_x = x_loc.reshape(seqs * seq, width)
        grad_x = grad_out.reshape(seqs * seq, width)
        attn_saved, mlp_saved, d_up, d_down = [], [], [], []

        def weight_grads(layer, norms, grads, d_down):
            down, parts = mlp_weight_grads(place, layer, pairs, d_down, up_flip[layer], w_down[layer], norms, grads)
            return exchange(parts), [down]

        for layer in range(pairs):
            x_own, saved = attn_forward(carry_x, attn_full[layer], q_width, head, seq)
            attn_saved.append(saved)
            if layer < pairs - 1:
                x_own, *later = lax.optimization_barrier((x_own, core, place))
                gather_weights(layer + 1, *later)
            n_own = norm_bf16(x_own)
            gelu_act, slope = mlp_hidden(pair_rows(n_own), up_full[layer])
            norms = gather_rows(n_own)
            if layer == pairs - 1:
                parts, d_down = weight_grads(layer, norms, gather_rows(grad_x), d_down)
            mlp_saved.append((x_own, norms, slope))
            if layer < pairs - 1:
                carry_x = mlp_output(x_own, gelu_act, down_full[layer])
        last = (x_own, gelu_act, down_full[-1])
        grad_lists = ([], [], [], [])
        for layer in reversed(range(pairs)):
            x_own, norms, slope = mlp_saved[layer]
            if layer < pairs - 1:
                parts, d_down = weight_grads(layer, norms, gather_rows(grad_x), d_down)
            d_up = [assemble(place, layer, pairs, d_up, parts)]
            grad_x = mlp_backward(x_own, slope, up_full[layer], down_full[layer], grad_x)
            grad_x, d_qkv, d_o = attn_backward(attn_saved[layer], attn_full[layer], q_width, head, seq, grad_x)
            parts = to_rows(core, scatter_sum(d_o))
            grad_lists[3].append(jnp.concatenate(parts, axis=1).reshape(shard, heads, head))
            parts = to_rows(core, scatter_sum(d_qkv))
            grad_lists[0].append(jnp.concatenate([part[:, :q_width] for part in parts], axis=1)
                                 .reshape(shard, heads, head))
            grad_lists[1].append(jnp.stack([part[:, q_width:q_width + head] for part in parts], axis=1))
            grad_lists[2].append(jnp.stack([part[:, q_width + head:] for part in parts], axis=1))
        last, d_down = lax.optimization_barrier((last, d_down))
        y_loc = mlp_output(*last).reshape(x_loc.shape)
        stacked = tuple(jnp.stack(grad_list[::-1]) for grad_list in grad_lists)
        return (y_loc, grad_x.reshape(x_loc.shape)) + stacked + (d_up[0], d_down[0])

    return jax.shard_map(body, mesh=mesh, in_specs=(row_spec,) + (weight_spec,) * 6 + (row_spec,),
                         out_specs=(row_spec, row_spec) + (weight_spec,) * 6, check_vma=False)
```

```python
import functools

import jax
import jax.numpy as jnp
from jax import lax
from jax.experimental import pallas as pl
from jax.experimental.pallas import tpu as pltpu
from jax.sharding import PartitionSpec as P


CHIP, CORE = AXES = ("sub", "fsdp")
EPS = 1e-6
MASK_FILL = -1e30
GELU_A = (2.0 / 3.141592653589793) ** 0.5
GELU_B = 0.044715
CHIPS = 4
CORES = 2
QUERY_BLOCK = 256
TOKEN_TILE = 512
ROW_TILE = 48
FLIP_TILE = 256
NEIGHBOURS = (1, 2)


def rms_norm(values):
    return values * lax.rsqrt(jnp.mean(values * values, axis=-1, keepdims=True) + EPS)


def norm_bf16(x_loc):
    return rms_norm(x_loc.astype(jnp.float32)).astype(jnp.bfloat16)


def norm_back(x_loc, grad_norm):
    _, pull_back = jax.vjp(rms_norm, x_loc.astype(jnp.float32))
    return pull_back(grad_norm)[0]


def dot(left, right, contract):
    return lax.dot_general(left, right, (contract, ((), ())), preferred_element_type=jnp.float32)


def times(left, right):
    return dot(left, right, ((1,), (0,)))


def times_flipped(left, right):
    return dot(left, right, ((1,), (1,)))


def over_rows(left, right):
    return dot(left, right, ((0,), (0,)))


def swap(value):
    return lax.ppermute(value, CORE, [(0, 1), (1, 0)])


def hop(value, step):
    return lax.ppermute(value, CHIP, [(chip, chip ^ step) for chip in range(CHIPS)])


def by_core(core, mine, other):
    return jnp.where(core == 0, mine, other), jnp.where(core == 0, other, mine)


def to_columns(core, keep, send):
    first, second = by_core(core, keep, swap(send))
    return jnp.concatenate([first, second], axis=0)


def to_rows(core, grad):
    rows = grad.shape[0] // CORES
    grad = grad.reshape((CORES, rows) + grad.shape[1:])
    keep = lax.dynamic_index_in_dim(grad, core, 0, keepdims=False)
    send = lax.dynamic_index_in_dim(grad, 1 - core, 0, keepdims=False)
    return by_core(core, keep, swap(send))


def blank_kernel(_, out_ref):
    del out_ref


def blank(piece):
    anywhere = pl.BlockSpec(memory_space=pl.ANY)
    return pl.pallas_call(blank_kernel, in_specs=[anywhere], out_specs=anywhere, name="blank",
                          out_shape=jax.ShapeDtypeStruct((CHIPS,) + piece.shape, piece.dtype))(piece)


def gather_weight(chip, piece):
    half = piece.shape[0] // 2
    near = [hop(piece, step) for step in NEIGHBOURS]
    opposite = [hop(near[0][:half], NEIGHBOURS[1]),
                hop(near[1][half:], NEIGHBOURS[0])]
    full = blank(piece)
    parts = [(piece, 0, 0), (near[0], NEIGHBOURS[0], 0), (near[1], NEIGHBOURS[1], 0),
             (opposite[0], sum(NEIGHBOURS), 0), (opposite[1], sum(NEIGHBOURS), half)]
    for part, step, row in parts:
        full = lax.dynamic_update_slice(full, part[None], (chip ^ step, row, 0))
    return full.reshape(-1, piece.shape[1])


def gather_rows(value):
    return functools.partial(lax.all_gather, axis=0, tiled=True)(value, AXES)


def scatter_sum(grad_full):
    return lax.psum_scatter(grad_full, CHIP, scatter_dimension=0, tiled=True)


def both_halves(left, right, rows, product):
    other = swap(product(left[rows:], right))
    own = lax.optimization_barrier(product(left[:rows], right))
    return own + other


def pair_rows(value):
    return jnp.concatenate([value, swap(value)], axis=0)


def causal_blocks(seq):
    return [(start, start + QUERY_BLOCK) for start in range(0, seq, QUERY_BLOCK)]


def probabilities(k_blk, q_blk, scale):
    scores = dot(k_blk, q_blk, ((1,), (1,))) * scale
    keys, queries = scores.shape
    key = lax.broadcasted_iota(jnp.int32, (queries, queries), 0)
    query = lax.broadcasted_iota(jnp.int32, (queries, queries), 1)
    last = jnp.where(key <= query, scores[keys - queries:], MASK_FILL)
    scores = last if keys == queries else jnp.concatenate([scores[:keys - queries], last], axis=0)
    powers = jnp.exp(scores - jnp.max(scores, axis=0, keepdims=True))
    return powers * (1.0 / jnp.sum(powers, axis=0, keepdims=True))


def attn_fwd_kernel(q_width, head, qkv_ref, o_ref):
    seq = qkv_ref.shape[0]
    k_all = qkv_ref[:, q_width:q_width + head]
    v_flip = jnp.transpose(qkv_ref[:, q_width + head:].astype(jnp.float32)).astype(jnp.bfloat16)
    for col in range(0, q_width, head):
        for start, end in causal_blocks(seq):
            probs = probabilities(k_all[:end], qkv_ref[start:end, col:col + head], head ** -0.5)
            o_flip = dot(v_flip[:, :end], probs.astype(jnp.bfloat16), ((1,), (0,)))
            o_ref[start:end, col:col + head] = jnp.transpose(o_flip).astype(jnp.bfloat16)


def attn_bwd_kernel(q_width, head, qkv_ref, d_o_ref, out_ref, d_k_ref, d_v_ref):
    seq = qkv_ref.shape[0]
    scale = head ** -0.5
    k_all = qkv_ref[:, q_width:q_width + head]
    v_all = qkv_ref[:, q_width + head:]
    k_flip = jnp.transpose(k_all.astype(jnp.float32)).astype(jnp.bfloat16)
    d_k_ref[...] = jnp.zeros_like(d_k_ref)
    d_v_ref[...] = jnp.zeros_like(d_v_ref)
    for col in range(0, q_width, head):
        for start, end in causal_blocks(seq):
            q_blk = qkv_ref[start:end, col:col + head]
            d_o_blk = d_o_ref[start:end, col:col + head]
            probs = probabilities(k_all[:end], q_blk, scale)
            d_p = dot(v_all[:end], d_o_blk, ((1,), (1,)))
            d_v_ref[:end] += dot(probs.astype(jnp.bfloat16), d_o_blk, ((1,), (0,)))
            d_s = probs * (d_p - jnp.sum(probs * d_p, axis=0, keepdims=True))
            d_s = (d_s * scale).astype(jnp.bfloat16)
            d_k_ref[:end] += dot(d_s, q_blk, ((1,), (0,)))
            d_q_flip = dot(k_flip[:, :end], d_s, ((1,), (0,)))
            out_ref[start:end, col:col + head] = jnp.transpose(d_q_flip).astype(jnp.bfloat16)
    out_ref[:, q_width:q_width + head] = d_k_ref[...].astype(jnp.bfloat16)
    out_ref[:, q_width + head:] = d_v_ref[...].astype(jnp.bfloat16)


def by_sequence(kernel, seq, q_width, head, args, width, scratch, flops):
    rows = args[0].shape[0]
    return pl.pallas_call(
        functools.partial(kernel, q_width, head),
        grid=(rows // seq,),
        in_specs=[pl.BlockSpec((seq, arg.shape[1]), lambda i: (i, 0)) for arg in args],
        out_specs=pl.BlockSpec((seq, width), lambda i: (i, 0)),
        out_shape=jax.ShapeDtypeStruct((rows, width), jnp.bfloat16),
        scratch_shapes=[pltpu.VMEM((seq, head), jnp.float32)] * scratch,
        cost_estimate=pl.CostEstimate(flops=flops, bytes_accessed=0, transcendentals=0),
    )(*args)


def attn_forward(x_own, weight, q_width, head, seq):
    normed = pair_rows(norm_bf16(x_own))
    qkv = times(normed, weight[:, :q_width + 2 * head]).astype(jnp.bfloat16)
    o_act = by_sequence(attn_fwd_kernel, seq, q_width, head, (qkv,), q_width, 0,
                  20_000_000_000)
    proj = both_halves(o_act, weight[:, q_width + 2 * head:], x_own.shape[0], times_flipped)
    y_own = (x_own.astype(jnp.float32) + proj).astype(jnp.bfloat16)
    return y_own, (x_own, normed, qkv, o_act)


def attn_backward(saved, weight, q_width, head, seq, grad_own):
    x_own, normed, qkv, o_act = saved
    grad_y = pair_rows(grad_own)
    d_o = times(grad_y, weight[:, q_width + 2 * head:]).astype(jnp.bfloat16)
    d_qkv = by_sequence(attn_bwd_kernel, seq, q_width, head, (qkv, d_o), qkv.shape[1], 2,
                  40_000_000_000)
    d_norm = both_halves(d_qkv, weight[:, :q_width + 2 * head], grad_own.shape[0], times_flipped)
    grad_x = (grad_own.astype(jnp.float32) + norm_back(x_own, d_norm)).astype(jnp.bfloat16)
    return grad_x, over_rows(normed, d_qkv), over_rows(grad_y, o_act)


def gelu_parts(hidden):
    square = hidden * hidden
    half = 0.5 + 0.5 * jnp.tanh(hidden * (GELU_A + GELU_A * GELU_B * square))
    value = hidden * half
    slope = half + value * (1.0 - half) * (2.0 * GELU_A + 6.0 * GELU_A * GELU_B * square)
    return value.astype(jnp.bfloat16), slope


def mlp_hidden(normed, up_weight):
    return lax.optimization_barrier(gelu_parts(times(normed, up_weight)))


def mlp_output(x_own, gelu_act, down_weight):
    proj = both_halves(gelu_act, down_weight, x_own.shape[0], times)
    return (x_own.astype(jnp.float32) + proj).astype(jnp.bfloat16)


def mlp_backward(x_own, slope, up_weight, down_weight, grad_own):
    grad_act = times_flipped(pair_rows(grad_own), down_weight)
    d_hid = (grad_act * slope).astype(jnp.bfloat16)
    d_norm = both_halves(d_hid, up_weight, grad_own.shape[0], times_flipped)
    return (grad_own.astype(jnp.float32) + norm_back(x_own, d_norm)).astype(jnp.bfloat16)


def mlp_grads_kernel(place_ref, up_ref, down_ref, norm_ref, grad_ref, *rest):
    d_down_ref, parts, d_up_ref, flip_ref = rest[-2 * CHIPS - 3], rest[-2 * CHIPS - 2:-2], rest[-2], rest[-1]
    step = pl.program_id(0)
    normed, grad_y = norm_ref[...], grad_ref[...]

    @pl.when(step == 0)
    def _():
        d_down_ref[...] = jnp.zeros_like(d_down_ref)
        d_up_ref[...] = jnp.zeros_like(d_up_ref)

    gelu_act, slope = gelu_parts(dot(up_ref[...], normed, ((1,), (1,))))
    d_hid = (dot(down_ref[...], grad_y, ((1,), (1,))) * slope).astype(jnp.bfloat16)
    d_down_ref[0] += dot(gelu_act, grad_y, ((1,), (0,)))
    d_up_ref[...] += dot(d_hid, normed, ((1,), (0,)))

    @pl.when(step == pl.num_programs(0) - 1)
    def _():
        rows = parts[0].shape[0]
        for i in range(CHIPS):
            start = pl.multiple_of((place_ref[0] ^ i) * (CORES * rows), CORES * rows)
            flip_ref[...] = jnp.transpose(d_up_ref[:, pl.ds(start, CORES * rows)])
            for j in range(CORES):
                start = pl.multiple_of((place_ref[1] ^ j) * rows, rows)
                parts[CORES * i + j][...] = flip_ref[pl.ds(start, rows), :]


def mlp_weight_grads(place, layer, pairs, earlier, up_flip, down_block, norms, grads):
    block, width = down_block.shape
    rows = width // (CHIPS * CORES)
    once = pl.Buffered(1)
    whole = pl.BlockSpec((block, width), lambda i, p: (0, 0), pipeline_mode=once)
    tokens = pl.BlockSpec((TOKEN_TILE, width), lambda i, p: (i, 0))
    part = pl.BlockSpec((rows, block), lambda i, p: (0, 0), pipeline_mode=once)
    args = [place, up_flip, down_block, norms, grads, *earlier]
    outs = pl.pallas_call(
        mlp_grads_kernel,
        grid_spec=pltpu.PrefetchScalarGridSpec(
            num_scalar_prefetch=1,
            grid=(norms.shape[0] // TOKEN_TILE,),
            in_specs=[whole, whole, tokens, tokens] + [pl.BlockSpec(memory_space=pl.ANY)] * len(earlier),
            out_specs=[pl.BlockSpec((1, block, width), lambda i, p: (layer, 0, 0), pipeline_mode=once)]
            + [part] * (CHIPS * CORES),
            scratch_shapes=[pltpu.VMEM((block, width), jnp.float32), pltpu.VMEM((CORES * rows, block), jnp.float32)],
        ),
        out_shape=[jax.ShapeDtypeStruct((pairs, block, width), jnp.float32)]
        + [jax.ShapeDtypeStruct((rows, block), jnp.float32)] * (CHIPS * CORES),
        input_output_aliases={len(args) - 1: 0} if earlier else {},
        compiler_params=pltpu.CompilerParams(vmem_limit_bytes=60 * 1024 * 1024),
        cost_estimate=pl.CostEstimate(flops=8 * norms.shape[0] * block * width, bytes_accessed=0,
                                      transcendentals=0),
        name="mlp_grads",
    )(*args)
    return outs[0], outs[1:]


def exchange(parts):
    devices = range(CHIPS * CORES)
    return [lax.ppermute(part, AXES, [(d, d ^ i) for d in devices]) if i else part for i, part in enumerate(parts)]


def assemble_kernel(place_ref, *refs):
    parts, out_ref = [ref[...] for ref in refs[:CHIPS * CORES]], refs[-1]
    for bit in range(3):
        swapped = ((place_ref[0] * CORES + place_ref[1]) >> bit) % 2 == 1
        parts = [jnp.where(swapped, parts[i ^ (1 << bit)], part) for i, part in enumerate(parts)]
    for i, part in enumerate(parts):
        out_ref[0, :, i * part.shape[1]:(i + 1) * part.shape[1]] = part


def assemble(place, layer, pairs, earlier, parts):
    rows, block = parts[0].shape
    out_width = block * len(parts)
    return pl.pallas_call(
        assemble_kernel,
        grid_spec=pltpu.PrefetchScalarGridSpec(
            num_scalar_prefetch=1,
            grid=(rows // ROW_TILE,),
            in_specs=[pl.BlockSpec((ROW_TILE, block), lambda i, p: (i, 0))] * len(parts)
            + [pl.BlockSpec(memory_space=pl.ANY)] * len(earlier),
            out_specs=pl.BlockSpec((1, ROW_TILE, out_width), lambda i, p: (layer, i, 0)),
        ),
        out_shape=jax.ShapeDtypeStruct((pairs, rows, out_width), jnp.float32),
        input_output_aliases={1 + len(parts): 0} if earlier else {},
        cost_estimate=pl.CostEstimate(flops=5_000_000_000, bytes_accessed=0, transcendentals=0),
        name="assemble",
    )(place, *parts, *earlier)


def split_kernel(place_ref, rows_ref, keep_ref, send_ref):
    block = rows_ref.shape[2] // (CHIPS * CORES)
    for i in range(CHIPS):
        pair = [rows_ref[0, :, (CORES * i + j) * block:(CORES * i + j + 1) * block] for j in range(CORES)]
        cols = slice(i * block, (i + 1) * block)
        keep_ref[:, cols] = jnp.where(place_ref[1] == 0, pair[0], pair[1])
        send_ref[:, cols] = jnp.where(place_ref[1] == 0, pair[1], pair[0])


def split_columns(place, layer, weight):
    rows, cols = weight.shape[1:]
    half = jax.ShapeDtypeStruct((rows, cols // CORES), weight.dtype)
    return pl.pallas_call(
        split_kernel,
        grid_spec=pltpu.PrefetchScalarGridSpec(
            num_scalar_prefetch=1,
            grid=(rows // ROW_TILE,),
            in_specs=[pl.BlockSpec((1, ROW_TILE, cols), lambda i, p: (layer, i, 0))],
            out_specs=[pl.BlockSpec((ROW_TILE, cols // CORES), lambda i, p: (i, 0))] * CORES,
        ),
        out_shape=[half] * CORES,
        cost_estimate=pl.CostEstimate(flops=5_000_000_000, bytes_accessed=0, transcendentals=0),
        name="split",
    )(place, weight)


def flip_kernel(place_ref, up_ref, out_ref):
    block = out_ref.shape[0]
    for i in range(CHIPS):
        @pl.when(place_ref[0] == i)
        def _():
            out_ref[...] = jnp.transpose(up_ref[:, i * block:(i + 1) * block])


def flip(place, up_weight):
    width, cols = up_weight.shape
    return pl.pallas_call(
        flip_kernel,
        grid_spec=pltpu.PrefetchScalarGridSpec(
            num_scalar_prefetch=1,
            grid=(width // FLIP_TILE,),
            in_specs=[pl.BlockSpec((FLIP_TILE, cols), lambda i, p: (i, 0))],
            out_specs=pl.BlockSpec((cols // CHIPS, FLIP_TILE), lambda i, p: (0, i)),
        ),
        out_shape=jax.ShapeDtypeStruct((cols // CHIPS, width), jnp.bfloat16),
        cost_estimate=pl.CostEstimate(flops=5_000_000_000, bytes_accessed=0, transcendentals=0),
        name="flip",
    )(place, up_weight)


def solution(mesh):
    row_spec = P(AXES)
    weight_spec = P(None, AXES)

    def body(x_loc, w_q, w_k, w_v, w_o, w_up, w_down, grad_out):
        core = lax.axis_index(CORE)
        chip = lax.axis_index(CHIP)
        pairs, shard, heads, head = w_q.shape
        seqs, seq, width = x_loc.shape
        q_width = heads // CORES * head

        place = jnp.stack([chip, core]).astype(jnp.int32)

        def attn_piece(layer, core):
            halves = []
            for part in range(CORES):
                cols = [w[layer].reshape(shard, CORES, -1)[:, part] for w in (w_q, w_k, w_v, w_o)]
                halves.append(jnp.concatenate(cols, axis=1))
            return to_columns(core, *by_core(core, *halves))

        def up_piece(layer, core, place):
            return to_columns(core, *split_columns(place, layer, w_up))

        attn_full, up_full, down_full, up_flip = [], [], [], []

        def gather_weights(layer, core, place):
            attn_full.append(gather_weight(chip, attn_piece(layer, core)))
            up_full.append(gather_weight(chip, up_piece(layer, core, place)))
            down_full.append(gather_weight(chip, w_down[layer]))
            up_flip.append(flip(place, up_full[layer]))

        gather_weights(0, core, place)
        carry_x = x_loc.reshape(seqs * seq, width)
        grad_x = grad_out.reshape(seqs * seq, width)
        attn_saved, mlp_saved, d_up, d_down = [], [], [], []

        def weight_grads(layer, norms, grads, d_down):
            down, parts = mlp_weight_grads(place, layer, pairs, d_down, up_flip[layer], w_down[layer], norms, grads)
            return exchange(parts), [down]

        for layer in range(pairs):
            x_own, saved = attn_forward(carry_x, attn_full[layer], q_width, head, seq)
            attn_saved.append(saved)
            if layer < pairs - 1:
                x_own, *later = lax.optimization_barrier((x_own, core, place))
                gather_weights(layer + 1, *later)
            n_own = norm_bf16(x_own)
            gelu_act, slope = mlp_hidden(pair_rows(n_own), up_full[layer])
            norms = gather_rows(n_own)
            if layer == pairs - 1:
                parts, d_down = weight_grads(layer, norms, gather_rows(grad_x), d_down)
            mlp_saved.append((x_own, norms, slope))
            if layer < pairs - 1:
                carry_x = mlp_output(x_own, gelu_act, down_full[layer])
        last = (x_own, gelu_act, down_full[-1])
        grad_lists = ([], [], [], [])
        for layer in reversed(range(pairs)):
            x_own, norms, slope = mlp_saved[layer]
            if layer < pairs - 1:
                parts, d_down = weight_grads(layer, norms, gather_rows(grad_x), d_down)
            d_up = [assemble(place, layer, pairs, d_up, parts)]
            grad_x = mlp_backward(x_own, slope, up_full[layer], down_full[layer], grad_x)
            grad_x, d_qkv, d_o = attn_backward(attn_saved[layer], attn_full[layer], q_width, head, seq, grad_x)
            parts = to_rows(core, scatter_sum(d_o))
            grad_lists[3].append(jnp.concatenate(parts, axis=1).reshape(shard, heads, head))
            parts = to_rows(core, scatter_sum(d_qkv))
            grad_lists[0].append(jnp.concatenate([part[:, :q_width] for part in parts], axis=1)
                                 .reshape(shard, heads, head))
            grad_lists[1].append(jnp.stack([part[:, q_width:q_width + head] for part in parts], axis=1))
            grad_lists[2].append(jnp.stack([part[:, q_width + head:] for part in parts], axis=1))
        last, d_down = lax.optimization_barrier((last, d_down))
        y_loc = mlp_output(*last).reshape(x_loc.shape)
        stacked = tuple(jnp.stack(grad_list[::-1]) for grad_list in grad_lists)
        return (y_loc, grad_x.reshape(x_loc.shape)) + stacked + (d_up[0], d_down[0])

    return jax.shard_map(body, mesh=mesh, in_specs=(row_spec,) + (weight_spec,) * 6 + (row_spec,),
                         out_specs=(row_spec, row_spec) + (weight_spec,) * 6, check_vma=False)
```

```python
import functools

import jax
import jax.numpy as jnp
from jax import lax
from jax.experimental import pallas as pl
from jax.experimental.pallas import tpu as pltpu
from jax.sharding import PartitionSpec as P


CHIP, CORE = AXES = ("sub", "fsdp")
EPS = 1e-6
MASK_FILL = -1e30
GELU_A = (2.0 / 3.141592653589793) ** 0.5
GELU_B = 0.044715
CHIPS = 4
CORES = 2
QUERY_BLOCK = 256
TOKEN_TILE = 512
ROW_TILE = 48
FLIP_TILE = 256
WIDTH_TILE = 512
COLUMN_TILE = 896
NEIGHBOURS = (1, 2)


def rms_norm(values):
    return values * lax.rsqrt(jnp.mean(values * values, axis=-1, keepdims=True) + EPS)


def norm_bf16(x_loc):
    return rms_norm(x_loc.astype(jnp.float32)).astype(jnp.bfloat16)


def norm_back(x_loc, grad_norm):
    _, pull_back = jax.vjp(rms_norm, x_loc.astype(jnp.float32))
    return pull_back(grad_norm)[0]


def dot(left, right, contract):
    return lax.dot_general(left, right, (contract, ((), ())), preferred_element_type=jnp.float32)


def times(left, right):
    return dot(left, right, ((1,), (0,)))


def times_flipped(left, right):
    return dot(left, right, ((1,), (1,)))


def swap(value):
    return lax.ppermute(value, CORE, [(0, 1), (1, 0)])


def hop(value, step):
    return lax.ppermute(value, CHIP, [(chip, chip ^ step) for chip in range(CHIPS)])


def by_core(core, mine, other):
    return jnp.where(core == 0, mine, other), jnp.where(core == 0, other, mine)


def to_columns(core, keep, send):
    first, second = by_core(core, keep, swap(send))
    return jnp.concatenate([first, second], axis=0)


def to_rows(core, grad):
    rows = grad.shape[0] // CORES
    grad = grad.reshape((CORES, rows) + grad.shape[1:])
    keep = lax.dynamic_index_in_dim(grad, core, 0, keepdims=False)
    send = lax.dynamic_index_in_dim(grad, 1 - core, 0, keepdims=False)
    return by_core(core, keep, swap(send))


def blank_kernel(_, out_ref):
    del out_ref


def blank(piece):
    anywhere = pl.BlockSpec(memory_space=pl.ANY)
    return pl.pallas_call(blank_kernel, in_specs=[anywhere], out_specs=anywhere, name="blank",
                          out_shape=jax.ShapeDtypeStruct((CHIPS,) + piece.shape, piece.dtype))(piece)


def gather_weight(chip, piece):
    half = piece.shape[0] // 2
    near = [hop(piece, step) for step in NEIGHBOURS]
    opposite = [hop(near[0][:half], NEIGHBOURS[1]),
                hop(near[1][half:], NEIGHBOURS[0])]
    full = blank(piece)
    parts = [(piece, 0, 0), (near[0], NEIGHBOURS[0], 0), (near[1], NEIGHBOURS[1], 0),
             (opposite[0], sum(NEIGHBOURS), 0), (opposite[1], sum(NEIGHBOURS), half)]
    for part, step, row in parts:
        full = lax.dynamic_update_slice(full, part[None], (chip ^ step, row, 0))
    return full.reshape(-1, piece.shape[1])


def gather_rows(value):
    return functools.partial(lax.all_gather, axis=0, tiled=True)(value, AXES)


def scatter_sum(grad_full):
    return lax.psum_scatter(grad_full, CHIP, scatter_dimension=0, tiled=True)


def both_halves(left, right, rows, product):
    other = swap(product(left[rows:], right))
    own = lax.optimization_barrier(product(left[:rows], right))
    return own + other


def pair_rows(value):
    return jnp.concatenate([value, swap(value)], axis=0)


def causal_blocks(seq):
    return [(start, start + QUERY_BLOCK) for start in range(0, seq, QUERY_BLOCK)]


def probabilities(k_blk, q_blk, scale):
    scores = dot(k_blk, q_blk, ((1,), (1,))) * scale
    keys, queries = scores.shape
    key = lax.broadcasted_iota(jnp.int32, (queries, queries), 0)
    query = lax.broadcasted_iota(jnp.int32, (queries, queries), 1)
    last = jnp.where(key <= query, scores[keys - queries:], MASK_FILL)
    scores = last if keys == queries else jnp.concatenate([scores[:keys - queries], last], axis=0)
    powers = jnp.exp(scores - jnp.max(scores, axis=0, keepdims=True))
    return powers * (1.0 / jnp.sum(powers, axis=0, keepdims=True))


def attn_fwd_kernel(q_width, head, qkv_ref, o_ref):
    seq = qkv_ref.shape[0]
    k_all = qkv_ref[:, q_width:q_width + head]
    v_flip = jnp.transpose(qkv_ref[:, q_width + head:].astype(jnp.float32)).astype(jnp.bfloat16)
    for col in range(0, q_width, head):
        for start, end in causal_blocks(seq):
            probs = probabilities(k_all[:end], qkv_ref[start:end, col:col + head], head ** -0.5)
            o_flip = dot(v_flip[:, :end], probs.astype(jnp.bfloat16), ((1,), (0,)))
            o_ref[start:end, col:col + head] = jnp.transpose(o_flip).astype(jnp.bfloat16)


def attn_bwd_kernel(q_width, head, qkv_ref, d_o_ref, out_ref, d_k_ref, d_v_ref):
    seq = qkv_ref.shape[0]
    scale = head ** -0.5
    k_all = qkv_ref[:, q_width:q_width + head]
    v_all = qkv_ref[:, q_width + head:]
    k_flip = jnp.transpose(k_all.astype(jnp.float32)).astype(jnp.bfloat16)
    d_k_ref[...] = jnp.zeros_like(d_k_ref)
    d_v_ref[...] = jnp.zeros_like(d_v_ref)
    for col in range(0, q_width, head):
        for start, end in causal_blocks(seq):
            q_blk = qkv_ref[start:end, col:col + head]
            d_o_blk = d_o_ref[start:end, col:col + head]
            probs = probabilities(k_all[:end], q_blk, scale)
            d_p = dot(v_all[:end], d_o_blk, ((1,), (1,)))
            d_v_ref[:end] += dot(probs.astype(jnp.bfloat16), d_o_blk, ((1,), (0,)))
            d_s = probs * (d_p - jnp.sum(probs * d_p, axis=0, keepdims=True))
            d_s = (d_s * scale).astype(jnp.bfloat16)
            d_k_ref[:end] += dot(d_s, q_blk, ((1,), (0,)))
            d_q_flip = dot(k_flip[:, :end], d_s, ((1,), (0,)))
            out_ref[start:end, col:col + head] = jnp.transpose(d_q_flip).astype(jnp.bfloat16)
    out_ref[:, q_width:q_width + head] = d_k_ref[...].astype(jnp.bfloat16)
    out_ref[:, q_width + head:] = d_v_ref[...].astype(jnp.bfloat16)


def by_sequence(kernel, seq, q_width, head, args, width, scratch, flops):
    rows = args[0].shape[0]
    return pl.pallas_call(
        functools.partial(kernel, q_width, head),
        grid=(rows // seq,),
        in_specs=[pl.BlockSpec((seq, arg.shape[1]), lambda i: (i, 0)) for arg in args],
        out_specs=pl.BlockSpec((seq, width), lambda i: (i, 0)),
        out_shape=jax.ShapeDtypeStruct((rows, width), jnp.bfloat16),
        scratch_shapes=[pltpu.VMEM((seq, head), jnp.float32)] * scratch,
        cost_estimate=pl.CostEstimate(flops=flops, bytes_accessed=0, transcendentals=0),
    )(*args)


def attn_forward(x_own, weight, q_width, head, seq):
    normed = pair_rows(norm_bf16(x_own))
    qkv = times(normed, weight[:, :q_width + 2 * head]).astype(jnp.bfloat16)
    o_act = by_sequence(attn_fwd_kernel, seq, q_width, head, (qkv,), q_width, 0,
                  20_000_000_000)
    proj = both_halves(o_act, weight[:, q_width + 2 * head:], x_own.shape[0], times_flipped)
    y_own = (x_own.astype(jnp.float32) + proj).astype(jnp.bfloat16)
    return y_own, (x_own, normed, qkv, o_act)


def attn_grads_kernel(norm_ref, d_qkv_ref, grad_ref, o_ref, out_ref):
    width = d_qkv_ref.shape[1]
    out_ref[:, :width] = dot(norm_ref[...], d_qkv_ref[...], ((0,), (0,)))
    out_ref[:, width:] = dot(grad_ref[...], o_ref[...], ((0,), (0,)))


def attn_grads(normed, d_qkv, grad_y, o_act):
    rows, width = normed.shape
    cols = d_qkv.shape[1] + o_act.shape[1]
    piece = pl.BlockSpec((rows, WIDTH_TILE), lambda i: (0, i))
    whole = [pl.BlockSpec(arg.shape, lambda i: (0, 0), pipeline_mode=pl.Buffered(1)) for arg in (d_qkv, o_act)]
    return pl.pallas_call(
        attn_grads_kernel,
        grid=(width // WIDTH_TILE,),
        in_specs=[piece, whole[0], piece, whole[1]],
        out_specs=pl.BlockSpec((WIDTH_TILE, cols), lambda i: (i, 0)),
        out_shape=jax.ShapeDtypeStruct((width, cols), jnp.float32),
        cost_estimate=pl.CostEstimate(flops=2 * rows * width * cols, bytes_accessed=0, transcendentals=0),
        name="attn_grads",
    )(normed, d_qkv, grad_y, o_act)


def attn_backward(saved, weight, q_width, head, seq, grad_own):
    x_own, normed, qkv, o_act = saved
    grad_y = pair_rows(grad_own)
    d_o = times(grad_y, weight[:, q_width + 2 * head:]).astype(jnp.bfloat16)
    d_qkv = by_sequence(attn_bwd_kernel, seq, q_width, head, (qkv, d_o), qkv.shape[1], 2,
                  40_000_000_000)
    d_norm = both_halves(d_qkv, weight[:, :q_width + 2 * head], grad_own.shape[0], times_flipped)
    grad_x = (grad_own.astype(jnp.float32) + norm_back(x_own, d_norm)).astype(jnp.bfloat16)
    return grad_x, attn_grads(normed, d_qkv, grad_y, o_act)


def gelu_parts(hidden):
    square = hidden * hidden
    half = 0.5 + 0.5 * jnp.tanh(hidden * (GELU_A + GELU_A * GELU_B * square))
    value = hidden * half
    slope = half + value * (1.0 - half) * (2.0 * GELU_A + 6.0 * GELU_A * GELU_B * square)
    return value.astype(jnp.bfloat16), slope


def mlp_hidden(normed, up_weight):
    return lax.optimization_barrier(gelu_parts(times(normed, up_weight)))


def mlp_output(x_own, gelu_act, down_weight):
    proj = both_halves(gelu_act, down_weight, x_own.shape[0], times)
    return (x_own.astype(jnp.float32) + proj).astype(jnp.bfloat16)


def mlp_back_kernel(grad_ref, slope_ref, down_ref, up_ref, out_ref):
    @pl.when(pl.program_id(0) == 0)
    def _():
        out_ref[...] = jnp.zeros_like(out_ref)

    d_hid = (dot(grad_ref[...], down_ref[...], ((1,), (1,))) * slope_ref[...]).astype(jnp.bfloat16)
    out_ref[...] += dot(d_hid, up_ref[...], ((1,), (1,)))


def mlp_back(half, grad_y, slope, down_weight, up_weight):
    rows, (width, cols) = grad_y.shape[0] // CORES, up_weight.shape
    once = pl.Buffered(1)
    return pl.pallas_call(
        mlp_back_kernel,
        grid=(cols // COLUMN_TILE,),
        in_specs=[pl.BlockSpec((rows, width), lambda i: (half, 0), pipeline_mode=once),
                  pl.BlockSpec((rows, COLUMN_TILE), lambda i: (half, i)),
                  pl.BlockSpec((COLUMN_TILE, width), lambda i: (i, 0)),
                  pl.BlockSpec((width, COLUMN_TILE), lambda i: (0, i))],
        out_specs=pl.BlockSpec((rows, width), lambda i: (0, 0), pipeline_mode=once),
        out_shape=jax.ShapeDtypeStruct((rows, width), jnp.float32),
        compiler_params=pltpu.CompilerParams(vmem_limit_bytes=50 * 1024 * 1024),
        cost_estimate=pl.CostEstimate(flops=4 * rows * width * cols, bytes_accessed=0, transcendentals=0),
        name="mlp_back",
    )(grad_y, slope, down_weight, up_weight)


def mlp_backward(x_own, slope, up_weight, down_weight, grad_own):
    args = (pair_rows(grad_own), slope, down_weight, up_weight)
    other = swap(mlp_back(1, *args))
    d_norm = mlp_back(0, *args) + other
    return (grad_own.astype(jnp.float32) + norm_back(x_own, d_norm)).astype(jnp.bfloat16)


def mlp_grads_kernel(place_ref, up_ref, down_ref, norm_ref, grad_ref, *rest):
    d_down_ref, parts, d_up_ref, flip_ref = rest[-2 * CHIPS - 3], rest[-2 * CHIPS - 2:-2], rest[-2], rest[-1]
    step = pl.program_id(0)
    normed, grad_y = norm_ref[...], grad_ref[...]

    @pl.when(step == 0)
    def _():
        d_down_ref[...] = jnp.zeros_like(d_down_ref)
        d_up_ref[...] = jnp.zeros_like(d_up_ref)

    gelu_act, slope = gelu_parts(dot(up_ref[...], normed, ((1,), (1,))))
    d_hid = (dot(down_ref[...], grad_y, ((1,), (1,))) * slope).astype(jnp.bfloat16)
    d_down_ref[0] += dot(gelu_act, grad_y, ((1,), (0,)))
    d_up_ref[...] += dot(d_hid, normed, ((1,), (0,)))

    @pl.when(step == pl.num_programs(0) - 1)
    def _():
        rows = parts[0].shape[0]
        for i in range(CHIPS):
            start = pl.multiple_of((place_ref[0] ^ i) * (CORES * rows), CORES * rows)
            flip_ref[...] = jnp.transpose(d_up_ref[:, pl.ds(start, CORES * rows)])
            for j in range(CORES):
                start = pl.multiple_of((place_ref[1] ^ j) * rows, rows)
                parts[CORES * i + j][...] = flip_ref[pl.ds(start, rows), :]


def mlp_weight_grads(place, layer, pairs, earlier, up_flip, down_block, norms, grads):
    block, width = down_block.shape
    rows = width // (CHIPS * CORES)
    once = pl.Buffered(1)
    whole = pl.BlockSpec((block, width), lambda i, p: (0, 0), pipeline_mode=once)
    tokens = pl.BlockSpec((TOKEN_TILE, width), lambda i, p: (i, 0))
    part = pl.BlockSpec((rows, block), lambda i, p: (0, 0), pipeline_mode=once)
    args = [place, up_flip, down_block, norms, grads, *earlier]
    outs = pl.pallas_call(
        mlp_grads_kernel,
        grid_spec=pltpu.PrefetchScalarGridSpec(
            num_scalar_prefetch=1,
            grid=(norms.shape[0] // TOKEN_TILE,),
            in_specs=[whole, whole, tokens, tokens] + [pl.BlockSpec(memory_space=pl.ANY)] * len(earlier),
            out_specs=[pl.BlockSpec((1, block, width), lambda i, p: (layer, 0, 0), pipeline_mode=once)]
            + [part] * (CHIPS * CORES),
            scratch_shapes=[pltpu.VMEM((block, width), jnp.float32), pltpu.VMEM((CORES * rows, block), jnp.float32)],
        ),
        out_shape=[jax.ShapeDtypeStruct((pairs, block, width), jnp.float32)]
        + [jax.ShapeDtypeStruct((rows, block), jnp.float32)] * (CHIPS * CORES),
        input_output_aliases={len(args) - 1: 0} if earlier else {},
        compiler_params=pltpu.CompilerParams(vmem_limit_bytes=60 * 1024 * 1024),
        cost_estimate=pl.CostEstimate(flops=8 * norms.shape[0] * block * width, bytes_accessed=0,
                                      transcendentals=0),
        name="mlp_grads",
    )(*args)
    return outs[0], outs[1:]


def exchange(parts):
    devices = range(CHIPS * CORES)
    return [lax.ppermute(part, AXES, [(d, d ^ i) for d in devices]) if i else part for i, part in enumerate(parts)]


def assemble_kernel(place_ref, *refs):
    parts, out_ref = [ref[...] for ref in refs[:CHIPS * CORES]], refs[-1]
    for bit in range(3):
        swapped = ((place_ref[0] * CORES + place_ref[1]) >> bit) % 2 == 1
        parts = [jnp.where(swapped, parts[i ^ (1 << bit)], part) for i, part in enumerate(parts)]
    for i, part in enumerate(parts):
        out_ref[0, :, i * part.shape[1]:(i + 1) * part.shape[1]] = part


def assemble(place, layer, pairs, earlier, parts):
    rows, block = parts[0].shape
    out_width = block * len(parts)
    return pl.pallas_call(
        assemble_kernel,
        grid_spec=pltpu.PrefetchScalarGridSpec(
            num_scalar_prefetch=1,
            grid=(rows // ROW_TILE,),
            in_specs=[pl.BlockSpec((ROW_TILE, block), lambda i, p: (i, 0))] * len(parts)
            + [pl.BlockSpec(memory_space=pl.ANY)] * len(earlier),
            out_specs=pl.BlockSpec((1, ROW_TILE, out_width), lambda i, p: (layer, i, 0)),
        ),
        out_shape=jax.ShapeDtypeStruct((pairs, rows, out_width), jnp.float32),
        input_output_aliases={1 + len(parts): 0} if earlier else {},
        cost_estimate=pl.CostEstimate(flops=5_000_000_000, bytes_accessed=0, transcendentals=0),
        name="assemble",
    )(place, *parts, *earlier)


def split_kernel(place_ref, rows_ref, keep_ref, send_ref):
    block = rows_ref.shape[2] // (CHIPS * CORES)
    for i in range(CHIPS):
        pair = [rows_ref[0, :, (CORES * i + j) * block:(CORES * i + j + 1) * block] for j in range(CORES)]
        cols = slice(i * block, (i + 1) * block)
        keep_ref[:, cols] = jnp.where(place_ref[1] == 0, pair[0], pair[1])
        send_ref[:, cols] = jnp.where(place_ref[1] == 0, pair[1], pair[0])


def split_columns(place, layer, weight):
    rows, cols = weight.shape[1:]
    half = jax.ShapeDtypeStruct((rows, cols // CORES), weight.dtype)
    return pl.pallas_call(
        split_kernel,
        grid_spec=pltpu.PrefetchScalarGridSpec(
            num_scalar_prefetch=1,
            grid=(rows // ROW_TILE,),
            in_specs=[pl.BlockSpec((1, ROW_TILE, cols), lambda i, p: (layer, i, 0))],
            out_specs=[pl.BlockSpec((ROW_TILE, cols // CORES), lambda i, p: (i, 0))] * CORES,
        ),
        out_shape=[half] * CORES,
        cost_estimate=pl.CostEstimate(flops=5_000_000_000, bytes_accessed=0, transcendentals=0),
        name="split",
    )(place, weight)


def flip_kernel(place_ref, up_ref, out_ref):
    block = out_ref.shape[0]
    for i in range(CHIPS):
        @pl.when(place_ref[0] == i)
        def _():
            out_ref[...] = jnp.transpose(up_ref[:, i * block:(i + 1) * block])


def flip(place, up_weight):
    width, cols = up_weight.shape
    return pl.pallas_call(
        flip_kernel,
        grid_spec=pltpu.PrefetchScalarGridSpec(
            num_scalar_prefetch=1,
            grid=(width // FLIP_TILE,),
            in_specs=[pl.BlockSpec((FLIP_TILE, cols), lambda i, p: (i, 0))],
            out_specs=pl.BlockSpec((cols // CHIPS, FLIP_TILE), lambda i, p: (0, i)),
        ),
        out_shape=jax.ShapeDtypeStruct((cols // CHIPS, width), jnp.bfloat16),
        cost_estimate=pl.CostEstimate(flops=5_000_000_000, bytes_accessed=0, transcendentals=0),
        name="flip",
    )(place, up_weight)


def solution(mesh):
    row_spec = P(AXES)
    weight_spec = P(None, AXES)

    def body(x_loc, w_q, w_k, w_v, w_o, w_up, w_down, grad_out):
        core = lax.axis_index(CORE)
        chip = lax.axis_index(CHIP)
        pairs, shard, heads, head = w_q.shape
        seqs, seq, width = x_loc.shape
        q_width = heads // CORES * head

        place = jnp.stack([chip, core]).astype(jnp.int32)

        def attn_piece(layer, core):
            halves = []
            for part in range(CORES):
                cols = [w[layer].reshape(shard, CORES, -1)[:, part] for w in (w_q, w_k, w_v, w_o)]
                halves.append(jnp.concatenate(cols, axis=1))
            return to_columns(core, *by_core(core, *halves))

        def up_piece(layer, core, place):
            return to_columns(core, *split_columns(place, layer, w_up))

        attn_full, up_full, down_full, up_flip = [], [], [], []

        def gather_weights(layer, core, place):
            attn_full.append(gather_weight(chip, attn_piece(layer, core)))
            up_full.append(gather_weight(chip, up_piece(layer, core, place)))
            down_full.append(gather_weight(chip, w_down[layer]))
            up_flip.append(flip(place, up_full[layer]))

        gather_weights(0, core, place)
        carry_x = x_loc.reshape(seqs * seq, width)
        grad_x = grad_out.reshape(seqs * seq, width)
        attn_saved, mlp_saved, d_up, d_down = [], [], [], []

        def weight_grads(layer, norms, grads, d_down):
            down, parts = mlp_weight_grads(place, layer, pairs, d_down, up_flip[layer], w_down[layer], norms, grads)
            return exchange(parts), [down]

        for layer in range(pairs):
            x_own, saved = attn_forward(carry_x, attn_full[layer], q_width, head, seq)
            attn_saved.append(saved)
            if layer < pairs - 1:
                x_own, *later = lax.optimization_barrier((x_own, core, place))
                gather_weights(layer + 1, *later)
            n_own = norm_bf16(x_own)
            gelu_act, slope = mlp_hidden(pair_rows(n_own), up_full[layer])
            norms = gather_rows(n_own)
            if layer == pairs - 1:
                parts, d_down = weight_grads(layer, norms, gather_rows(grad_x), d_down)
            mlp_saved.append((x_own, norms, slope))
            if layer < pairs - 1:
                carry_x = mlp_output(x_own, gelu_act, down_full[layer])
        last = (x_own, gelu_act, down_full[-1])
        grad_lists = ([], [], [], [])
        for layer in reversed(range(pairs)):
            x_own, norms, slope = mlp_saved[layer]
            if layer < pairs - 1:
                parts, d_down = weight_grads(layer, norms, gather_rows(grad_x), d_down)
            d_up = [assemble(place, layer, pairs, d_up, parts)]
            grad_x = mlp_backward(x_own, slope, up_full[layer], down_full[layer], grad_x)
            grad_x, d_attn = attn_backward(attn_saved[layer], attn_full[layer], q_width, head, seq, grad_x)
            parts = to_rows(core, scatter_sum(d_attn))
            k_end, v_end = q_width + head, q_width + 2 * head
            for cols, start, end in zip(grad_lists[::3], (0, v_end), (q_width, v_end + q_width)):
                cols.append(jnp.concatenate([part[:, start:end] for part in parts], axis=1).reshape(shard, heads, head))
            grad_lists[1].append(jnp.stack([part[:, q_width:k_end] for part in parts], axis=1))
            grad_lists[2].append(jnp.stack([part[:, k_end:v_end] for part in parts], axis=1))
        last, d_down = lax.optimization_barrier((last, d_down))
        y_loc = mlp_output(*last).reshape(x_loc.shape)
        stacked = tuple(jnp.stack(grad_list[::-1]) for grad_list in grad_lists)
        return (y_loc, grad_x.reshape(x_loc.shape)) + stacked + (d_up[0], d_down[0])

    return jax.shard_map(body, mesh=mesh, in_specs=(row_spec,) + (weight_spec,) * 6 + (row_spec,),
                         out_specs=(row_spec, row_spec) + (weight_spec,) * 6, check_vma=False)
```

```python
import functools

import jax
import jax.numpy as jnp
from jax import lax
from jax.experimental import pallas as pl
from jax.experimental.pallas import tpu as pltpu
from jax.sharding import PartitionSpec as P


CHIP, CORE = AXES = ("sub", "fsdp")
EPS = 1e-6
MASK_FILL = -1e30
GELU_A = (2.0 / 3.141592653589793) ** 0.5
GELU_B = 0.044715
CHIPS = 4
CORES = 2
QUERY_BLOCK = 256
TOKEN_TILE = 512
ROW_TILE = 48
FLIP_TILE = 256
WIDTH_TILE = 512
NEIGHBOURS = (1, 2)


def rms_norm(values):
    return values * lax.rsqrt(jnp.mean(values * values, axis=-1, keepdims=True) + EPS)


def norm_bf16(x_loc):
    return rms_norm(x_loc.astype(jnp.float32)).astype(jnp.bfloat16)


def norm_back(x_loc, grad_norm):
    _, pull_back = jax.vjp(rms_norm, x_loc.astype(jnp.float32))
    return pull_back(grad_norm)[0]


def dot(left, right, contract):
    return lax.dot_general(left, right, (contract, ((), ())), preferred_element_type=jnp.float32)


def times(left, right):
    return dot(left, right, ((1,), (0,)))


def times_flipped(left, right):
    return dot(left, right, ((1,), (1,)))


def swap(value):
    return lax.ppermute(value, CORE, [(0, 1), (1, 0)])


def hop(value, step):
    return lax.ppermute(value, CHIP, [(chip, chip ^ step) for chip in range(CHIPS)])


def by_core(core, mine, other):
    return jnp.where(core == 0, mine, other), jnp.where(core == 0, other, mine)


def to_columns(core, keep, send):
    first, second = by_core(core, keep, swap(send))
    return jnp.concatenate([first, second], axis=0)


def to_rows(core, grad):
    rows = grad.shape[0] // CORES
    grad = grad.reshape((CORES, rows) + grad.shape[1:])
    keep = lax.dynamic_index_in_dim(grad, core, 0, keepdims=False)
    return keep, swap(lax.dynamic_index_in_dim(grad, 1 - core, 0, keepdims=False))


def heads_kernel(place_ref, mine_ref, other_ref, *refs):
    outs = refs[-4:]
    head = outs[0].shape[3]
    for part in range(CORES):
        mine, other = mine_ref[...], other_ref[...]
        cols = jnp.where(place_ref[1] == part, mine, other)
        start = 0
        for out in outs:
            count = out.shape[2] // CORES
            for i in range(count):
                out[0, :, part * count + i, :] = cols[:, start:start + head]
                start += head


def place_heads(place, layer, shapes, earlier, mine, other):
    rows, cols = mine.shape
    anywhere = [pl.BlockSpec(memory_space=pl.ANY)] * len(earlier)
    return pl.pallas_call(
        heads_kernel,
        grid_spec=pltpu.PrefetchScalarGridSpec(
            num_scalar_prefetch=1,
            grid=(rows // ROW_TILE,),
            in_specs=[pl.BlockSpec((ROW_TILE, cols), lambda i, p: (i, 0))] * CORES + anywhere,
            out_specs=[pl.BlockSpec((1, ROW_TILE) + shape[2:], lambda i, p: (layer, i, 0, 0)) for shape in shapes],
        ),
        out_shape=[jax.ShapeDtypeStruct(shape, jnp.float32) for shape in shapes],
        input_output_aliases={3 + i: i for i in range(len(earlier))},
        cost_estimate=pl.CostEstimate(flops=2_000_000_000, bytes_accessed=0, transcendentals=0),
        name="place_heads",
    )(place, mine, other, *earlier)


def blank_kernel(_, out_ref):
    del out_ref


def blank(piece):
    anywhere = pl.BlockSpec(memory_space=pl.ANY)
    return pl.pallas_call(blank_kernel, in_specs=[anywhere], out_specs=anywhere, name="blank",
                          out_shape=jax.ShapeDtypeStruct((CHIPS,) + piece.shape, piece.dtype))(piece)


def gather_weight(chip, piece):
    half = piece.shape[0] // 2
    near = [hop(piece, step) for step in NEIGHBOURS]
    opposite = [hop(near[0][:half], NEIGHBOURS[1]),
                hop(near[1][half:], NEIGHBOURS[0])]
    full = blank(piece)
    parts = [(piece, 0, 0), (near[0], NEIGHBOURS[0], 0), (near[1], NEIGHBOURS[1], 0),
             (opposite[0], sum(NEIGHBOURS), 0), (opposite[1], sum(NEIGHBOURS), half)]
    for part, step, row in parts:
        full = lax.dynamic_update_slice(full, part[None], (chip ^ step, row, 0))
    return full.reshape(-1, piece.shape[1])


def gather_rows(value):
    return functools.partial(lax.all_gather, axis=0, tiled=True)(value, AXES)


def scatter_sum(grad_full):
    return lax.psum_scatter(grad_full, CHIP, scatter_dimension=0, tiled=True)


def both_halves(left, right, rows, product):
    other = swap(product(left[rows:], right))
    own = lax.optimization_barrier(product(left[:rows], right))
    return own + other


def pair_rows(value):
    return jnp.concatenate([value, swap(value)], axis=0)


def causal_blocks(seq):
    return [(start, start + QUERY_BLOCK) for start in range(0, seq, QUERY_BLOCK)]


def probabilities(k_blk, q_blk, scale):
    scores = dot(k_blk, q_blk, ((1,), (1,))) * scale
    keys, queries = scores.shape
    key = lax.broadcasted_iota(jnp.int32, (queries, queries), 0)
    query = lax.broadcasted_iota(jnp.int32, (queries, queries), 1)
    last = jnp.where(key <= query, scores[keys - queries:], MASK_FILL)
    scores = last if keys == queries else jnp.concatenate([scores[:keys - queries], last], axis=0)
    powers = jnp.exp(scores - jnp.max(scores, axis=0, keepdims=True))
    return powers * (1.0 / jnp.sum(powers, axis=0, keepdims=True))


def attn_fwd_kernel(q_width, head, qkv_ref, o_ref):
    seq = qkv_ref.shape[0]
    k_all = qkv_ref[:, q_width:q_width + head]
    v_flip = jnp.transpose(qkv_ref[:, q_width + head:].astype(jnp.float32)).astype(jnp.bfloat16)
    for col in range(0, q_width, head):
        for start, end in causal_blocks(seq):
            probs = probabilities(k_all[:end], qkv_ref[start:end, col:col + head], head ** -0.5)
            o_flip = dot(v_flip[:, :end], probs.astype(jnp.bfloat16), ((1,), (0,)))
            o_ref[start:end, col:col + head] = jnp.transpose(o_flip).astype(jnp.bfloat16)


def attn_bwd_kernel(q_width, head, qkv_ref, d_o_ref, out_ref, d_k_ref, d_v_ref):
    seq = qkv_ref.shape[0]
    scale = head ** -0.5
    k_all = qkv_ref[:, q_width:q_width + head]
    v_all = qkv_ref[:, q_width + head:]
    k_flip = jnp.transpose(k_all.astype(jnp.float32)).astype(jnp.bfloat16)
    d_k_ref[...] = jnp.zeros_like(d_k_ref)
    d_v_ref[...] = jnp.zeros_like(d_v_ref)
    for col in range(0, q_width, head):
        for start, end in causal_blocks(seq):
            q_blk = qkv_ref[start:end, col:col + head]
            d_o_blk = d_o_ref[start:end, col:col + head]
            probs = probabilities(k_all[:end], q_blk, scale)
            d_p = dot(v_all[:end], d_o_blk, ((1,), (1,)))
            d_v_ref[:end] += dot(probs.astype(jnp.bfloat16), d_o_blk, ((1,), (0,)))
            d_s = probs * (d_p - jnp.sum(probs * d_p, axis=0, keepdims=True))
            d_s = (d_s * scale).astype(jnp.bfloat16)
            d_k_ref[:end] += dot(d_s, q_blk, ((1,), (0,)))
            d_q_flip = dot(k_flip[:, :end], d_s, ((1,), (0,)))
            out_ref[start:end, col:col + head] = jnp.transpose(d_q_flip).astype(jnp.bfloat16)
    out_ref[:, q_width:q_width + head] = d_k_ref[...].astype(jnp.bfloat16)
    out_ref[:, q_width + head:] = d_v_ref[...].astype(jnp.bfloat16)


def by_sequence(kernel, seq, q_width, head, args, width, scratch, flops):
    rows = args[0].shape[0]
    return pl.pallas_call(
        functools.partial(kernel, q_width, head),
        grid=(rows // seq,),
        in_specs=[pl.BlockSpec((seq, arg.shape[1]), lambda i: (i, 0)) for arg in args],
        out_specs=pl.BlockSpec((seq, width), lambda i: (i, 0)),
        out_shape=jax.ShapeDtypeStruct((rows, width), jnp.bfloat16),
        scratch_shapes=[pltpu.VMEM((seq, head), jnp.float32)] * scratch,
        cost_estimate=pl.CostEstimate(flops=flops, bytes_accessed=0, transcendentals=0),
    )(*args)


def attn_forward(x_own, weight, q_width, head, seq):
    normed = pair_rows(norm_bf16(x_own))
    qkv = times(normed, weight[:, :q_width + 2 * head]).astype(jnp.bfloat16)
    o_act = by_sequence(attn_fwd_kernel, seq, q_width, head, (qkv,), q_width, 0,
                  20_000_000_000)
    proj = both_halves(o_act, weight[:, q_width + 2 * head:], x_own.shape[0], times_flipped)
    y_own = (x_own.astype(jnp.float32) + proj).astype(jnp.bfloat16)
    return y_own, (x_own, normed, qkv, o_act)


def attn_grads_kernel(norm_ref, d_qkv_ref, grad_ref, o_ref, out_ref):
    width = d_qkv_ref.shape[1]
    out_ref[:, :width] = dot(norm_ref[...], d_qkv_ref[...], ((0,), (0,)))
    out_ref[:, width:] = dot(grad_ref[...], o_ref[...], ((0,), (0,)))


def attn_grads(normed, d_qkv, grad_y, o_act):
    rows, width = normed.shape
    cols = d_qkv.shape[1] + o_act.shape[1]
    piece = pl.BlockSpec((rows, WIDTH_TILE), lambda i: (0, i))
    whole = [pl.BlockSpec(arg.shape, lambda i: (0, 0), pipeline_mode=pl.Buffered(1)) for arg in (d_qkv, o_act)]
    return pl.pallas_call(
        attn_grads_kernel,
        grid=(width // WIDTH_TILE,),
        in_specs=[piece, whole[0], piece, whole[1]],
        out_specs=pl.BlockSpec((WIDTH_TILE, cols), lambda i: (i, 0)),
        out_shape=jax.ShapeDtypeStruct((width, cols), jnp.float32),
        cost_estimate=pl.CostEstimate(flops=2 * rows * width * cols, bytes_accessed=0, transcendentals=0),
        name="attn_grads",
    )(normed, d_qkv, grad_y, o_act)


def attn_backward(saved, weight, q_width, head, seq, grad_own):
    x_own, normed, qkv, o_act = saved
    grad_y = pair_rows(grad_own)
    d_o = times(grad_y, weight[:, q_width + 2 * head:]).astype(jnp.bfloat16)
    d_qkv = by_sequence(attn_bwd_kernel, seq, q_width, head, (qkv, d_o), qkv.shape[1], 2,
                  40_000_000_000)
    d_norm = both_halves(d_qkv, weight[:, :q_width + 2 * head], grad_own.shape[0], times_flipped)
    grad_x = (grad_own.astype(jnp.float32) + norm_back(x_own, d_norm)).astype(jnp.bfloat16)
    return grad_x, attn_grads(normed, d_qkv, grad_y, o_act)


def gelu_parts(hidden):
    square = hidden * hidden
    half = 0.5 + 0.5 * jnp.tanh(hidden * (GELU_A + GELU_A * GELU_B * square))
    value = hidden * half
    slope = half + value * (1.0 - half) * (2.0 * GELU_A + 6.0 * GELU_A * GELU_B * square)
    return value.astype(jnp.bfloat16), slope


def mlp_hidden(normed, up_weight):
    return lax.optimization_barrier(gelu_parts(times(normed, up_weight)))


def mlp_output(x_own, gelu_act, down_weight):
    proj = both_halves(gelu_act, down_weight, x_own.shape[0], times)
    return (x_own.astype(jnp.float32) + proj).astype(jnp.bfloat16)


def mlp_backward(x_own, slope, up_weight, down_weight, grad_own):
    grad_act = times_flipped(pair_rows(grad_own), down_weight)
    d_hid = (grad_act * slope).astype(jnp.bfloat16)
    d_norm = both_halves(d_hid, up_weight, grad_own.shape[0], times_flipped)
    return (grad_own.astype(jnp.float32) + norm_back(x_own, d_norm)).astype(jnp.bfloat16)


def mlp_grads_kernel(place_ref, up_ref, down_ref, norm_ref, grad_ref, *rest):
    d_down_ref, parts, d_up_ref, flip_ref = rest[-2 * CHIPS - 3], rest[-2 * CHIPS - 2:-2], rest[-2], rest[-1]
    step = pl.program_id(0)
    normed, grad_y = norm_ref[...], grad_ref[...]

    @pl.when(step == 0)
    def _():
        d_down_ref[...] = jnp.zeros_like(d_down_ref)
        d_up_ref[...] = jnp.zeros_like(d_up_ref)

    gelu_act, slope = gelu_parts(dot(up_ref[...], normed, ((1,), (1,))))
    d_hid = (dot(down_ref[...], grad_y, ((1,), (1,))) * slope).astype(jnp.bfloat16)
    d_down_ref[0] += dot(gelu_act, grad_y, ((1,), (0,)))
    d_up_ref[...] += dot(d_hid, normed, ((1,), (0,)))

    @pl.when(step == pl.num_programs(0) - 1)
    def _():
        rows = parts[0].shape[0]
        for i in range(CHIPS):
            start = pl.multiple_of((place_ref[0] ^ i) * (CORES * rows), CORES * rows)
            flip_ref[...] = jnp.transpose(d_up_ref[:, pl.ds(start, CORES * rows)])
            for j in range(CORES):
                start = pl.multiple_of((place_ref[1] ^ j) * rows, rows)
                parts[CORES * i + j][...] = flip_ref[pl.ds(start, rows), :]


def mlp_weight_grads(place, layer, pairs, earlier, up_flip, down_block, norms, grads):
    block, width = down_block.shape
    rows = width // (CHIPS * CORES)
    once = pl.Buffered(1)
    whole = pl.BlockSpec((block, width), lambda i, p: (0, 0), pipeline_mode=once)
    tokens = pl.BlockSpec((TOKEN_TILE, width), lambda i, p: (i, 0))
    part = pl.BlockSpec((rows, block), lambda i, p: (0, 0), pipeline_mode=once)
    args = [place, up_flip, down_block, norms, grads, *earlier]
    outs = pl.pallas_call(
        mlp_grads_kernel,
        grid_spec=pltpu.PrefetchScalarGridSpec(
            num_scalar_prefetch=1,
            grid=(norms.shape[0] // TOKEN_TILE,),
            in_specs=[whole, whole, tokens, tokens] + [pl.BlockSpec(memory_space=pl.ANY)] * len(earlier),
            out_specs=[pl.BlockSpec((1, block, width), lambda i, p: (layer, 0, 0), pipeline_mode=once)]
            + [part] * (CHIPS * CORES),
            scratch_shapes=[pltpu.VMEM((block, width), jnp.float32), pltpu.VMEM((CORES * rows, block), jnp.float32)],
        ),
        out_shape=[jax.ShapeDtypeStruct((pairs, block, width), jnp.float32)]
        + [jax.ShapeDtypeStruct((rows, block), jnp.float32)] * (CHIPS * CORES),
        input_output_aliases={len(args) - 1: 0} if earlier else {},
        compiler_params=pltpu.CompilerParams(vmem_limit_bytes=60 * 1024 * 1024),
        cost_estimate=pl.CostEstimate(flops=8 * norms.shape[0] * block * width, bytes_accessed=0,
                                      transcendentals=0),
        name="mlp_grads",
    )(*args)
    return outs[0], outs[1:]


def exchange(parts):
    devices = range(CHIPS * CORES)
    return [lax.ppermute(part, AXES, [(d, d ^ i) for d in devices]) if i else part for i, part in enumerate(parts)]


def assemble_kernel(place_ref, *refs):
    parts, out_ref = [ref[...] for ref in refs[:CHIPS * CORES]], refs[-1]
    for bit in range(3):
        swapped = ((place_ref[0] * CORES + place_ref[1]) >> bit) % 2 == 1
        parts = [jnp.where(swapped, parts[i ^ (1 << bit)], part) for i, part in enumerate(parts)]
    for i, part in enumerate(parts):
        out_ref[0, :, i * part.shape[1]:(i + 1) * part.shape[1]] = part


def assemble(place, layer, pairs, earlier, parts):
    rows, block = parts[0].shape
    out_width = block * len(parts)
    return pl.pallas_call(
        assemble_kernel,
        grid_spec=pltpu.PrefetchScalarGridSpec(
            num_scalar_prefetch=1,
            grid=(rows // ROW_TILE,),
            in_specs=[pl.BlockSpec((ROW_TILE, block), lambda i, p: (i, 0))] * len(parts)
            + [pl.BlockSpec(memory_space=pl.ANY)] * len(earlier),
            out_specs=pl.BlockSpec((1, ROW_TILE, out_width), lambda i, p: (layer, i, 0)),
        ),
        out_shape=jax.ShapeDtypeStruct((pairs, rows, out_width), jnp.float32),
        input_output_aliases={1 + len(parts): 0} if earlier else {},
        cost_estimate=pl.CostEstimate(flops=5_000_000_000, bytes_accessed=0, transcendentals=0),
        name="assemble",
    )(place, *parts, *earlier)


def split_kernel(place_ref, rows_ref, keep_ref, send_ref):
    block = rows_ref.shape[2] // (CHIPS * CORES)
    for i in range(CHIPS):
        pair = [rows_ref[0, :, (CORES * i + j) * block:(CORES * i + j + 1) * block] for j in range(CORES)]
        cols = slice(i * block, (i + 1) * block)
        keep_ref[:, cols] = jnp.where(place_ref[1] == 0, pair[0], pair[1])
        send_ref[:, cols] = jnp.where(place_ref[1] == 0, pair[1], pair[0])


def split_columns(place, layer, weight):
    rows, cols = weight.shape[1:]
    half = jax.ShapeDtypeStruct((rows, cols // CORES), weight.dtype)
    return pl.pallas_call(
        split_kernel,
        grid_spec=pltpu.PrefetchScalarGridSpec(
            num_scalar_prefetch=1,
            grid=(rows // ROW_TILE,),
            in_specs=[pl.BlockSpec((1, ROW_TILE, cols), lambda i, p: (layer, i, 0))],
            out_specs=[pl.BlockSpec((ROW_TILE, cols // CORES), lambda i, p: (i, 0))] * CORES,
        ),
        out_shape=[half] * CORES,
        cost_estimate=pl.CostEstimate(flops=5_000_000_000, bytes_accessed=0, transcendentals=0),
        name="split",
    )(place, weight)


def flip_kernel(place_ref, up_ref, out_ref):
    block = out_ref.shape[0]
    for i in range(CHIPS):
        @pl.when(place_ref[0] == i)
        def _():
            out_ref[...] = jnp.transpose(up_ref[:, i * block:(i + 1) * block])


def flip(place, up_weight):
    width, cols = up_weight.shape
    return pl.pallas_call(
        flip_kernel,
        grid_spec=pltpu.PrefetchScalarGridSpec(
            num_scalar_prefetch=1,
            grid=(width // FLIP_TILE,),
            in_specs=[pl.BlockSpec((FLIP_TILE, cols), lambda i, p: (i, 0))],
            out_specs=pl.BlockSpec((cols // CHIPS, FLIP_TILE), lambda i, p: (0, i)),
        ),
        out_shape=jax.ShapeDtypeStruct((cols // CHIPS, width), jnp.bfloat16),
        cost_estimate=pl.CostEstimate(flops=5_000_000_000, bytes_accessed=0, transcendentals=0),
        name="flip",
    )(place, up_weight)


def solution(mesh):
    row_spec = P(AXES)
    weight_spec = P(None, AXES)

    def body(x_loc, w_q, w_k, w_v, w_o, w_up, w_down, grad_out):
        core = lax.axis_index(CORE)
        chip = lax.axis_index(CHIP)
        pairs, shard, heads, head = w_q.shape
        seqs, seq, width = x_loc.shape
        q_width = heads // CORES * head

        place = jnp.stack([chip, core]).astype(jnp.int32)

        def attn_piece(layer, core):
            halves = []
            for part in range(CORES):
                cols = [w[layer].reshape(shard, CORES, -1)[:, part] for w in (w_q, w_k, w_v, w_o)]
                halves.append(jnp.concatenate(cols, axis=1))
            return to_columns(core, *by_core(core, *halves))

        def up_piece(layer, core, place):
            return to_columns(core, *split_columns(place, layer, w_up))

        attn_full, up_full, down_full, up_flip = [], [], [], []

        def gather_weights(layer, core, place):
            attn_full.append(gather_weight(chip, attn_piece(layer, core)))
            up_full.append(gather_weight(chip, up_piece(layer, core, place)))
            down_full.append(gather_weight(chip, w_down[layer]))
            up_flip.append(flip(place, up_full[layer]))

        gather_weights(0, core, place)
        carry_x = x_loc.reshape(seqs * seq, width)
        grad_x = grad_out.reshape(seqs * seq, width)
        attn_saved, mlp_saved, d_up, d_down = [], [], [], []

        def weight_grads(layer, norms, grads, d_down):
            down, parts = mlp_weight_grads(place, layer, pairs, d_down, up_flip[layer], w_down[layer], norms, grads)
            return exchange(parts), [down]

        for layer in range(pairs):
            x_own, saved = attn_forward(carry_x, attn_full[layer], q_width, head, seq)
            attn_saved.append(saved)
            if layer < pairs - 1:
                x_own, *later = lax.optimization_barrier((x_own, core, place))
                gather_weights(layer + 1, *later)
            n_own = norm_bf16(x_own)
            gelu_act, slope = mlp_hidden(pair_rows(n_own), up_full[layer])
            norms = gather_rows(n_own)
            if layer == pairs - 1:
                parts, d_down = weight_grads(layer, norms, gather_rows(grad_x), d_down)
            mlp_saved.append((x_own, norms, slope))
            if layer < pairs - 1:
                carry_x = mlp_output(x_own, gelu_act, down_full[layer])
        last = (x_own, gelu_act, down_full[-1])
        d_heads, head_shapes = [], [weight.shape for weight in (w_q, w_k, w_v, w_o)]
        for layer in reversed(range(pairs)):
            x_own, norms, slope = mlp_saved[layer]
            if layer < pairs - 1:
                parts, d_down = weight_grads(layer, norms, gather_rows(grad_x), d_down)
            d_up = [assemble(place, layer, pairs, d_up, parts)]
            grad_x = mlp_backward(x_own, slope, up_full[layer], down_full[layer], grad_x)
            grad_x, d_attn = attn_backward(attn_saved[layer], attn_full[layer], q_width, head, seq, grad_x)
            parts = to_rows(core, scatter_sum(d_attn))
            d_heads = place_heads(place, layer, head_shapes, d_heads, *parts)
        last, d_down = lax.optimization_barrier((last, d_down))
        y_loc = mlp_output(*last).reshape(x_loc.shape)
        return (y_loc, grad_x.reshape(x_loc.shape)) + (*d_heads, d_up[0], d_down[0])

    return jax.shard_map(body, mesh=mesh, in_specs=(row_spec,) + (weight_spec,) * 6 + (row_spec,),
                         out_specs=(row_spec, row_spec) + (weight_spec,) * 6, check_vma=False)
```

```python
import functools

import jax
import jax.numpy as jnp
from jax import lax
from jax.experimental import pallas as pl
from jax.experimental.pallas import tpu as pltpu
from jax.sharding import PartitionSpec as P


CHIP, CORE = AXES = ("sub", "fsdp")
EPS = 1e-6
MASK_FILL = -1e30
GELU_A = (2.0 / 3.141592653589793) ** 0.5
GELU_B = 0.044715
CHIPS = 4
CORES = 2
QUERY_BLOCK = 256
TOKEN_TILE = 512
ROW_TILE = 48
FLIP_TILE = 256
WIDTH_TILE = 512
NEIGHBOURS = (1, 2)
BY_HEAD = (True, False, False, True)


def rms_norm(values):
    return values * lax.rsqrt(jnp.mean(values * values, axis=-1, keepdims=True) + EPS)


def norm_bf16(x_loc):
    return rms_norm(x_loc.astype(jnp.float32)).astype(jnp.bfloat16)


def norm_back(x_loc, grad_norm):
    _, pull_back = jax.vjp(rms_norm, x_loc.astype(jnp.float32))
    return pull_back(grad_norm)[0]


def dot(left, right, contract):
    return lax.dot_general(left, right, (contract, ((), ())), preferred_element_type=jnp.float32)


def times(left, right):
    return dot(left, right, ((1,), (0,)))


def times_flipped(left, right):
    return dot(left, right, ((1,), (1,)))


def swap(value):
    return lax.ppermute(value, CORE, [(0, 1), (1, 0)])


def hop(value, step):
    return lax.ppermute(value, CHIP, [(chip, chip ^ step) for chip in range(CHIPS)])


def by_core(core, mine, other):
    return jnp.where(core == 0, mine, other), jnp.where(core == 0, other, mine)


def to_columns(core, keep, send):
    first, second = by_core(core, keep, swap(send))
    return jnp.concatenate([first, second], axis=0)


def to_rows(core, grad):
    rows = grad.shape[0] // CORES
    grad = grad.reshape((CORES, rows) + grad.shape[1:])
    keep = lax.dynamic_index_in_dim(grad, core, 0, keepdims=False)
    return keep, swap(lax.dynamic_index_in_dim(grad, 1 - core, 0, keepdims=False))


def heads_kernel(place_ref, mine_ref, other_ref, *refs):
    outs = refs[-4:]
    head = outs[0].shape[3]
    for part in range(CORES):
        cols = jnp.where(place_ref[1] == part, mine_ref[...], other_ref[...])
        start = 0
        for out, by_head in zip(outs, BY_HEAD):
            count = out.shape[1 if by_head else 2] // CORES
            for i in range(part * count, (part + 1) * count):
                if by_head:
                    out[0, i] = cols[:, start:start + head]
                else:
                    out[0, :, i, :] = cols[:, start:start + head]
                start += head


def flip_heads(weight):
    return weight.transpose(0, 2, 1, 3)


def heads_specs(shapes, layer):
    return [pl.BlockSpec((1, shape[1], ROW_TILE, shape[3]), lambda i, p: (layer, 0, i, 0)) if by_head
            else pl.BlockSpec((1, ROW_TILE) + shape[2:], lambda i, p: (layer, i, 0, 0))
            for shape, by_head in zip(shapes, BY_HEAD)]


def place_heads(place, layer, shapes, earlier, mine, other):
    rows, cols = mine.shape
    anywhere = [pl.BlockSpec(memory_space=pl.ANY)] * len(earlier)
    return pl.pallas_call(
        heads_kernel,
        grid_spec=pltpu.PrefetchScalarGridSpec(
            num_scalar_prefetch=1,
            grid=(rows // ROW_TILE,),
            in_specs=[pl.BlockSpec((ROW_TILE, cols), lambda i, p: (i, 0))] * CORES + anywhere,
            out_specs=heads_specs(shapes, layer),
        ),
        out_shape=[jax.ShapeDtypeStruct(shape, jnp.float32) for shape in shapes],
        input_output_aliases={3 + i: i for i in range(len(earlier))},
        cost_estimate=pl.CostEstimate(flops=2_000_000_000, bytes_accessed=0, transcendentals=0),
        name="place_heads",
    )(place, mine, other, *earlier)


def pack_kernel(place_ref, *refs):
    weights, outs = refs[:4], refs[4:]
    head = weights[0].shape[3]
    start = 0
    for weight, by_head in zip(weights, BY_HEAD):
        count = weight.shape[1 if by_head else 2] // CORES
        for i in range(count):
            pair = [weight[0, i + part * count] if by_head else weight[0, :, i + part * count, :] for part in range(CORES)]
            for j, out in enumerate(outs):
                out[:, start:start + head] = jnp.where(place_ref[1] == j, pair[0], pair[1])
            start += head


def pack_heads(place, layer, weights):
    rows, head = weights[1].shape[1], weights[1].shape[3]
    cols = sum(weight.shape[1 if by_head else 2] for weight, by_head in zip(weights, BY_HEAD)) // CORES * head
    half = jax.ShapeDtypeStruct((rows, cols), weights[0].dtype)
    return pl.pallas_call(
        pack_kernel,
        grid_spec=pltpu.PrefetchScalarGridSpec(
            num_scalar_prefetch=1,
            grid=(rows // ROW_TILE,),
            in_specs=heads_specs([weight.shape for weight in weights], layer),
            out_specs=[pl.BlockSpec((ROW_TILE, cols), lambda i, p: (i, 0))] * CORES,
        ),
        out_shape=[half] * CORES,
        cost_estimate=pl.CostEstimate(flops=2_000_000_000, bytes_accessed=0, transcendentals=0),
        name="pack",
    )(place, *weights)


def blank_kernel(_, out_ref):
    del out_ref


def blank(piece):
    anywhere = pl.BlockSpec(memory_space=pl.ANY)
    return pl.pallas_call(blank_kernel, in_specs=[anywhere], out_specs=anywhere, name="blank",
                          out_shape=jax.ShapeDtypeStruct((CHIPS,) + piece.shape, piece.dtype))(piece)


def gather_weight(chip, piece):
    half = piece.shape[0] // 2
    near = [hop(piece, step) for step in NEIGHBOURS]
    opposite = [hop(near[0][:half], NEIGHBOURS[1]),
                hop(near[1][half:], NEIGHBOURS[0])]
    full = blank(piece)
    parts = [(piece, 0, 0), (near[0], NEIGHBOURS[0], 0), (near[1], NEIGHBOURS[1], 0),
             (opposite[0], sum(NEIGHBOURS), 0), (opposite[1], sum(NEIGHBOURS), half)]
    for part, step, row in parts:
        full = lax.dynamic_update_slice(full, part[None], (chip ^ step, row, 0))
    return full.reshape(-1, piece.shape[1])


def gather_rows(value):
    return functools.partial(lax.all_gather, axis=0, tiled=True)(value, AXES)


def scatter_sum(grad_full):
    return lax.psum_scatter(grad_full, CHIP, scatter_dimension=0, tiled=True)


def both_halves(left, right, rows, product):
    other = swap(product(left[rows:], right))
    own = lax.optimization_barrier(product(left[:rows], right))
    return own + other


def pair_rows(value):
    return jnp.concatenate([value, swap(value)], axis=0)


def causal_blocks(seq):
    return [(start, start + QUERY_BLOCK) for start in range(0, seq, QUERY_BLOCK)]


def probabilities(k_blk, q_blk, scale):
    scores = dot(k_blk, q_blk, ((1,), (1,))) * scale
    keys, queries = scores.shape
    key = lax.broadcasted_iota(jnp.int32, (queries, queries), 0)
    query = lax.broadcasted_iota(jnp.int32, (queries, queries), 1)
    last = jnp.where(key <= query, scores[keys - queries:], MASK_FILL)
    scores = last if keys == queries else jnp.concatenate([scores[:keys - queries], last], axis=0)
    powers = jnp.exp(scores - jnp.max(scores, axis=0, keepdims=True))
    return powers * (1.0 / jnp.sum(powers, axis=0, keepdims=True))


def attn_fwd_kernel(q_width, head, qkv_ref, o_ref):
    seq = qkv_ref.shape[0]
    k_all = qkv_ref[:, q_width:q_width + head]
    v_flip = jnp.transpose(qkv_ref[:, q_width + head:].astype(jnp.float32)).astype(jnp.bfloat16)
    for col in range(0, q_width, head):
        for start, end in causal_blocks(seq):
            probs = probabilities(k_all[:end], qkv_ref[start:end, col:col + head], head ** -0.5)
            o_flip = dot(v_flip[:, :end], probs.astype(jnp.bfloat16), ((1,), (0,)))
            o_ref[start:end, col:col + head] = jnp.transpose(o_flip).astype(jnp.bfloat16)


def attn_bwd_kernel(q_width, head, qkv_ref, d_o_ref, out_ref, d_k_ref, d_v_ref):
    seq = qkv_ref.shape[0]
    scale = head ** -0.5
    k_all = qkv_ref[:, q_width:q_width + head]
    v_all = qkv_ref[:, q_width + head:]
    k_flip = jnp.transpose(k_all.astype(jnp.float32)).astype(jnp.bfloat16)
    d_k_ref[...] = jnp.zeros_like(d_k_ref)
    d_v_ref[...] = jnp.zeros_like(d_v_ref)
    for col in range(0, q_width, head):
        for start, end in causal_blocks(seq):
            q_blk = qkv_ref[start:end, col:col + head]
            d_o_blk = d_o_ref[start:end, col:col + head]
            probs = probabilities(k_all[:end], q_blk, scale)
            d_p = dot(v_all[:end], d_o_blk, ((1,), (1,)))
            d_v_ref[:end] += dot(probs.astype(jnp.bfloat16), d_o_blk, ((1,), (0,)))
            d_s = probs * (d_p - jnp.sum(probs * d_p, axis=0, keepdims=True))
            d_s = (d_s * scale).astype(jnp.bfloat16)
            d_k_ref[:end] += dot(d_s, q_blk, ((1,), (0,)))
            d_q_flip = dot(k_flip[:, :end], d_s, ((1,), (0,)))
            out_ref[start:end, col:col + head] = jnp.transpose(d_q_flip).astype(jnp.bfloat16)
    out_ref[:, q_width:q_width + head] = d_k_ref[...].astype(jnp.bfloat16)
    out_ref[:, q_width + head:] = d_v_ref[...].astype(jnp.bfloat16)


def by_sequence(kernel, seq, q_width, head, args, width, scratch, flops):
    rows = args[0].shape[0]
    return pl.pallas_call(
        functools.partial(kernel, q_width, head),
        grid=(rows // seq,),
        in_specs=[pl.BlockSpec((seq, arg.shape[1]), lambda i: (i, 0)) for arg in args],
        out_specs=pl.BlockSpec((seq, width), lambda i: (i, 0)),
        out_shape=jax.ShapeDtypeStruct((rows, width), jnp.bfloat16),
        scratch_shapes=[pltpu.VMEM((seq, head), jnp.float32)] * scratch,
        cost_estimate=pl.CostEstimate(flops=flops, bytes_accessed=0, transcendentals=0),
    )(*args)


def attn_forward(x_own, weight, q_width, head, seq):
    normed = pair_rows(norm_bf16(x_own))
    qkv = times(normed, weight[:, :q_width + 2 * head]).astype(jnp.bfloat16)
    o_act = by_sequence(attn_fwd_kernel, seq, q_width, head, (qkv,), q_width, 0,
                  20_000_000_000)
    proj = both_halves(o_act, weight[:, q_width + 2 * head:], x_own.shape[0], times_flipped)
    y_own = (x_own.astype(jnp.float32) + proj).astype(jnp.bfloat16)
    return y_own, (x_own, normed, qkv, o_act)


def attn_grads_kernel(norm_ref, d_qkv_ref, grad_ref, o_ref, out_ref):
    width = d_qkv_ref.shape[1]
    out_ref[:, :width] = dot(norm_ref[...], d_qkv_ref[...], ((0,), (0,)))
    out_ref[:, width:] = dot(grad_ref[...], o_ref[...], ((0,), (0,)))


def attn_grads(normed, d_qkv, grad_y, o_act):
    rows, width = normed.shape
    cols = d_qkv.shape[1] + o_act.shape[1]
    piece = pl.BlockSpec((rows, WIDTH_TILE), lambda i: (0, i))
    whole = [pl.BlockSpec(arg.shape, lambda i: (0, 0), pipeline_mode=pl.Buffered(1)) for arg in (d_qkv, o_act)]
    return pl.pallas_call(
        attn_grads_kernel,
        grid=(width // WIDTH_TILE,),
        in_specs=[piece, whole[0], piece, whole[1]],
        out_specs=pl.BlockSpec((WIDTH_TILE, cols), lambda i: (i, 0)),
        out_shape=jax.ShapeDtypeStruct((width, cols), jnp.float32),
        cost_estimate=pl.CostEstimate(flops=2 * rows * width * cols, bytes_accessed=0, transcendentals=0),
        name="attn_grads",
    )(normed, d_qkv, grad_y, o_act)


def attn_backward(saved, weight, q_width, head, seq, grad_own):
    x_own, normed, qkv, o_act = saved
    grad_y = pair_rows(grad_own)
    d_o = times(grad_y, weight[:, q_width + 2 * head:]).astype(jnp.bfloat16)
    d_qkv = by_sequence(attn_bwd_kernel, seq, q_width, head, (qkv, d_o), qkv.shape[1], 2,
                  40_000_000_000)
    d_norm = both_halves(d_qkv, weight[:, :q_width + 2 * head], grad_own.shape[0], times_flipped)
    grad_x = (grad_own.astype(jnp.float32) + norm_back(x_own, d_norm)).astype(jnp.bfloat16)
    return grad_x, attn_grads(normed, d_qkv, grad_y, o_act)


def gelu_parts(hidden):
    square = hidden * hidden
    half = 0.5 + 0.5 * jnp.tanh(hidden * (GELU_A + GELU_A * GELU_B * square))
    value = hidden * half
    slope = half + value * (1.0 - half) * (2.0 * GELU_A + 6.0 * GELU_A * GELU_B * square)
    return value.astype(jnp.bfloat16), slope


def mlp_hidden(normed, up_weight):
    return lax.optimization_barrier(gelu_parts(times(normed, up_weight)))


def mlp_output(x_own, gelu_act, down_weight):
    proj = both_halves(gelu_act, down_weight, x_own.shape[0], times)
    return (x_own.astype(jnp.float32) + proj).astype(jnp.bfloat16)


def mlp_backward(x_own, slope, up_weight, down_weight, grad_own):
    grad_act = times_flipped(pair_rows(grad_own), down_weight)
    d_hid = (grad_act * slope).astype(jnp.bfloat16)
    d_norm = both_halves(d_hid, up_weight, grad_own.shape[0], times_flipped)
    return (grad_own.astype(jnp.float32) + norm_back(x_own, d_norm)).astype(jnp.bfloat16)


def mlp_grads_kernel(place_ref, up_ref, down_ref, norm_ref, grad_ref, *rest):
    d_down_ref, parts, d_up_ref, flip_ref = rest[-2 * CHIPS - 3], rest[-2 * CHIPS - 2:-2], rest[-2], rest[-1]
    step = pl.program_id(0)
    normed, grad_y = norm_ref[...], grad_ref[...]

    @pl.when(step == 0)
    def _():
        d_down_ref[...] = jnp.zeros_like(d_down_ref)
        d_up_ref[...] = jnp.zeros_like(d_up_ref)

    gelu_act, slope = gelu_parts(dot(up_ref[...], normed, ((1,), (1,))))
    d_hid = (dot(down_ref[...], grad_y, ((1,), (1,))) * slope).astype(jnp.bfloat16)
    d_down_ref[0] += dot(gelu_act, grad_y, ((1,), (0,)))
    d_up_ref[...] += dot(d_hid, normed, ((1,), (0,)))

    @pl.when(step == pl.num_programs(0) - 1)
    def _():
        rows = parts[0].shape[0]
        for i in range(CHIPS):
            start = pl.multiple_of((place_ref[0] ^ i) * (CORES * rows), CORES * rows)
            flip_ref[...] = jnp.transpose(d_up_ref[:, pl.ds(start, CORES * rows)])
            for j in range(CORES):
                start = pl.multiple_of((place_ref[1] ^ j) * rows, rows)
                parts[CORES * i + j][...] = flip_ref[pl.ds(start, rows), :]


def mlp_weight_grads(place, layer, pairs, earlier, up_flip, down_block, tokens):
    block, width = down_block.shape
    rows = width // (CHIPS * CORES)
    once = pl.Buffered(1)
    whole = pl.BlockSpec((block, width), lambda i, p: (0, 0), pipeline_mode=once)
    tiles = tokens.shape[0] // (2 * CHIPS * CORES * TOKEN_TILE)
    norms, grads = [pl.BlockSpec((TOKEN_TILE, width), lambda i, p, k=k: (2 * tiles * (i // tiles) + k * tiles + i % tiles, 0))
                    for k in range(2)]
    part = pl.BlockSpec((rows, block), lambda i, p: (0, 0), pipeline_mode=once)
    args = [place, up_flip, down_block, tokens, tokens, *earlier]
    outs = pl.pallas_call(
        mlp_grads_kernel,
        grid_spec=pltpu.PrefetchScalarGridSpec(
            num_scalar_prefetch=1,
            grid=(tiles * CHIPS * CORES,),
            in_specs=[whole, whole, norms, grads] + [pl.BlockSpec(memory_space=pl.ANY)] * len(earlier),
            out_specs=[pl.BlockSpec((1, block, width), lambda i, p: (layer, 0, 0), pipeline_mode=once)]
            + [part] * (CHIPS * CORES),
            scratch_shapes=[pltpu.VMEM((block, width), jnp.float32), pltpu.VMEM((CORES * rows, block), jnp.float32)],
        ),
        out_shape=[jax.ShapeDtypeStruct((pairs, block, width), jnp.float32)]
        + [jax.ShapeDtypeStruct((rows, block), jnp.float32)] * (CHIPS * CORES),
        input_output_aliases={len(args) - 1: 0} if earlier else {},
        compiler_params=pltpu.CompilerParams(vmem_limit_bytes=60 * 1024 * 1024),
        cost_estimate=pl.CostEstimate(flops=4 * tokens.shape[0] * block * width, bytes_accessed=0,
                                      transcendentals=0),
        name="mlp_grads",
    )(*args)
    return outs[0], outs[1:]


def exchange(parts):
    devices = range(CHIPS * CORES)
    return [lax.ppermute(part, AXES, [(d, d ^ i) for d in devices]) if i else part for i, part in enumerate(parts)]


def assemble_kernel(place_ref, *refs):
    parts, out_ref = [ref[...] for ref in refs[:CHIPS * CORES]], refs[-1]
    for bit in range(3):
        swapped = ((place_ref[0] * CORES + place_ref[1]) >> bit) % 2 == 1
        parts = [jnp.where(swapped, parts[i ^ (1 << bit)], part) for i, part in enumerate(parts)]
    for i, part in enumerate(parts):
        out_ref[0, :, i * part.shape[1]:(i + 1) * part.shape[1]] = part


def assemble(place, layer, pairs, earlier, parts):
    rows, block = parts[0].shape
    out_width = block * len(parts)
    return pl.pallas_call(
        assemble_kernel,
        grid_spec=pltpu.PrefetchScalarGridSpec(
            num_scalar_prefetch=1,
            grid=(rows // ROW_TILE,),
            in_specs=[pl.BlockSpec((ROW_TILE, block), lambda i, p: (i, 0))] * len(parts)
            + [pl.BlockSpec(memory_space=pl.ANY)] * len(earlier),
            out_specs=pl.BlockSpec((1, ROW_TILE, out_width), lambda i, p: (layer, i, 0)),
        ),
        out_shape=jax.ShapeDtypeStruct((pairs, rows, out_width), jnp.float32),
        input_output_aliases={1 + len(parts): 0} if earlier else {},
        cost_estimate=pl.CostEstimate(flops=5_000_000_000, bytes_accessed=0, transcendentals=0),
        name="assemble",
    )(place, *parts, *earlier)


def split_kernel(place_ref, rows_ref, keep_ref, send_ref):
    block = rows_ref.shape[2] // (CHIPS * CORES)
    for i in range(CHIPS):
        pair = [rows_ref[0, :, (CORES * i + j) * block:(CORES * i + j + 1) * block] for j in range(CORES)]
        cols = slice(i * block, (i + 1) * block)
        keep_ref[:, cols] = jnp.where(place_ref[1] == 0, pair[0], pair[1])
        send_ref[:, cols] = jnp.where(place_ref[1] == 0, pair[1], pair[0])


def split_columns(place, layer, weight):
    rows, cols = weight.shape[1:]
    half = jax.ShapeDtypeStruct((rows, cols // CORES), weight.dtype)
    return pl.pallas_call(
        split_kernel,
        grid_spec=pltpu.PrefetchScalarGridSpec(
            num_scalar_prefetch=1,
            grid=(rows // ROW_TILE,),
            in_specs=[pl.BlockSpec((1, ROW_TILE, cols), lambda i, p: (layer, i, 0))],
            out_specs=[pl.BlockSpec((ROW_TILE, cols // CORES), lambda i, p: (i, 0))] * CORES,
        ),
        out_shape=[half] * CORES,
        cost_estimate=pl.CostEstimate(flops=5_000_000_000, bytes_accessed=0, transcendentals=0),
        name="split",
    )(place, weight)


def flip_kernel(place_ref, up_ref, out_ref):
    block = out_ref.shape[0]
    for i in range(CHIPS):
        @pl.when(place_ref[0] == i)
        def _():
            out_ref[...] = jnp.transpose(up_ref[:, i * block:(i + 1) * block])


def flip(place, up_weight):
    width, cols = up_weight.shape
    return pl.pallas_call(
        flip_kernel,
        grid_spec=pltpu.PrefetchScalarGridSpec(
            num_scalar_prefetch=1,
            grid=(width // FLIP_TILE,),
            in_specs=[pl.BlockSpec((FLIP_TILE, cols), lambda i, p: (i, 0))],
            out_specs=pl.BlockSpec((cols // CHIPS, FLIP_TILE), lambda i, p: (0, i)),
        ),
        out_shape=jax.ShapeDtypeStruct((cols // CHIPS, width), jnp.bfloat16),
        cost_estimate=pl.CostEstimate(flops=5_000_000_000, bytes_accessed=0, transcendentals=0),
        name="flip",
    )(place, up_weight)


def solution(mesh):
    row_spec = P(AXES)
    weight_spec = P(None, AXES)

    def body(x_loc, w_q, w_k, w_v, w_o, w_up, w_down, grad_out):
        core = lax.axis_index(CORE)
        chip = lax.axis_index(CHIP)
        pairs, _, heads, head = w_q.shape
        seqs, seq, width = x_loc.shape
        q_width = heads // CORES * head

        place = jnp.stack([chip, core]).astype(jnp.int32)

        heads_in = [flip_heads(w) if by_head else w for w, by_head in zip((w_q, w_k, w_v, w_o), BY_HEAD)]

        def attn_piece(layer, core, place):
            return to_columns(core, *pack_heads(place, layer, heads_in))

        def up_piece(layer, core, place):
            return to_columns(core, *split_columns(place, layer, w_up))

        attn_full, up_full, down_full, up_flip = [], [], [], []

        def gather_weights(layer, core, place):
            attn_full.append(gather_weight(chip, attn_piece(layer, core, place)))
            up_full.append(gather_weight(chip, up_piece(layer, core, place)))
            down_full.append(gather_weight(chip, lax.optimization_barrier(w_down[layer])))
            up_flip.append(flip(place, up_full[layer]))

        gather_weights(0, core, place)
        carry_x = x_loc.reshape(seqs * seq, width)
        grad_x = grad_out.reshape(seqs * seq, width)
        attn_saved, mlp_saved, d_up, d_down = [], [], [], []

        def weight_grads(layer, n_own, grad_own, d_down):
            tokens = gather_rows(jnp.concatenate([n_own, grad_own], axis=0))
            down, parts = mlp_weight_grads(place, layer, pairs, d_down, up_flip[layer], w_down[layer], tokens)
            return exchange(parts), [down]

        for layer in range(pairs):
            x_own, saved = attn_forward(carry_x, attn_full[layer], q_width, head, seq)
            attn_saved.append(saved)
            if layer < pairs - 1:
                x_own, *later = lax.optimization_barrier((x_own, core, place))
                gather_weights(layer + 1, *later)
            n_own = norm_bf16(x_own)
            gelu_act, slope = mlp_hidden(pair_rows(n_own), up_full[layer])
            if layer == pairs - 1:
                parts, d_down = weight_grads(layer, n_own, grad_x, d_down)
            mlp_saved.append((x_own, n_own, slope))
            if layer < pairs - 1:
                carry_x = mlp_output(x_own, gelu_act, down_full[layer])
        last = (x_own, gelu_act, down_full[-1])
        d_heads, head_shapes = [], [weight.shape for weight in heads_in]
        for layer in reversed(range(pairs)):
            x_own, n_own, slope = mlp_saved[layer]
            if layer < pairs - 1:
                parts, d_down = weight_grads(layer, n_own, grad_x, d_down)
            d_up = [assemble(place, layer, pairs, d_up, parts)]
            grad_x = mlp_backward(x_own, slope, up_full[layer], down_full[layer], grad_x)
            grad_x, d_attn = attn_backward(attn_saved[layer], attn_full[layer], q_width, head, seq, grad_x)
            parts = to_rows(core, scatter_sum(d_attn))
            d_heads = place_heads(place, layer, head_shapes, d_heads, *parts)
        heads_out = tuple(flip_heads(w) if by_head else w for w, by_head in zip(d_heads, BY_HEAD))
        last, d_down = lax.optimization_barrier((last, d_down))
        y_loc = mlp_output(*last).reshape(x_loc.shape)
        return (y_loc, grad_x.reshape(x_loc.shape)) + heads_out + (d_up[0], d_down[0])

    return jax.shard_map(body, mesh=mesh, in_specs=(row_spec,) + (weight_spec,) * 6 + (row_spec,),
                         out_specs=(row_spec, row_spec) + (weight_spec,) * 6, check_vma=False)
```

```python
import functools

import jax
import jax.numpy as jnp
from jax import lax
from jax.experimental import pallas as pl
from jax.experimental.pallas import tpu as pltpu
from jax.sharding import PartitionSpec as P


CHIP, CORE = AXES = ("sub", "fsdp")
EPS = 1e-6
MASK_FILL = -1e30
GELU_A = (2.0 / 3.141592653589793) ** 0.5
GELU_B = 0.044715
CHIPS = 4
CORES = 2
QUERY_BLOCK = 256
TOKEN_TILE = 512
ROW_TILE = 48
FLIP_TILE = 256
WIDTH_TILE = 512
NEIGHBOURS = (1, 2)
BY_HEAD = (True, False, False, True)


def rms_norm(values):
    return values * lax.rsqrt(jnp.mean(values * values, axis=-1, keepdims=True) + EPS)


def norm_bf16(x_loc):
    return rms_norm(x_loc.astype(jnp.float32)).astype(jnp.bfloat16)


def norm_back(x_loc, grad_norm):
    _, pull_back = jax.vjp(rms_norm, x_loc.astype(jnp.float32))
    return pull_back(grad_norm)[0]


def dot(left, right, contract):
    return lax.dot_general(left, right, (contract, ((), ())), preferred_element_type=jnp.float32)


def times(left, right):
    return dot(left, right, ((1,), (0,)))


def times_flipped(left, right):
    return dot(left, right, ((1,), (1,)))


def swap(value):
    return lax.ppermute(value, CORE, [(0, 1), (1, 0)])


def hop(value, step):
    return lax.ppermute(value, CHIP, [(chip, chip ^ step) for chip in range(CHIPS)])


def by_core(core, mine, other):
    return jnp.where(core == 0, mine, other), jnp.where(core == 0, other, mine)


def to_columns(core, keep, send):
    first, second = by_core(core, keep, swap(send))
    return jnp.concatenate([first, second], axis=0)


def to_rows(core, grad):
    rows = grad.shape[0] // CORES
    grad = grad.reshape((CORES, rows) + grad.shape[1:])
    keep = lax.dynamic_index_in_dim(grad, core, 0, keepdims=False)
    return keep, swap(lax.dynamic_index_in_dim(grad, 1 - core, 0, keepdims=False))


def heads_kernel(place_ref, mine_ref, other_ref, *refs):
    outs = refs[-4:]
    head = outs[0].shape[3]
    for part in range(CORES):
        cols = jnp.where(place_ref[1] == part, mine_ref[...], other_ref[...])
        start = 0
        for out, by_head in zip(outs, BY_HEAD):
            count = out.shape[1 if by_head else 2] // CORES
            for i in range(part * count, (part + 1) * count):
                if by_head:
                    out[0, i] = cols[:, start:start + head]
                else:
                    out[0, :, i, :] = cols[:, start:start + head]
                start += head


def flip_heads(weight):
    return weight.transpose(0, 2, 1, 3)


def heads_specs(shapes, layer):
    return [pl.BlockSpec((1, shape[1], ROW_TILE, shape[3]), lambda i, p: (layer, 0, i, 0)) if by_head
            else pl.BlockSpec((1, ROW_TILE) + shape[2:], lambda i, p: (layer, i, 0, 0))
            for shape, by_head in zip(shapes, BY_HEAD)]


def place_heads(place, layer, shapes, earlier, mine, other):
    rows, cols = mine.shape
    anywhere = [pl.BlockSpec(memory_space=pl.ANY)] * len(earlier)
    return pl.pallas_call(
        heads_kernel,
        grid_spec=pltpu.PrefetchScalarGridSpec(
            num_scalar_prefetch=1,
            grid=(rows // ROW_TILE,),
            in_specs=[pl.BlockSpec((ROW_TILE, cols), lambda i, p: (i, 0))] * CORES + anywhere,
            out_specs=heads_specs(shapes, layer),
        ),
        out_shape=[jax.ShapeDtypeStruct(shape, jnp.float32) for shape in shapes],
        input_output_aliases={3 + i: i for i in range(len(earlier))},
        cost_estimate=pl.CostEstimate(flops=2_000_000_000, bytes_accessed=0, transcendentals=0),
        name="place_heads",
    )(place, mine, other, *earlier)


def pack_kernel(place_ref, *refs):
    weights, outs = refs[:4], refs[4:]
    head = weights[0].shape[3]
    start = 0
    for weight, by_head in zip(weights, BY_HEAD):
        count = weight.shape[1 if by_head else 2] // CORES
        for i in range(count):
            pair = [weight[0, i + part * count] if by_head else weight[0, :, i + part * count, :] for part in range(CORES)]
            for j, out in enumerate(outs):
                out[:, start:start + head] = jnp.where(place_ref[1] == j, pair[0], pair[1])
            start += head


def pack_heads(place, layer, weights):
    rows, head = weights[1].shape[1], weights[1].shape[3]
    cols = sum(weight.shape[1 if by_head else 2] for weight, by_head in zip(weights, BY_HEAD)) // CORES * head
    half = jax.ShapeDtypeStruct((rows, cols), weights[0].dtype)
    return pl.pallas_call(
        pack_kernel,
        grid_spec=pltpu.PrefetchScalarGridSpec(
            num_scalar_prefetch=1,
            grid=(rows // ROW_TILE,),
            in_specs=heads_specs([weight.shape for weight in weights], layer),
            out_specs=[pl.BlockSpec((ROW_TILE, cols), lambda i, p: (i, 0))] * CORES,
        ),
        out_shape=[half] * CORES,
        cost_estimate=pl.CostEstimate(flops=2_000_000_000, bytes_accessed=0, transcendentals=0),
        name="pack",
    )(place, *weights)


def blank_kernel(_, out_ref):
    del out_ref


def blank(piece):
    anywhere = pl.BlockSpec(memory_space=pl.ANY)
    return pl.pallas_call(blank_kernel, in_specs=[anywhere], out_specs=anywhere, name="blank",
                          out_shape=jax.ShapeDtypeStruct((CHIPS,) + piece.shape, piece.dtype))(piece)


def gather_weight(chip, piece):
    half = piece.shape[0] // 2
    near = [hop(piece, step) for step in NEIGHBOURS]
    opposite = [hop(near[0][:half], NEIGHBOURS[1]),
                hop(near[1][half:], NEIGHBOURS[0])]
    full = blank(piece)
    parts = [(piece, 0, 0), (near[0], NEIGHBOURS[0], 0), (near[1], NEIGHBOURS[1], 0),
             (opposite[0], sum(NEIGHBOURS), 0), (opposite[1], sum(NEIGHBOURS), half)]
    for part, step, row in parts:
        full = lax.dynamic_update_slice(full, part[None], (chip ^ step, row, 0))
    return full.reshape(-1, piece.shape[1])


def gather_rows(value):
    return functools.partial(lax.all_gather, axis=0, tiled=True)(value, AXES)


def scatter_sum(grad_full):
    return lax.psum_scatter(grad_full, CHIP, scatter_dimension=0, tiled=True)


def both_halves(left, right, rows, product):
    other = swap(product(left[rows:], right))
    own = lax.optimization_barrier(product(left[:rows], right))
    return own + other


def halves_of(value):
    return value, swap(value)


def pair_rows(value):
    return jnp.concatenate(halves_of(value))


def causal_blocks(seq):
    return [(start, start + QUERY_BLOCK) for start in range(0, seq, QUERY_BLOCK)]


def probabilities(k_blk, q_blk, scale):
    scores = dot(k_blk, q_blk, ((1,), (1,))) * scale
    keys, queries = scores.shape
    key = lax.broadcasted_iota(jnp.int32, (queries, queries), 0)
    query = lax.broadcasted_iota(jnp.int32, (queries, queries), 1)
    last = jnp.where(key <= query, scores[keys - queries:], MASK_FILL)
    scores = last if keys == queries else jnp.concatenate([scores[:keys - queries], last], axis=0)
    powers = jnp.exp(scores - jnp.max(scores, axis=0, keepdims=True))
    return powers * (1.0 / jnp.sum(powers, axis=0, keepdims=True))


def attn_fwd_kernel(q_width, head, qkv_ref, o_ref):
    seq = qkv_ref.shape[0]
    k_all = qkv_ref[:, q_width:q_width + head]
    v_flip = jnp.transpose(qkv_ref[:, q_width + head:].astype(jnp.float32)).astype(jnp.bfloat16)
    for col in range(0, q_width, head):
        for start, end in causal_blocks(seq):
            probs = probabilities(k_all[:end], qkv_ref[start:end, col:col + head], head ** -0.5)
            o_flip = dot(v_flip[:, :end], probs.astype(jnp.bfloat16), ((1,), (0,)))
            o_ref[start:end, col:col + head] = jnp.transpose(o_flip).astype(jnp.bfloat16)


def attn_bwd_kernel(q_width, head, qkv_ref, d_o_ref, out_ref, d_k_ref, d_v_ref):
    seq = qkv_ref.shape[0]
    scale = head ** -0.5
    k_all = qkv_ref[:, q_width:q_width + head]
    v_all = qkv_ref[:, q_width + head:]
    k_flip = jnp.transpose(k_all.astype(jnp.float32)).astype(jnp.bfloat16)
    d_k_ref[...] = jnp.zeros_like(d_k_ref)
    d_v_ref[...] = jnp.zeros_like(d_v_ref)
    for col in range(0, q_width, head):
        for start, end in causal_blocks(seq):
            q_blk = qkv_ref[start:end, col:col + head]
            d_o_blk = d_o_ref[start:end, col:col + head]
            probs = probabilities(k_all[:end], q_blk, scale)
            d_p = dot(v_all[:end], d_o_blk, ((1,), (1,)))
            d_v_ref[:end] += dot(probs.astype(jnp.bfloat16), d_o_blk, ((1,), (0,)))
            d_s = probs * (d_p - jnp.sum(probs * d_p, axis=0, keepdims=True))
            d_s = (d_s * scale).astype(jnp.bfloat16)
            d_k_ref[:end] += dot(d_s, q_blk, ((1,), (0,)))
            d_q_flip = dot(k_flip[:, :end], d_s, ((1,), (0,)))
            out_ref[start:end, col:col + head] = jnp.transpose(d_q_flip).astype(jnp.bfloat16)
    out_ref[:, q_width:q_width + head] = d_k_ref[...].astype(jnp.bfloat16)
    out_ref[:, q_width + head:] = d_v_ref[...].astype(jnp.bfloat16)


def by_sequence(kernel, seq, q_width, head, args, width, scratch, flops):
    rows = args[0].shape[0]
    return pl.pallas_call(
        functools.partial(kernel, q_width, head),
        grid=(rows // seq,),
        in_specs=[pl.BlockSpec((seq, arg.shape[1]), lambda i: (i, 0)) for arg in args],
        out_specs=pl.BlockSpec((seq, width), lambda i: (i, 0)),
        out_shape=jax.ShapeDtypeStruct((rows, width), jnp.bfloat16),
        scratch_shapes=[pltpu.VMEM((seq, head), jnp.float32)] * scratch,
        cost_estimate=pl.CostEstimate(flops=flops, bytes_accessed=0, transcendentals=0),
    )(*args)


def attn_forward(x_own, weight, q_width, head, seq):
    normed = halves_of(norm_bf16(x_own))
    qkv = times(jnp.concatenate(normed), weight[:, :q_width + 2 * head]).astype(jnp.bfloat16)
    o_act = by_sequence(attn_fwd_kernel, seq, q_width, head, (qkv,), q_width, 0,
                  20_000_000_000)
    proj = both_halves(o_act, weight[:, q_width + 2 * head:], x_own.shape[0], times_flipped)
    y_own = (x_own.astype(jnp.float32) + proj).astype(jnp.bfloat16)
    return y_own, (x_own, normed, qkv, o_act)


def attn_grads_kernel(n0_ref, n1_ref, d_qkv_ref, g0_ref, g1_ref, o_ref, out_ref):
    width, rows = d_qkv_ref.shape[1], n0_ref.shape[0]
    halves = (slice(0, rows), slice(rows, 2 * rows))
    for cols, lefts, right in ((slice(0, width), (n0_ref, n1_ref), d_qkv_ref), (slice(width, None), (g0_ref, g1_ref), o_ref)):
        out_ref[:, cols] = sum(dot(left[...], right[half, :], ((0,), (0,))) for left, half in zip(lefts, halves))


def attn_grads(normed, d_qkv, grad_y, o_act):
    rows, width = normed[0].shape
    cols = d_qkv.shape[1] + o_act.shape[1]
    piece = pl.BlockSpec((rows, WIDTH_TILE), lambda i: (0, i))
    whole = [pl.BlockSpec(arg.shape, lambda i: (0, 0), pipeline_mode=pl.Buffered(1)) for arg in (d_qkv, o_act)]
    return pl.pallas_call(
        attn_grads_kernel,
        grid=(width // WIDTH_TILE,),
        in_specs=[piece, piece, whole[0], piece, piece, whole[1]],
        out_specs=pl.BlockSpec((WIDTH_TILE, cols), lambda i: (i, 0)),
        out_shape=jax.ShapeDtypeStruct((width, cols), jnp.float32),
        cost_estimate=pl.CostEstimate(flops=4 * rows * width * cols, bytes_accessed=0, transcendentals=0),
        name="attn_grads",
    )(*normed, d_qkv, *grad_y, o_act)


def attn_backward(saved, weight, q_width, head, seq, grad_own):
    x_own, normed, qkv, o_act = saved
    grad_y = (grad_own, swap(grad_own))
    d_o = times(jnp.concatenate(grad_y), weight[:, q_width + 2 * head:]).astype(jnp.bfloat16)
    d_qkv = by_sequence(attn_bwd_kernel, seq, q_width, head, (qkv, d_o), qkv.shape[1], 2,
                  40_000_000_000)
    d_norm = both_halves(d_qkv, weight[:, :q_width + 2 * head], grad_own.shape[0], times_flipped)
    grad_x = (grad_own.astype(jnp.float32) + norm_back(x_own, d_norm)).astype(jnp.bfloat16)
    return grad_x, attn_grads(normed, d_qkv, grad_y, o_act)


def gelu_parts(hidden):
    square = hidden * hidden
    half = 0.5 + 0.5 * jnp.tanh(hidden * (GELU_A + GELU_A * GELU_B * square))
    value = hidden * half
    slope = half + value * (1.0 - half) * (2.0 * GELU_A + 6.0 * GELU_A * GELU_B * square)
    return value.astype(jnp.bfloat16), slope


def mlp_hidden(normed, up_weight):
    return lax.optimization_barrier(gelu_parts(times(normed, up_weight)))


def mlp_output(x_own, gelu_act, down_weight):
    proj = both_halves(gelu_act, down_weight, x_own.shape[0], times)
    return (x_own.astype(jnp.float32) + proj).astype(jnp.bfloat16)


def mlp_backward(x_own, slope, up_weight, down_weight, grad_own):
    grad_act = times_flipped(pair_rows(grad_own), down_weight)
    d_hid = (grad_act * slope).astype(jnp.bfloat16)
    d_norm = both_halves(d_hid, up_weight, grad_own.shape[0], times_flipped)
    return (grad_own.astype(jnp.float32) + norm_back(x_own, d_norm)).astype(jnp.bfloat16)


def mlp_grads_kernel(place_ref, up_ref, down_ref, norm_ref, grad_ref, *rest):
    d_down_ref, parts, d_up_ref, flip_ref = rest[-2 * CHIPS - 3], rest[-2 * CHIPS - 2:-2], rest[-2], rest[-1]
    step = pl.program_id(0)
    normed, grad_y = norm_ref[...], grad_ref[...]

    @pl.when(step == 0)
    def _():
        d_down_ref[...] = jnp.zeros_like(d_down_ref)
        d_up_ref[...] = jnp.zeros_like(d_up_ref)

    gelu_act, slope = gelu_parts(dot(up_ref[...], normed, ((1,), (1,))))
    d_hid = (dot(down_ref[...], grad_y, ((1,), (1,))) * slope).astype(jnp.bfloat16)
    d_down_ref[0] += dot(gelu_act, grad_y, ((1,), (0,)))
    d_up_ref[...] += dot(d_hid, normed, ((1,), (0,)))

    @pl.when(step == pl.num_programs(0) - 1)
    def _():
        rows = parts[0].shape[0]
        for i in range(CHIPS):
            start = pl.multiple_of((place_ref[0] ^ i) * (CORES * rows), CORES * rows)
            flip_ref[...] = jnp.transpose(d_up_ref[:, pl.ds(start, CORES * rows)])
            for j in range(CORES):
                start = pl.multiple_of((place_ref[1] ^ j) * rows, rows)
                parts[CORES * i + j][...] = flip_ref[pl.ds(start, rows), :]


def mlp_weight_grads(place, layer, pairs, earlier, up_flip, down_block, rows_dev, tokens):
    block, width = down_block.shape
    rows = width // (CHIPS * CORES)
    once = pl.Buffered(1)
    whole = pl.BlockSpec((block, width), lambda i, p: (0, 0), pipeline_mode=once)
    tiles, specs = rows_dev // TOKEN_TILE, []
    for source, place_in in tokens:
        count = source.shape[0] // (CHIPS * CORES * rows_dev)
        specs.append(pl.BlockSpec((TOKEN_TILE, width), lambda i, p, count=count, k=place_in:
                                  (count * tiles * (i // tiles) + k * tiles + i % tiles, 0)))
    part = pl.BlockSpec((rows, block), lambda i, p: (0, 0), pipeline_mode=once)
    args = [place, up_flip, down_block, *[source for source, _ in tokens], *earlier]
    outs = pl.pallas_call(
        mlp_grads_kernel,
        grid_spec=pltpu.PrefetchScalarGridSpec(
            num_scalar_prefetch=1,
            grid=(tiles * CHIPS * CORES,),
            in_specs=[whole, whole] + specs + [pl.BlockSpec(memory_space=pl.ANY)] * len(earlier),
            out_specs=[pl.BlockSpec((1, block, width), lambda i, p: (layer, 0, 0), pipeline_mode=once)]
            + [part] * (CHIPS * CORES),
            scratch_shapes=[pltpu.VMEM((block, width), jnp.float32), pltpu.VMEM((CORES * rows, block), jnp.float32)],
        ),
        out_shape=[jax.ShapeDtypeStruct((pairs, block, width), jnp.float32)]
        + [jax.ShapeDtypeStruct((rows, block), jnp.float32)] * (CHIPS * CORES),
        input_output_aliases={len(args) - 1: 0} if earlier else {},
        compiler_params=pltpu.CompilerParams(vmem_limit_bytes=60 * 1024 * 1024),
        cost_estimate=pl.CostEstimate(flops=8 * CHIPS * CORES * rows_dev * block * width, bytes_accessed=0,
                                      transcendentals=0),
        name="mlp_grads",
    )(*args)
    return outs[0], outs[1:]


def exchange(parts):
    devices = range(CHIPS * CORES)
    return [lax.ppermute(part, AXES, [(d, d ^ i) for d in devices]) if i else part for i, part in enumerate(parts)]


def assemble_kernel(place_ref, *refs):
    parts, out_ref = [ref[...] for ref in refs[:CHIPS * CORES]], refs[-1]
    for bit in range(3):
        swapped = ((place_ref[0] * CORES + place_ref[1]) >> bit) % 2 == 1
        parts = [jnp.where(swapped, parts[i ^ (1 << bit)], part) for i, part in enumerate(parts)]
    for i, part in enumerate(parts):
        out_ref[0, :, i * part.shape[1]:(i + 1) * part.shape[1]] = part


def assemble(place, layer, pairs, earlier, parts):
    rows, block = parts[0].shape
    out_width = block * len(parts)
    return pl.pallas_call(
        assemble_kernel,
        grid_spec=pltpu.PrefetchScalarGridSpec(
            num_scalar_prefetch=1,
            grid=(rows // ROW_TILE,),
            in_specs=[pl.BlockSpec((ROW_TILE, block), lambda i, p: (i, 0))] * len(parts)
            + [pl.BlockSpec(memory_space=pl.ANY)] * len(earlier),
            out_specs=pl.BlockSpec((1, ROW_TILE, out_width), lambda i, p: (layer, i, 0)),
        ),
        out_shape=jax.ShapeDtypeStruct((pairs, rows, out_width), jnp.float32),
        input_output_aliases={1 + len(parts): 0} if earlier else {},
        cost_estimate=pl.CostEstimate(flops=5_000_000_000, bytes_accessed=0, transcendentals=0),
        name="assemble",
    )(place, *parts, *earlier)


def split_kernel(place_ref, rows_ref, keep_ref, send_ref):
    block = rows_ref.shape[2] // (CHIPS * CORES)
    for i in range(CHIPS):
        pair = [rows_ref[0, :, (CORES * i + j) * block:(CORES * i + j + 1) * block] for j in range(CORES)]
        cols = slice(i * block, (i + 1) * block)
        keep_ref[:, cols] = jnp.where(place_ref[1] == 0, pair[0], pair[1])
        send_ref[:, cols] = jnp.where(place_ref[1] == 0, pair[1], pair[0])


def split_columns(place, layer, weight):
    rows, cols = weight.shape[1:]
    half = jax.ShapeDtypeStruct((rows, cols // CORES), weight.dtype)
    return pl.pallas_call(
        split_kernel,
        grid_spec=pltpu.PrefetchScalarGridSpec(
            num_scalar_prefetch=1,
            grid=(rows // ROW_TILE,),
            in_specs=[pl.BlockSpec((1, ROW_TILE, cols), lambda i, p: (layer, i, 0))],
            out_specs=[pl.BlockSpec((ROW_TILE, cols // CORES), lambda i, p: (i, 0))] * CORES,
        ),
        out_shape=[half] * CORES,
        cost_estimate=pl.CostEstimate(flops=5_000_000_000, bytes_accessed=0, transcendentals=0),
        name="split",
    )(place, weight)


def flip_kernel(place_ref, up_ref, out_ref):
    block = out_ref.shape[0]
    for i in range(CHIPS):
        @pl.when(place_ref[0] == i)
        def _():
            out_ref[...] = jnp.transpose(up_ref[:, i * block:(i + 1) * block])


def flip(place, up_weight):
    width, cols = up_weight.shape
    return pl.pallas_call(
        flip_kernel,
        grid_spec=pltpu.PrefetchScalarGridSpec(
            num_scalar_prefetch=1,
            grid=(width // FLIP_TILE,),
            in_specs=[pl.BlockSpec((FLIP_TILE, cols), lambda i, p: (i, 0))],
            out_specs=pl.BlockSpec((cols // CHIPS, FLIP_TILE), lambda i, p: (0, i)),
        ),
        out_shape=jax.ShapeDtypeStruct((cols // CHIPS, width), jnp.bfloat16),
        cost_estimate=pl.CostEstimate(flops=5_000_000_000, bytes_accessed=0, transcendentals=0),
        name="flip",
    )(place, up_weight)


def solution(mesh):
    row_spec = P(AXES)
    weight_spec = P(None, AXES)

    def body(x_loc, w_q, w_k, w_v, w_o, w_up, w_down, grad_out):
        core = lax.axis_index(CORE)
        chip = lax.axis_index(CHIP)
        pairs, _, heads, head = w_q.shape
        seqs, seq, width = x_loc.shape
        q_width = heads // CORES * head

        place = jnp.stack([chip, core]).astype(jnp.int32)

        heads_in = [flip_heads(w) if by_head else w for w, by_head in zip((w_q, w_k, w_v, w_o), BY_HEAD)]

        def attn_piece(layer, core, place):
            return to_columns(core, *pack_heads(place, layer, heads_in))

        def up_piece(layer, core, place):
            return to_columns(core, *split_columns(place, layer, w_up))

        attn_full, up_full, down_full, up_flip = [], [], [], []

        def gather_weights(layer, core, place):
            attn_full.append(gather_weight(chip, attn_piece(layer, core, place)))
            up_full.append(gather_weight(chip, up_piece(layer, core, place)))
            down_full.append(gather_weight(chip, lax.optimization_barrier(w_down[layer])))
            up_flip.append(flip(place, up_full[layer]))

        gather_weights(0, core, place)
        carry_x = x_loc.reshape(seqs * seq, width)
        grad_x = grad_out.reshape(seqs * seq, width)
        attn_saved, mlp_saved, d_up, d_down = [], [], [], []

        def weight_grads(layer, tokens, d_down):
            down, parts = mlp_weight_grads(place, layer, pairs, d_down, up_flip[layer], w_down[layer],
                                           seqs * seq, tokens)
            return exchange(parts), [down]

        for layer in range(pairs):
            x_own, saved = attn_forward(carry_x, attn_full[layer], q_width, head, seq)
            attn_saved.append(saved)
            if layer < pairs - 1:
                x_own, *later = lax.optimization_barrier((x_own, core, place))
                gather_weights(layer + 1, *later)
            n_own = norm_bf16(x_own)
            gelu_act, slope = mlp_hidden(pair_rows(n_own), up_full[layer])
            mlp_saved.append((x_own, n_own, slope))
            if layer < pairs - 1:
                carry_x = mlp_output(x_own, gelu_act, down_full[layer])
        last = (x_own, gelu_act, down_full[-1])
        joined = jnp.concatenate([grad_x] + [saved[1] for saved in mlp_saved[::-1]])
        together = gather_rows(joined)
        d_heads, head_shapes = [], [weight.shape for weight in heads_in]
        for layer in reversed(range(pairs)):
            x_own, n_own, slope = mlp_saved[layer]
            grads = (together, 0) if layer == pairs - 1 else (gather_rows(grad_x), 0)
            parts, d_down = weight_grads(layer, [(together, pairs - layer), grads], d_down)
            d_up = [assemble(place, layer, pairs, d_up, parts)]
            grad_x = mlp_backward(x_own, slope, up_full[layer], down_full[layer], grad_x)
            grad_x, d_attn = attn_backward(attn_saved[layer], attn_full[layer], q_width, head, seq, grad_x)
            parts = to_rows(core, scatter_sum(d_attn))
            d_heads = place_heads(place, layer, head_shapes, d_heads, *parts)
        heads_out = tuple(flip_heads(w) if by_head else w for w, by_head in zip(d_heads, BY_HEAD))
        last, d_down = lax.optimization_barrier((last, d_down))
        y_loc = mlp_output(*last).reshape(x_loc.shape)
        return (y_loc, grad_x.reshape(x_loc.shape)) + heads_out + (d_up[0], d_down[0])

    return jax.shard_map(body, mesh=mesh, in_specs=(row_spec,) + (weight_spec,) * 6 + (row_spec,),
                         out_specs=(row_spec, row_spec) + (weight_spec,) * 6, check_vma=False)
```
